32 devices in a mesh: section: 4 (over z), dp: 8 (over y, x, core).
Axes of the slice: x: 2, y: 2, z: 4, core: 2. Of those that a mesh axis runs over, the one named last changes fastest.
Arguments:
- entry: bfloat16 [1536, 3584], P('dp'), may hold values from -6 to 6
- norm_gain: float32 [4, 3584], P('section'), may hold values from 0.5 to 1.5
- w_qkv: bfloat16 [4, 3584, 1152], P('section', 'dp'), may hold values from -0.09375 to 0.09375
- w_out: bfloat16 [4, 896, 3584], P('section', 'dp'), may hold values from -0.1875 to 0.1875
- final_gain: float32 [3584], replicated, may hold values from 0.5 to 1.5
- lengths: int32 [32], P('dp'), may hold values from 24 to 48
- positive: int32 [16], P('dp'), may hold values from 0 to 15, each once
Outputs:
- section_grads: bfloat16 [4, 1536, 3584], P('section', 'dp')
The draws below stay inside these ranges and needn't reach their ends.
Inputs may be any that keep to these rules, and one draw needn't show every extreme that they name: lengths[j] is the count of tokens of sequence j; its last token is pooled. Each document index is the positive of exactly one query.
All inputs are finite; a program needn't handle non-finite values.
Results may differ from the reference program's by a relative error of at most 0.022.
Values may be sent and summed in bfloat16 or wider, within the bound.
A program may use at most 192 MiB of HBM per device.

```python
import jax
import jax.numpy as jnp
from jax import lax

D = 3584
HEAD_DIM = 64
GROUP_HEADS = 7
KV_GROUPS = 2
LEN = 48
QW = 896
QUERIES = 16
SEQS = 32
TOKENS = 1536
N_SECTION = 4


def place_ends(values, rng, smallest, high):
    index_at = [jax.random.randint(jax.random.fold_in(rng, axis), (), 0, length) for axis, length in enumerate(values.shape)]
    main_axis = values.shape.index(max(values.shape))
    next_to = index_at[:main_axis] + [(index_at[main_axis] + 1) % values.shape[main_axis]] + index_at[main_axis + 1:]
    return values.at[tuple(index_at)].set(smallest).at[tuple(next_to)].set(high)


def shard_levels(rng, dims, shards, smallest, high):
    def one(axis_at, shards_of):
        steps = jax.random.uniform(jax.random.fold_in(jax.random.fold_in(rng, 6), axis_at), (shards_of,), jnp.float32, smallest / len(shards), high / len(shards))
        return jnp.repeat(jnp.exp(steps), dims[axis_at] // shards_of).reshape((-1,) + (1,) * (len(dims) - axis_at - 1))

    level = one(*shards[0])
    for cut in shards[1:]:
        level = level * one(*cut)
    return level


def noise(rng, dims, deviation, reach, shards=(), kind=jnp.bfloat16):
    drawn = jax.random.normal(rng, dims, jnp.float32) * deviation
    if len(shards) > 0:
        drawn = shard_levels(rng, dims, shards, -0.22, 0.18) * drawn
    return jnp.clip(drawn, min=-reach, max=reach).astype(kind)


def setup_inputs(seed: int = 0) -> dict:
    arg_keys = jax.random.split(jax.random.key(seed), 8)
    return {
        "entry": noise(arg_keys[0], (TOKENS, D), 1.0, 6.0, ((0, 8),)),
        "norm_gain": jnp.clip(1.0 + 0.1 * jax.random.normal(arg_keys[1], (N_SECTION, D), jnp.float32), 0.5, 1.5),
        "w_qkv": noise(arg_keys[2], (N_SECTION, D, QW + 2 * KV_GROUPS * HEAD_DIM), D ** -0.5, 0.09375, ((0, 4), (1, 8))),
        "w_out": noise(arg_keys[3], (N_SECTION, QW, D), QW ** -0.5, 0.1875, ((0, 4), (1, 8))),
        "final_gain": jnp.clip(1.0 + 0.1 * jax.random.normal(arg_keys[4], (D,), jnp.float32), 0.5, 1.5),
        "lengths": place_ends(jax.random.randint(arg_keys[5], (SEQS,), LEN // 2, LEN + 1), jax.random.fold_in(arg_keys[5], 1), LEN // 2, LEN).astype(jnp.int32),
        "positive": jax.random.permutation(arg_keys[6], QUERIES).astype(jnp.int32),
    }


rope_base = 1000000.0
norm_eps = 1e-06
sharpness_divisor = 0.05
objective_coefficient = 256.0

def rotary(values, positions):
    half_dim = values.shape[-1] // 2
    frequency = rope_base ** (-jnp.arange(half_dim, dtype=jnp.float32) * (2.0 / values.shape[-1]))
    angles = positions.astype(jnp.float32)[:, None] * frequency[None, :]
    cosine = jnp.cos(angles)[:, None, :]
    sine_part = jnp.sin(angles)[:, None, :]
    first_half = values[..., :half_dim]
    second_half = values[..., half_dim:]
    return jnp.concatenate([first_half * cosine - second_half * sine_part, second_half * cosine + first_half * sine_part], axis=-1)

def rms_scale(values, gain_row):
    return values * lax.rsqrt(lax.optimization_barrier(jnp.mean(values * values, axis=-1, keepdims=True)) + norm_eps) * gain_row

def attention_layer(hidden, seq_lengths, gain_row, weight_qkv, weight_out):
    row_count, row_width = hidden.shape
    seq_count = seq_lengths.shape[0]
    length = row_count // seq_count
    q_width = weight_out.shape[0]
    kv_width = KV_GROUPS * HEAD_DIM
    wide_in = hidden.astype(jnp.float32)
    normed = rms_scale(wide_in, gain_row).astype(jnp.bfloat16)
    projected = jnp.dot(normed, weight_qkv, preferred_element_type=jnp.float32)
    positions = jnp.arange(length, dtype=jnp.int32)
    query_rot = rotary(projected[:, :q_width].reshape(seq_count, length, KV_GROUPS * GROUP_HEADS, HEAD_DIM), positions).astype(jnp.bfloat16)
    key_rot = rotary(projected[:, q_width:q_width + kv_width].reshape(seq_count, length, KV_GROUPS, HEAD_DIM), positions).astype(jnp.bfloat16)
    value_rows = projected[:, q_width + kv_width:].reshape(seq_count, length, KV_GROUPS, HEAD_DIM).astype(jnp.bfloat16)
    query_grid = query_rot.reshape(seq_count, length, KV_GROUPS, GROUP_HEADS, HEAD_DIM)
    scores = jnp.einsum('sqgzd,skgd->sgzqk', query_grid.astype(jnp.float32), key_rot.astype(jnp.float32)) * HEAD_DIM ** (-0.5)
    key_live = positions[None, :] < seq_lengths[:, None]
    weights = jnp.where(key_live[:, None, None, None, :], jnp.exp(scores), 0.0)
    prob_low = (weights / lax.optimization_barrier(jnp.sum(weights, axis=-1, keepdims=True))).astype(jnp.bfloat16)
    context = jnp.einsum('sgzqk,skgd->sqgzd', prob_low.astype(jnp.float32), value_rows.astype(jnp.float32)).astype(jnp.bfloat16)
    branch = jnp.dot(context.reshape(row_count, q_width), weight_out, preferred_element_type=jnp.float32)
    return (wide_in + branch).astype(jnp.bfloat16)

def embed_rows(rows_in, final_gain):
    pooled = rms_scale(rows_in.astype(jnp.float32), final_gain)
    return pooled * lax.rsqrt(lax.optimization_barrier(jnp.sum(pooled * pooled, axis=-1, keepdims=True)))

def pair_terms(question_representation, passage_representation, positive):
    match_raw_scores = jnp.dot(question_representation, passage_representation.T, preferred_element_type=jnp.float32) * (1.0 / sharpness_divisor)
    weights = jnp.exp(match_raw_scores)
    normalized_exponential_odds = weights / lax.optimization_barrier(jnp.sum(weights, axis=-1, keepdims=True))
    correct_target_column = (positive[:, None] == jnp.arange(passage_representation.shape[0], dtype=jnp.int32)[None, :]).astype(jnp.float32)
    return (normalized_exponential_odds - correct_target_column) * (objective_coefficient / sharpness_divisor)

def reference(entry, norm_gain, w_qkv, w_out, final_gain, lengths, positive):
    section_count = norm_gain.shape[0]
    seq_count = lengths.shape[0]
    length = entry.shape[0] // seq_count
    row_width = entry.shape[1]
    hidden = entry
    inputs = []
    for layer_id in range(section_count):
        inputs.append(hidden)
        hidden = attention_layer(hidden, lengths, norm_gain[layer_id], w_qkv[layer_id], w_out[layer_id])
    seq_grid = hidden.reshape(seq_count, length, row_width)
    last_rows = jnp.take_along_axis(seq_grid, (lengths - 1)[:, None, None], axis=1)[:, 0]
    embedding, back_embed = jax.vjp(lambda rows_in: embed_rows(rows_in, final_gain), last_rows)
    emb_low = embedding.astype(jnp.bfloat16)
    question_representation = emb_low[0::2]
    passage_representation = emb_low[1::2]
    pair_coef = pair_terms(question_representation, passage_representation, positive)
    grad_query = jnp.dot(pair_coef, passage_representation.astype(jnp.float32), precision=lax.Precision.HIGHEST)
    grad_doc = jnp.dot(pair_coef.T, question_representation.astype(jnp.float32), precision=lax.Precision.HIGHEST)
    grad_emb = jnp.stack([grad_query, grad_doc], axis=1).reshape(seq_count, row_width)
    grad_last = back_embed(grad_emb)[0]
    slot_hit = jnp.arange(length, dtype=jnp.int32)[None, :] == (lengths - 1)[:, None]
    seed_grad = jnp.where(slot_hit[:, :, None], grad_last[:, None, :], 0).astype(jnp.bfloat16).reshape(-1, row_width)
    cotangent = seed_grad
    collected = []
    for layer_id in reversed(range(section_count)):
        _, pull_back = jax.vjp(lambda values: attention_layer(values, lengths, norm_gain[layer_id], w_qkv[layer_id], w_out[layer_id]), inputs[layer_id])
        cotangent = pull_back(cotangent)[0]
        collected.append(cotangent)
    return jnp.stack(collected[::-1])
```

```python
import functools

import jax
import jax.numpy as jnp
import numpy as np
from jax import lax
from jax.experimental import pallas as pl
from jax.experimental.pallas import tpu as pltpu
from jax.sharding import PartitionSpec as P

HEAD_DIM = 64
GROUP_HEADS = 7
KV_GROUPS = 2
HEADS = GROUP_HEADS * KV_GROUPS
ROPE_BASE = 1000000.0
EPS = 1e-06
SHARPNESS = 20.0
COEF = 256.0
MESH = pl.DeviceIdType.MESH
F32 = jnp.float32
BF16 = jnp.bfloat16
HI = lax.Precision.HIGHEST


def dot_nn(a, b):
    return lax.dot_general(a, b, (((1,), (0,)), ((), ())), preferred_element_type=F32)


def dot_nt(a, b):
    return lax.dot_general(a, b, (((1,), (1,)), ((), ())), preferred_element_type=F32)


def dot_tn(a, b):
    return lax.dot_general(a, b, (((0,), (0,)), ((), ())), preferred_element_type=F32)


def dot_hi(a, b):
    return lax.dot_general(
        a, b, (((1,), (0,)), ((), ())), preferred_element_type=F32, precision=HI
    )


def rotate(x, cos, sin_signed):
    width = x.shape[-1]
    lane = lax.broadcasted_iota(jnp.int32, x.shape, 1)
    first = lax.rem(lane, HEAD_DIM) < HEAD_DIM // 2
    ahead = pltpu.roll(x, width - HEAD_DIM // 2, 1)
    behind = pltpu.roll(x, HEAD_DIM // 2, 1)
    return x * cos + jnp.where(first, ahead, behind) * sin_signed


def low_half(shape):
    return lax.broadcasted_iota(jnp.int32, shape, 1) < HEAD_DIM


def both_halves(tile):
    wide = tile.astype(F32)
    turned = pltpu.roll(wide, HEAD_DIM, 1)
    low = low_half(wide.shape)
    return (
        jnp.where(low, wide, turned).astype(BF16),
        jnp.where(low, turned, wide).astype(BF16),
    )


def stack_heads(rows, group):
    parts = []
    for head in range(group * GROUP_HEADS, (group + 1) * GROUP_HEADS):
        tile = rows[:, head // 2 * 128 : head // 2 * 128 + 128].astype(F32)
        low = low_half(tile.shape)
        keep = low if head % 2 == 0 else jnp.logical_not(low)
        parts.append(jnp.where(keep, tile, 0.0).astype(BF16))
    return jnp.concatenate(parts, axis=0)


def merge_heads(stacks, length):
    tiles = []
    for pair in range(HEADS // 2):
        halves = []
        for head in (2 * pair, 2 * pair + 1):
            at = head % GROUP_HEADS * length
            halves.append(stacks[head // GROUP_HEADS][at : at + length])
        tiles.append(jnp.where(low_half(halves[0].shape), halves[0], halves[1]))
    return jnp.concatenate(tiles, axis=1)


def fold_groups(sums):
    full = [value + pltpu.roll(value, HEAD_DIM, 1) for value in sums]
    return jnp.where(low_half(full[0].shape), full[0], full[1])


def rms_of(wide):
    return lax.rsqrt(jnp.mean(wide * wide, axis=-1, keepdims=True) + EPS)


def kernel(
    n_sec, n_dp, seqs, length, ring,
    entry, gain, w_in, w_up, final_gain, cos_ref, sin_ref, lengths, positive,
    out,
    hin, hout, gin, xs, probs, rows_buf, emb_all, pos_all, contexts,
    f_send, f_recv, b_send, b_recv, e_send, e_recv, p_send, p_recv,
    *gathering,
):
    sec = lax.axis_index("section")
    rep = lax.axis_index("dp")
    last = n_sec - 1
    width = entry.shape[-1]
    wqkv, wout = gathering[:2] if ring else (w_in, w_up)
    qw = wout.shape[0]
    blocks = 16 // seqs
    part = width // blocks
    micro = seqs // 2

    barrier = pltpu.get_barrier_semaphore()

    def peer(step):
        return lax.rem(rep + step, n_dp)

    for near in (lax.rem(sec + 1, n_sec), lax.rem(sec + n_sec - 1, n_sec)):
        pl.semaphore_signal(barrier, inc=1, device_id={"section": near}, device_id_type=MESH)
    for step in range(1, n_dp):
        pl.semaphore_signal(barrier, inc=1, device_id={"dp": peer(step)}, device_id_type=MESH)
    pl.semaphore_wait(barrier, n_dp + 1)

    def forward_copy(m):
        return pltpu.make_async_remote_copy(
            src_ref=hout.at[m], dst_ref=hin.at[m], send_sem=f_send.at[m], recv_sem=f_recv.at[m],
            device_id={"section": sec + 1}, device_id_type=MESH,
        )

    def backward_copy(m):
        return pltpu.make_async_remote_copy(
            src_ref=out.at[m], dst_ref=gin.at[m], send_sem=b_send.at[m], recv_sem=b_recv.at[m],
            device_id={"section": sec - 1}, device_id_type=MESH,
        )

    @pl.when(sec == 0)
    def _():
        hin[...] = entry[...]

    def live_keys(m):
        keys = lax.broadcasted_iota(jnp.int32, (GROUP_HEADS * length, length), 1)
        return keys < lengths[m]

    def attend(m):
        wide = hin[m].astype(F32)
        normed = (wide * rms_of(wide) * gain[...]).astype(BF16)
        x = rotate(dot_nn(normed, wqkv[...]), cos_ref[...], sin_ref[...]).astype(BF16)
        xs[m] = x
        keys = both_halves(x[:, qw : qw + 128])
        values = both_halves(x[:, qw + 128 : qw + 256])
        live = live_keys(m)
        stacks = []
        for group in range(KV_GROUPS):
            scores = dot_nt(stack_heads(x, group), keys[group]) * HEAD_DIM ** (-0.5)
            weights = jnp.where(live, jnp.exp(scores), 0.0)
            prob = weights / jnp.sum(weights, axis=-1, keepdims=True)
            probs[m, group] = prob
            stacks.append(dot_nn(prob.astype(BF16), values[group]))
        contexts[m] = merge_heads(stacks, length).astype(BF16)

    if ring:
        hop_send, hop_recv, side_send, side_recv, keep_sem = gathering[2:]
        chips = n_dp // 2
        reach = chips // 2
        core = lax.rem(rep, 2)
        chip = rep // 2

        def place(c):
            return c + (c // 2) * (1 - 2 * lax.rem(c, 2)) if chips == 4 else c

        at = place(chip)
        pieces = ((w_in, wqkv), (w_up, wout))

        def region(piece, shard, half):
            held = pieces[piece][1]
            rows = pieces[piece][0].shape[0]
            cols = held.shape[1]
            cut = (cols // 128 + 1) // 2 * 128
            span = {None: (0, cols), 0: (0, cut), 1: (cut, cols - cut)}[half]
            start = pl.multiple_of(shard * rows, rows)
            return held.at[pl.ds(start, rows), pl.ds(*span)]

        def own(piece, half):
            mine, held = pieces[piece]
            if half is None:
                return mine
            cols = held.shape[1]
            cut = (cols // 128 + 1) // 2 * 128
            return mine.at[:, pl.ds(*((0, cut), (cut, cols - cut))[half])]

        def half_of(way, step):
            return way if step == reach else None

        def hop(piece, way, step):
            turn = 1 if way == 0 else chips - 1
            source = place(lax.rem(at + (step - 1) * (chips - turn), chips)) * 2 + core
            half = half_of(way, step)
            target = place(lax.rem(at + turn, chips)) * 2 + core
            dst = region(piece, source, half)
            return pltpu.make_async_remote_copy(
                src_ref=own(piece, half) if step == 1 else dst, dst_ref=dst,
                send_sem=hop_send.at[piece, way, step - 1],
                recv_sem=hop_recv.at[piece, way, step - 1],
                device_id={"dp": target}, device_id_type=MESH,
            )

        def side(piece, way, step):
            turn = 1 if way == 0 else chips - 1
            source = place(lax.rem(at + step * (chips - turn), chips)) * 2 + core
            half = half_of(way, step)
            dst = region(piece, source, half)
            return pltpu.make_async_remote_copy(
                src_ref=own(piece, None) if step == 0 else dst, dst_ref=dst,
                send_sem=side_send.at[piece, way, step],
                recv_sem=side_recv.at[piece, way, step],
                device_id={"dp": chip * 2 + 1 - core}, device_id_type=MESH,
            )

        def keep(piece):
            return pltpu.make_async_copy(
                own(piece, None), region(piece, rep, None), keep_sem.at[piece]
            )

        sides = [(0, 0)] + [(way, step) for step in range(1, reach + 1) for way in (0, 1)]

        def begin(piece):
            for way in (0, 1):
                hop(piece, way, 1).start()
            side(piece, 0, 0).start()
            keep(piece).start()

        def advance(piece, step):
            for way in (0, 1):
                hop(piece, way, step).wait_recv()
                if step < reach:
                    hop(piece, way, step + 1).start()
                side(piece, way, step).start()

        def finish(piece):
            advance(piece, reach)
            keep(piece).wait()
            for way, step in sides:
                side(piece, way, step).wait_recv()

        begin(0)
        for step in range(1, reach):
            advance(0, step)
        begin(1)
        finish(0)

    def early(m, carry):
        if ring:
            @pl.when(m == seqs // 2)
            def _():
                for step in range(1, reach):
                    advance(1, step)

        @pl.when(sec == 0)
        def _():
            attend(m)

        return carry

    lax.fori_loop(0, seqs, early, 0)
    if ring:
        finish(1)

    def forward(m, carry):
        @pl.when(sec > 0)
        def _():
            forward_copy(m).wait_recv()
            attend(m)

        hout[m] = (hin[m].astype(F32) + dot_nn(contexts[m], wout[...])).astype(BF16)

        @pl.when(sec < last)
        def _():
            forward_copy(m).start()

        return carry

    lax.fori_loop(0, seqs, forward, 0)

    @pl.when(sec == last)
    def _():
        fgain = final_gain[...]
        row16 = lax.broadcasted_iota(jnp.int32, (16, part), 0)
        position = lax.broadcasted_iota(jnp.int32, (length, width), 0)
        own = jnp.zeros((16, part), F32)
        for j in range(seqs):
            picked = jnp.where(position == lengths[j] - 1, hout[j].astype(F32), 0.0)
            row = jnp.sum(picked, axis=0, keepdims=True)
            rows_buf[j] = row
            pooled = row * rms_of(row) * fgain
            unit = pooled * lax.rsqrt(jnp.sum(pooled * pooled, axis=-1, keepdims=True))
            for b in range(blocks):
                own = jnp.where(row16 == b * seqs + j, unit[:, b * part : (b + 1) * part], own)
        emb_all[rep] = own.astype(BF16)
        marks = jnp.zeros((8, 128), jnp.int32)
        mark_row = lax.broadcasted_iota(jnp.int32, (8, 128), 0)
        for i in range(micro):
            marks = jnp.where(mark_row == i, positive[i], marks)
        pos_all[rep] = marks

        def exchange(step):
            to = peer(step)
            return [
                pltpu.make_async_remote_copy(
                    src_ref=buf.at[rep], dst_ref=buf.at[rep],
                    send_sem=send.at[step], recv_sem=recv.at[step],
                    device_id={"dp": to}, device_id_type=MESH,
                )
                for buf, send, recv in ((emb_all, e_send, e_recv), (pos_all, p_send, p_recv))
            ]

        copies = [exchange(step) for step in range(1, n_dp)]
        for pair in copies:
            for copy in pair:
                copy.start()
        for pair in copies:
            for copy in pair:
                copy.wait()

        total = n_dp * seqs
        tall = n_dp * 16
        everyone = emb_all[...].reshape(tall, part)
        cross = dot_nt(everyone, everyone)
        ra = lax.broadcasted_iota(jnp.int32, (tall, tall), 0)
        ca = lax.broadcasted_iota(jnp.int32, (tall, tall), 1)
        same = lax.rem(ra, 16) // seqs == lax.rem(ca, 16) // seqs
        cross = jnp.where(same, cross, 0.0)
        fr = lax.broadcasted_iota(jnp.int32, (total, tall), 0)
        fc = lax.broadcasted_iota(jnp.int32, (total, tall), 1)
        fold = (fc // 16 * seqs + lax.rem(fc, seqs) == fr).astype(F32)
        logits = SHARPNESS * lax.dot_general(
            dot_hi(fold, cross), fold, (((1,), (1,)), ((), ())),
            preferred_element_type=F32, precision=HI,
        )
        qr = lax.broadcasted_iota(jnp.int32, (total, total), 0)
        dc = lax.broadcasted_iota(jnp.int32, (total, total), 1)
        doc = lax.rem(dc, 2) == 1
        weights = jnp.where(doc, jnp.exp(logits), 0.0)
        odds = weights / jnp.sum(weights, axis=-1, keepdims=True)
        marks_all = pos_all[...].reshape(n_dp * 8, 128).astype(F32)
        pr = lax.broadcasted_iota(jnp.int32, (total, n_dp * 8), 0)
        pc = lax.broadcasted_iota(jnp.int32, (total, n_dp * 8), 1)
        pick = (pr // seqs * 8 + lax.rem(pr, seqs) // 2 == pc).astype(F32)
        target = dot_hi(pick, marks_all)[:, :1]
        hit = jnp.logical_and(doc, (dc // 2).astype(F32) == target).astype(F32)
        coef = (odds - hit) * (COEF * SHARPNESS)
        coef = jnp.where(lax.rem(qr, 2) == 0, coef, 0.0)
        both = coef + coef.T
        ar = lax.broadcasted_iota(jnp.int32, (16, total), 0)
        ac = lax.broadcasted_iota(jnp.int32, (16, total), 1)
        mine = (rep * seqs + lax.rem(ar, seqs) == ac).astype(F32)
        spread = dot_hi(dot_hi(mine, both), fold)
        br = lax.broadcasted_iota(jnp.int32, (16, tall), 0)
        bc = lax.broadcasted_iota(jnp.int32, (16, tall), 1)
        spread = jnp.where(br // seqs == lax.rem(bc, 16) // seqs, spread, 0.0)
        grad16 = dot_hi(spread, everyone.astype(F32))
        for j in range(seqs):
            grad_e = jnp.concatenate(
                [grad16[b * seqs + j : b * seqs + j + 1] for b in range(blocks)], axis=1
            )
            row = rows_buf[j]
            scale = rms_of(row)
            pooled = row * scale * fgain
            size = lax.rsqrt(jnp.sum(pooled * pooled, axis=-1, keepdims=True))
            unit = pooled * size
            grad_f = size * (grad_e - unit * jnp.sum(unit * grad_e, axis=-1, keepdims=True))
            grad_n = grad_f * fgain
            grad_r = grad_n * scale - row * (
                scale * scale * scale * jnp.mean(row * grad_n, axis=-1, keepdims=True)
            )
            gin[j] = jnp.where(position == lengths[j] - 1, grad_r, 0.0).astype(BF16)

    def backward(m, carry):
        @pl.when(sec < last)
        def _():
            backward_copy(m).wait_recv()

        grad = gin[m]
        x = xs[m]
        keys = both_halves(x[:, qw : qw + 128])
        values = both_halves(x[:, qw + 128 : qw + 256])
        grad_ctx = dot_nt(grad, wout[...]).astype(BF16)
        grad_q, grad_k, grad_v = [], [], []
        for group in range(KV_GROUPS):
            prob = probs[m, group]
            upper = stack_heads(grad_ctx, group)
            grad_p = dot_nt(upper, values[group]).astype(BF16).astype(F32)
            grad_v.append(dot_tn(prob.astype(BF16), upper))
            inner = jnp.sum(grad_p * prob, axis=-1, keepdims=True)
            grad_s = (prob * (grad_p - inner) * HEAD_DIM ** (-0.5)).astype(BF16)
            grad_q.append(dot_nn(grad_s, keys[group]))
            grad_k.append(dot_tn(grad_s, stack_heads(x, group)))
        grad_x = jnp.concatenate(
            [merge_heads(grad_q, length), fold_groups(grad_k), fold_groups(grad_v)], axis=1
        )
        grad_x = grad_x.astype(BF16).astype(F32)
        grad_x = rotate(grad_x, cos_ref[...], -sin_ref[...]).astype(BF16)
        grad_n = dot_nt(grad_x, wqkv[...]).astype(BF16).astype(F32) * gain[...]
        wide = hin[m].astype(F32)
        scale = rms_of(wide)
        slope = scale * scale * scale * jnp.mean(wide * grad_n, axis=-1, keepdims=True)
        out[m] = (grad.astype(F32) + grad_n * scale - wide * slope).astype(BF16)

        @pl.when(sec > 0)
        def _():
            backward_copy(m).start()

        return carry

    lax.fori_loop(0, seqs, backward, 0)

    @pl.when(sec < last)
    def _():
        for m in range(seqs):
            forward_copy(m).wait_send()

    @pl.when(sec > 0)
    def _():
        for m in range(seqs):
            backward_copy(m).wait_send()

    if ring:
        for piece in (0, 1):
            for way in (0, 1):
                for step in range(1, reach + 1):
                    hop(piece, way, step).wait_send()
            for way, step in sides:
                side(piece, way, step).wait_send()


def swift(
    n_sec, n_dp, seqs, length,
    entry, gain, w_in, w_up, final_gain, cos_ref, sin_ref, lengths, positive,
    out,
    hin, hbase, hnext, gin, gout, pre, xs, probs, ctx, ctxp, wqkv, wout, wprev, wkvn, gain_next,
    kvn, rowf, rown, gkv, tail, emb_all, pos_all,
    hop_send, hop_recv, side_send, side_recv, keep_sem, up_send, up_recv,
    c_send, c_recv, f_send, f_recv, b_send, b_recv, k_send, k_recv,
    v_send, v_recv, g_send, g_recv, e_send, e_recv, p_send, p_recv,
):
    sec = lax.axis_index("section")
    rep = lax.axis_index("dp")
    last = n_sec - 1
    pen = n_sec - 2
    width = entry.shape[-1]
    qw = wout.shape[0]
    blocks = 16 // seqs
    part = width // blocks
    micro = seqs // 2
    inner_plane = jnp.logical_and(sec >= 1, sec <= pen)

    barrier = pltpu.get_barrier_semaphore()

    def peer(step):
        return lax.rem(rep + step, n_dp)

    for near in (lax.rem(sec + 1, n_sec), lax.rem(sec + n_sec - 1, n_sec)):
        pl.semaphore_signal(barrier, inc=1, device_id={"section": near}, device_id_type=MESH)
    for step in range(1, n_dp):
        pl.semaphore_signal(barrier, inc=1, device_id={"dp": peer(step)}, device_id_type=MESH)
    pl.semaphore_wait(barrier, n_dp + 1)

    def to_section(src, dst, send, recv, turn):
        return pltpu.make_async_remote_copy(
            src_ref=src, dst_ref=dst, send_sem=send, recv_sem=recv,
            device_id={"section": sec + turn}, device_id_type=MESH,
        )

    core = lax.rem(rep, 2)
    chip = rep // 2
    chips = n_dp // 2

    def place(c):
        return c + (c // 2) * (1 - 2 * lax.rem(c, 2))

    at = place(chip)
    held = (wqkv, wout, wprev)
    shard_rows = (w_in.shape[0], w_up.shape[0], w_up.shape[0])

    def span(piece, half):
        cols = held[piece].shape[1]
        cut = (cols // 128 + 1) // 2 * 128
        return {None: (0, cols), 0: (0, cut), 1: (cut, cols - cut)}[half]

    def region(piece, shard, half):
        rows = shard_rows[piece]
        start = pl.multiple_of(shard * rows, rows)
        return held[piece].at[pl.ds(start, rows), pl.ds(*span(piece, half))]

    def own(piece, half):
        if piece == 2:
            return region(2, rep, half)
        return (w_in, w_up)[piece].at[:, pl.ds(*span(piece, half))]

    def source_of(way, step):
        turn = 1 if way == 0 else chips - 1
        return place(lax.rem(at + step * (chips - turn), chips)) * 2 + core

    def hop(piece, way, slot):
        turn = 1 if way == 0 else chips - 1
        target = place(lax.rem(at + turn, chips)) * 2 + core
        half = way if slot == 2 else slot
        dst = region(piece, rep if slot < 2 else source_of(way, 1), half)
        return pltpu.make_async_remote_copy(
            src_ref=own(piece, half) if slot < 2 else dst, dst_ref=dst,
            send_sem=hop_send.at[piece, way, slot], recv_sem=hop_recv.at[piece, way, slot],
            device_id={"dp": target}, device_id_type=MESH,
        )

    def hop_in(piece, way, slot):
        half = way if slot == 2 else slot
        dst = region(piece, source_of(way, 2 if slot == 2 else 1), half)
        return pltpu.make_async_remote_copy(
            src_ref=dst, dst_ref=dst,
            send_sem=hop_send.at[piece, way, slot], recv_sem=hop_recv.at[piece, way, slot],
            device_id={"dp": chip * 2 + 1 - core}, device_id_type=MESH,
        )

    def side(piece, way, slot):
        half = way if slot == 2 else slot
        shard = rep if way == 2 else source_of(way, 2 if slot == 2 else 1)
        dst = region(piece, shard, half)
        return pltpu.make_async_remote_copy(
            src_ref=own(piece, half) if way == 2 else dst, dst_ref=dst,
            send_sem=side_send.at[piece, way, slot], recv_sem=side_recv.at[piece, way, slot],
            device_id={"dp": chip * 2 + 1 - core}, device_id_type=MESH,
        )

    near = [(2, 0), (2, 1)] + [(way, slot) for slot in range(2) for way in (0, 1)]
    far = [(0, 2), (1, 2)]

    def keep(piece):
        return pltpu.make_async_copy(own(piece, None), region(piece, rep, None), keep_sem.at[piece])

    def take(piece, way, slot):
        hop_in(piece, way, slot).wait_recv()
        side(piece, way, slot).start()

    def hand_on(piece):
        take(piece, 0, 0)
        hop(piece, 0, 2).start()
        take(piece, 1, 1)
        hop(piece, 1, 2).start()

    def finish_near(piece):
        take(piece, 0, 1)
        take(piece, 1, 0)
        if piece < 2:
            keep(piece).wait()
        for way, slot in near:
            side(piece, way, slot).wait_recv()

    def finish_far(piece):
        for way, slot in far:
            take(piece, way, slot)
        for way, slot in far:
            side(piece, way, slot).wait_recv()

    def finish(piece):
        finish_near(piece)
        finish_far(piece)

    def entry_copy(dst):
        return pltpu.make_async_copy(entry, dst, keep_sem.at[2])

    def up(half):
        return to_section(own(1, half), region(2, rep, half), up_send.at[half], up_recv.at[half], 1)

    def ctx_copy(m):
        return to_section(ctx.at[m], ctxp.at[m], c_send.at[m], c_recv.at[m], 1)

    def h_copy(m):
        return to_section(hin.at[m], hbase.at[m], f_send.at[m], f_recv.at[m], 1)

    def h_last(m):
        return to_section(hnext.at[m], hbase.at[m], f_send.at[m], f_recv.at[m], 1)

    cuts = 4
    piece_width = width // cuts

    def g_copy(m, c):
        return to_section(gout.at[m, c], gin.at[m, c], b_send.at[m, c], b_recv.at[m, c], -1)

    def kv_weights():
        return (
            to_section(wqkv.at[:, pl.ds(qw, 256)], wkvn, k_send.at[0], k_recv.at[0], -1),
            to_section(gain, gain_next, k_send.at[1], k_recv.at[1], -1),
        )

    def top(buf):
        return buf.at[pl.ds(0, 8)]

    def kv_up():
        return (
            to_section(kvn, kvn, v_send.at[0], v_recv.at[0], 1),
            to_section(top(rown), top(rown), v_send.at[1], v_recv.at[1], 1),
        )

    def gkv_copy(m):
        return to_section(gkv.at[m], gkv.at[m], g_send.at[m], g_recv.at[m], -1)

    def tail_copy():
        return to_section(top(tail), top(tail), g_send.at[seqs], g_recv.at[seqs], -1)

    @pl.when(sec < pen)
    def _():
        up(0).start()
        up(1).start()

    for way in (0, 1):
        hop(0, way, way).start()
    for piece in (0, 1):
        keep(piece).start()
        side(piece, 2, 0).start()
        side(piece, 2, 1).start()

    @pl.when(jnp.logical_not(inner_plane))
    def _():
        for way in (0, 1):
            hop(0, way, 1 - way).start()

    @pl.when(sec == 0)
    def _():
        entry_copy(hin).start()

    @pl.when(sec == 1)
    def _():
        entry_copy(hbase).start()

    @pl.when(inner_plane)
    def _():
        for half in (0, 1):
            up(half).wait_recv()
            side(2, 2, half).start()
            for way in (0, 1):
                hop(2, way, half).start()
        hand_on(2)
        for way in (0, 1):
            hop(0, way, 1 - way).start()

    hand_on(0)
    for way in (0, 1):
        hop(1, way, way).start()
    for way in (0, 1):
        hop(1, way, 1 - way).start()

    def step_in(m):
        ctx_copy(m).wait_recv()

        @pl.when(sec > 1)
        def _():
            h_copy(m).wait_recv()

        hin[m] = (hbase[m].astype(F32) + dot_nn(ctxp[m], wprev[...])).astype(BF16)

    def normalise(m, carry):
        wide = hin[m].astype(F32)
        hnext[m] = (wide * rms_of(wide) * gain[...]).astype(BF16)
        return carry

    def chip_part(c):
        depth = 2 * w_in.shape[0]
        rows = pl.ds(pl.multiple_of(c * depth, depth), depth)
        left = hnext[:, :, rows].reshape(seqs * length, depth)
        return dot_nn(left, wqkv[rows, :]).reshape(seqs, length, wqkv.shape[1])

    @pl.when(sec == 0)
    def _():
        entry_copy(hin).wait()
        lax.fori_loop(0, seqs, normalise, 0)

    @pl.when(inner_plane)
    def _():
        finish(2)

    @pl.when(sec == 1)
    def _():
        entry_copy(hbase).wait()

        def ahead(m, carry):
            step_in(m)
            normalise(m, 0)

            @pl.when(jnp.logical_and(sec < pen, m < seqs - 1))
            def _():
                h_copy(m).start()

            return carry

        lax.fori_loop(0, seqs, ahead, 0)

    finish_near(0)

    @pl.when(sec <= 1)
    def _():
        pre[...] = chip_part(chip)

        def beside(step, carry):
            pre[...] += chip_part(place(lax.rem(at + 2 * step + 1, chips)))
            return carry

        lax.fori_loop(0, 2, beside, 0)

    finish_far(0)

    @pl.when(sec <= 1)
    def _():
        pre[...] += chip_part(place(lax.rem(at + 2, chips)))

    @pl.when(sec == last)
    def _():
        for copy in kv_weights():
            copy.start()

    @pl.when(sec == last)
    def _():
        hand_on(1)

    def live_keys(m, rows):
        return lax.broadcasted_iota(jnp.int32, (rows, length), 1) < lengths[m]

    def project(m):
        wide = hin[m].astype(F32)
        normed = (wide * rms_of(wide) * gain[...]).astype(BF16)
        pre[m] = dot_nn(normed, wqkv[...])

    def attend(m):
        x = rotate(pre[m], cos_ref[...], sin_ref[...]).astype(BF16)
        xs[m] = x
        keys = both_halves(x[:, qw : qw + 128])
        values = both_halves(x[:, qw + 128 : qw + 256])
        live = live_keys(m, GROUP_HEADS * length)
        stacks = []
        for group in range(KV_GROUPS):
            scores = dot_nt(stack_heads(x, group), keys[group]) * HEAD_DIM ** (-0.5)
            weights = jnp.where(live, jnp.exp(scores), 0.0)
            prob = weights / jnp.sum(weights, axis=-1, keepdims=True)
            probs[m, group] = prob
            stacks.append(dot_nn(prob.astype(BF16), values[group]))
        ctx[m] = merge_heads(stacks, length).astype(BF16)

    @pl.when(sec < last)
    def _():
        def forward(m, carry):
            @pl.when(sec > 1)
            def _():
                step_in(m)

                @pl.when(sec < pen)
                def _():
                    h_copy(m).start()

                project(m)

                @pl.when(jnp.logical_and(sec == pen, m == seqs // 2))
                def _():
                    hand_on(1)

            attend(m)

            @pl.when(sec < pen)
            def _():
                ctx_copy(m).start()

                @pl.when(jnp.logical_and(sec == 1, m == seqs - 2))
                def _():
                    h_copy(seqs - 1).start()

            return carry

        lax.fori_loop(0, seqs, forward, 0)

    @pl.when(sec < pen)
    def _():
        hand_on(1)

    finish(1)

    flat = seqs * length
    row8 = lax.broadcasted_iota(jnp.int32, (8, 1), 0)
    spot = lax.broadcasted_iota(jnp.int32, (length, 1), 0)

    def pick(value, j):
        return jnp.sum(jnp.where(spot == lengths[j] - 1, value, 0.0), axis=0, keepdims=True)

    @pl.when(sec == pen)
    def _():
        for copy in kv_weights():
            copy.wait_recv()

        update = dot_nn(ctx[...].reshape(flat, qw), wout[...])
        wide_all = hin[...].reshape(flat, width).astype(F32) + update
        hnext[...] = wide_all.astype(BF16).reshape(seqs, length, width)
        rowf[...] = jnp.zeros_like(rowf)

        def next_norm(m, carry):
            wide = hnext[m].astype(F32)
            hbase[m] = (wide * rms_of(wide) * gain_next[...]).astype(BF16)
            rowf[...] = jnp.where(row8 == m, pick(wide, m), rowf[...])
            return carry

        lax.fori_loop(0, seqs, next_norm, 0)
        rown[...] = jnp.concatenate([rowf[...], rowf[...]], axis=0).astype(BF16)
        kv_all = dot_nn(hbase[...].reshape(flat, width), wkvn[...])
        for m in range(seqs):
            kvn[m] = rotate(
                kv_all[m * length : (m + 1) * length], cos_ref[:, qw:], sin_ref[:, qw:]
            ).astype(BF16)
        for copy in kv_up():
            copy.start()
        for m in range(seqs):
            h_last(m).start()

    def last_grad(m, wkv, gain_row, layer_in):
        here = spot == lengths[m] - 1
        mine = tail[0:8].astype(F32)
        query_part = jnp.sum(jnp.where(row8 == m, mine, 0.0), axis=0, keepdims=True)
        seed = jnp.sum(jnp.where(row8 == m + seqs, mine, 0.0), axis=0, keepdims=True)
        grad_n = dot_nt(gkv[m], wkv) + jnp.where(here, query_part, 0.0)
        grad_n = grad_n.astype(BF16).astype(F32) * gain_row
        wide = layer_in.astype(F32)
        scale = rms_of(wide)
        slope = scale * scale * scale * jnp.mean(wide * grad_n, axis=-1, keepdims=True)
        return (jnp.where(here, seed, 0.0) + grad_n * scale - wide * slope).astype(BF16)

    @pl.when(sec == last)
    def _():
        def gather_rows(parts):
            full = jnp.zeros((8, parts[0].shape[1]), F32)
            for j, row in enumerate(parts):
                full = jnp.where(row8 == j, row, full)
            return full

        def swap_half(head):
            return head // GROUP_HEADS != head % 2

        def half_mask(head, group_side):
            low = low_half((8, 128))
            upper_side = head // GROUP_HEADS if group_side else head % 2
            return low if upper_side == 0 else jnp.logical_not(low)

        def to_stack(rows):
            heads = []
            for head in range(HEADS):
                tile = rows[:, head // 2 * 128 : head // 2 * 128 + 128]
                if swap_half(head):
                    tile = pltpu.roll(tile, HEAD_DIM, 1)
                heads.append(jnp.where(half_mask(head, True), tile, 0.0))
            row16 = lax.broadcasted_iota(jnp.int32, (16, 128), 0)
            blocks_of = []
            for j in range(seqs):
                full = jnp.zeros((16, 128), F32)
                for head, tile in enumerate(heads):
                    full = jnp.where(row16 == head, tile[j : j + 1], full)
                blocks_of.append(full)
            return jnp.concatenate(blocks_of, axis=0).astype(BF16)

        def from_stack(stack):
            tiles = []
            for pair in range(HEADS // 2):
                halves = []
                for head in (2 * pair, 2 * pair + 1):
                    tile = gather_rows([stack[j * 16 + head : j * 16 + head + 1] for j in range(seqs)])
                    halves.append(pltpu.roll(tile, HEAD_DIM, 1) if swap_half(head) else tile)
                tiles.append(jnp.where(low_half((8, 128)), halves[0], halves[1]))
            return jnp.concatenate(tiles, axis=1)

        cos_row = gather_rows([pick(cos_ref[:, :qw], j) for j in range(seqs)])
        sin_row = gather_rows([pick(sin_ref[:, :qw], j) for j in range(seqs)])
        stacked_rows = lax.broadcasted_iota(jnp.int32, (16 * seqs, flat), 0) // 16
        key_at = lax.broadcasted_iota(jnp.int32, (16 * seqs, flat), 1)
        live = jnp.zeros((16 * seqs, flat), jnp.int32)
        for j in range(seqs):
            live = jnp.where(stacked_rows == j, j * length + lengths[j], live)
        live = jnp.logical_and(key_at >= stacked_rows * length, key_at < live)

        for copy in kv_up():
            copy.wait_recv()
        rows_in = rown[0:8].astype(F32)
        normed = (rows_in * rms_of(rows_in) * gain[...]).astype(BF16)
        query = rotate(dot_nn(normed, wqkv[:, :qw]), cos_row, sin_row).astype(BF16).astype(F32)
        keys = kvn[...].reshape(flat, 256)[:, :128]
        values = kvn[...].reshape(flat, 256)[:, 128:256]
        query_stack = to_stack(query)
        scores = dot_nt(query_stack, keys) * HEAD_DIM ** (-0.5)
        weights = jnp.where(live, jnp.exp(scores), 0.0)
        prob = weights / jnp.sum(weights, axis=-1, keepdims=True)
        prob_low = prob.astype(BF16)
        context = from_stack(dot_nn(prob_low, values)).astype(BF16)
        rows_out = (rows_in + dot_nn(context, wout[...])).astype(BF16).astype(F32)

        fgain = jnp.concatenate(
            [final_gain[i : i + 1] for i in range(final_gain.shape[0])], axis=1
        )
        row_part = lax.broadcasted_iota(jnp.int32, (16, part), 0)
        scale_out = rms_of(rows_out)
        pooled = rows_out * scale_out * fgain
        total_sq = jnp.sum(pooled * pooled, axis=-1, keepdims=True)
        size = lax.rsqrt(jnp.where(row8 < seqs, total_sq, 1.0))
        unit = pooled * size
        mine16 = jnp.zeros((16, part), F32)
        for j in range(seqs):
            for b in range(blocks):
                mine16 = jnp.where(
                    row_part == b * seqs + j, unit[j : j + 1, b * part : (b + 1) * part], mine16
                )
        emb_all[rep] = mine16.astype(BF16)
        marks = jnp.zeros((8, 128), jnp.int32)
        mark_row = lax.broadcasted_iota(jnp.int32, (8, 128), 0)
        for i in range(micro):
            marks = jnp.where(mark_row == i, positive[i], marks)
        pos_all[rep] = marks

        def exchange(step):
            to = peer(step)
            return [
                pltpu.make_async_remote_copy(
                    src_ref=buf.at[rep], dst_ref=buf.at[rep],
                    send_sem=send.at[step], recv_sem=recv.at[step],
                    device_id={"dp": to}, device_id_type=MESH,
                )
                for buf, send, recv in ((emb_all, e_send, e_recv), (pos_all, p_send, p_recv))
            ]

        copies = [exchange(step) for step in range(1, n_dp)]
        for pair in copies:
            for copy in pair:
                copy.start()
        for pair in copies:
            for copy in pair:
                copy.wait()

        total = n_dp * seqs
        tall = n_dp * 16
        everyone = emb_all[...].reshape(tall, part)
        pr = lax.broadcasted_iota(jnp.int32, (tall, tall), 0)
        pc = lax.broadcasted_iota(jnp.int32, (tall, tall), 1)
        in_block = lax.rem(pr, total)
        home = in_block // seqs * 16 + pr // total * seqs + lax.rem(in_block, seqs)
        sorted_rows = dot_nn((home == pc).astype(BF16), everyone).astype(BF16)
        every = jnp.concatenate(
            [sorted_rows[b * total : (b + 1) * total] for b in range(blocks)], axis=1
        )
        logits = SHARPNESS * dot_nt(every, every)
        qr = lax.broadcasted_iota(jnp.int32, (total, total), 0)
        dc = lax.broadcasted_iota(jnp.int32, (total, total), 1)
        doc = lax.rem(dc, 2) == 1
        weights = jnp.where(doc, jnp.exp(logits), 0.0)
        odds = weights / jnp.sum(weights, axis=-1, keepdims=True)
        marks_all = pos_all[...].reshape(n_dp * 8, 128).astype(F32)
        pr = lax.broadcasted_iota(jnp.int32, (total, n_dp * 8), 0)
        pc = lax.broadcasted_iota(jnp.int32, (total, n_dp * 8), 1)
        chosen = (pr // seqs * 8 + lax.rem(pr, seqs) // 2 == pc).astype(F32)
        target = dot_hi(chosen, marks_all)[:, :1]
        hit = jnp.logical_and(doc, (dc // 2).astype(F32) == target).astype(F32)
        coef = (odds - hit) * (COEF * SHARPNESS)
        coef = jnp.where(lax.rem(qr, 2) == 0, coef, 0.0)
        both = coef + coef.T
        own_coef = gather_rows([
            jnp.sum(jnp.where(qr == rep * seqs + j, both, 0.0), axis=0, keepdims=True)
            for j in range(seqs)
        ])
        grad_e = dot_hi(own_coef, every.astype(F32))
        grad_f = size * (grad_e - unit * jnp.sum(unit * grad_e, axis=-1, keepdims=True))
        grad_n = grad_f * fgain
        seeds = grad_n * scale_out - rows_out * (
            scale_out * scale_out * scale_out
            * jnp.mean(rows_out * grad_n, axis=-1, keepdims=True)
        )
        seed8 = jnp.where(row8 < seqs, seeds, 0.0).astype(BF16)
        grad_ctx = dot_nt(seed8, wout[...]).astype(BF16).astype(F32)
        upper = to_stack(grad_ctx)
        grad_p = dot_nt(upper, values).astype(BF16).astype(F32)
        grad_v = dot_tn(prob_low, upper)
        inner = jnp.sum(grad_p * prob, axis=-1, keepdims=True)
        grad_s = (prob * (grad_p - inner) * HEAD_DIM ** (-0.5)).astype(BF16)
        grad_k = dot_tn(grad_s, query_stack)
        grad_kv = jnp.concatenate([grad_k, grad_v], axis=1).astype(BF16).astype(F32)
        for j in range(seqs):
            gkv[j] = rotate(
                grad_kv[j * length : (j + 1) * length], cos_ref[:, qw:], -sin_ref[:, qw:]
            ).astype(BF16)
        for j in range(seqs):
            gkv_copy(j).start()
        grad_query = from_stack(dot_nn(grad_s, keys)).astype(BF16).astype(F32)
        grad_query = rotate(grad_query, cos_row, -sin_row).astype(BF16)
        query_part = dot_nt(grad_query, wqkv[:, :qw])
        seed_full = seed8.astype(F32)
        both_parts = query_part
        for j in range(seqs):
            both_parts = jnp.where(row8 == seqs + j, seed_full[j : j + 1], both_parts)
        tail[...] = jnp.concatenate([both_parts, both_parts], axis=0).astype(BF16)
        tail_copy().start()

        def own_grad(m, carry):
            h_last(m).wait_recv()
            out[m] = last_grad(m, wqkv[:, qw : qw + 256], gain[...], hbase[m])
            return carry

        lax.fori_loop(0, seqs, own_grad, 0)

    @pl.when(sec < last)
    def _():
        @pl.when(sec == pen)
        def _():
            tail_copy().wait_recv()

        def backward(m, carry):
            x = xs[m]
            keys = both_halves(x[:, qw : qw + 128])
            values = both_halves(x[:, qw + 128 : qw + 256])
            scale = rms_of(hin[m].astype(F32))
            gain_row = gain[...]

            @pl.when(sec == pen)
            def _():
                gkv_copy(m).wait_recv()
                first = last_grad(m, wkvn[...], gain_next[...], hnext[m])
                for c in range(cuts):
                    gin[m, c] = first[:, c * piece_width : (c + 1) * piece_width]

            grad_ctx = jnp.zeros((length, qw), F32)
            for c in range(cuts):
                @pl.when(sec < pen)
                def _():
                    g_copy(m, c).wait_recv()

                lanes = slice(c * piece_width, (c + 1) * piece_width)
                grad_ctx += dot_nt(gin[m, c], wout[:, lanes])
            grad_ctx = grad_ctx.astype(BF16)
            grad_q, grad_k, grad_v = [], [], []
            for group in range(KV_GROUPS):
                prob = probs[m, group]
                upper = stack_heads(grad_ctx, group)
                grad_p = dot_nt(upper, values[group]).astype(BF16).astype(F32)
                grad_v.append(dot_tn(prob.astype(BF16), upper))
                inner = jnp.sum(grad_p * prob, axis=-1, keepdims=True)
                grad_s = (prob * (grad_p - inner) * HEAD_DIM ** (-0.5)).astype(BF16)
                grad_q.append(dot_nn(grad_s, keys[group]))
                grad_k.append(dot_tn(grad_s, stack_heads(x, group)))
            grad_x = jnp.concatenate(
                [merge_heads(grad_q, length), fold_groups(grad_k), fold_groups(grad_v)], axis=1
            )
            grad_x = grad_x.astype(BF16).astype(F32)
            along = jnp.sum(grad_x * x.astype(F32), axis=-1, keepdims=True)
            slope = scale * scale * along * (1.0 / width)
            grad_x = rotate(grad_x, cos_ref[...], -sin_ref[...]).astype(BF16)
            for c in range(cuts):
                lanes = slice(c * piece_width, (c + 1) * piece_width)
                grad_n = dot_nt(grad_x, wqkv[lanes, :]).astype(BF16).astype(F32)
                grad_n = grad_n * gain_row[:, lanes]
                wide = hin[m, :, lanes].astype(F32)
                piece_grad = gin[m, c].astype(F32) + grad_n * scale - wide * slope
                piece_grad = piece_grad.astype(BF16)
                out[m, :, lanes] = piece_grad

                @pl.when(sec > 0)
                def _():
                    gout[m, c] = piece_grad
                    g_copy(m, c).start()

            return carry

        lax.fori_loop(0, seqs, backward, 0)

    @pl.when(sec < pen)
    def _():
        up(0).wait_send()
        up(1).wait_send()
        for m in range(seqs):
            ctx_copy(m).wait_send()

    @pl.when(jnp.logical_and(sec >= 1, sec < pen))
    def _():
        for m in range(seqs):
            h_copy(m).wait_send()

    @pl.when(inner_plane)
    def _():
        for m in range(seqs):
            for c in range(cuts):
                g_copy(m, c).wait_send()

    @pl.when(sec == pen)
    def _():
        for copy in kv_up():
            copy.wait_send()
        for m in range(seqs):
            h_last(m).wait_send()

    @pl.when(sec == last)
    def _():
        for copy in kv_weights():
            copy.wait_send()
        for m in range(seqs):
            gkv_copy(m).wait_send()
        tail_copy().wait_send()

    def settle(piece):
        for way in (0, 1):
            for slot in range(3):
                hop(piece, way, slot).wait_send()
        for way, slot in near + far:
            side(piece, way, slot).wait_send()

    settle(0)
    settle(1)

    @pl.when(inner_plane)
    def _():
        settle(2)


def tables(length, qw, columns):
    lane = np.arange(columns)
    half = HEAD_DIM // 2
    frequency = np.float32(ROPE_BASE) ** (
        -(lane % half).astype(np.float32) * np.float32(2.0 / HEAD_DIM)
    )
    angles = np.arange(length, dtype=np.float32)[:, None] * frequency[None, :]
    turned = (lane < columns - KV_GROUPS * HEAD_DIM)[None, :]
    sign = np.where(lane % HEAD_DIM < half, -1.0, 1.0)[None, :]
    cos = np.where(turned, np.cos(angles), 1.0).astype(np.float32)
    sin = np.where(turned, np.sin(angles) * sign, 0.0).astype(np.float32)
    return jnp.asarray(cos), jnp.asarray(sin)


def per_device(entry, norm_gain, w_qkv, w_out, final_gain, lengths, positive):
    n_sec = lax.axis_size("section")
    n_dp = lax.axis_size("dp")
    seqs = lengths.shape[0]
    rows, width = entry.shape
    length = rows // seqs
    qw = w_out.shape[1] * n_dp
    columns = w_qkv.shape[2]
    ring = w_qkv.shape[1] % 16 == 0 and w_out.shape[1] % 16 == 0 and n_dp % 4 == 0
    if ring:
        full_qkv, full_out = w_qkv[0], w_out[0]
    else:
        full_qkv = lax.all_gather(w_qkv, "dp", axis=1, tiled=True)[0]
        full_out = lax.all_gather(w_out, "dp", axis=1, tiled=True)[0]
    cos, sin = tables(length, qw, columns)
    vmem = pl.BlockSpec(memory_space=pltpu.VMEM)
    smem = pl.BlockSpec(memory_space=pltpu.SMEM)
    anywhere = pl.BlockSpec(memory_space=pl.ANY)
    part = width // (16 // seqs)
    dma = pltpu.SemaphoreType.DMA
    block = (seqs, length, width)
    if ring and n_dp // 2 == 4 and n_sec > 3:
        kv = columns - qw
        result = pl.pallas_call(
            functools.partial(swift, n_sec, n_dp, seqs, length),
            out_shape=jax.ShapeDtypeStruct(block, BF16),
            in_specs=[anywhere, vmem, anywhere, anywhere] + [vmem] * 3 + [smem] * 2,
            out_specs=vmem,
            scratch_shapes=[
                pltpu.VMEM(block, BF16),
                pltpu.VMEM(block, BF16),
                pltpu.VMEM(block, BF16),
                pltpu.VMEM((seqs, 4, length, width // 4), BF16),
                pltpu.VMEM((seqs, 4, length, width // 4), BF16),
                pltpu.VMEM((seqs, length, columns), F32),
                pltpu.VMEM((seqs, length, columns), BF16),
                pltpu.VMEM((seqs, KV_GROUPS, GROUP_HEADS * length, length), F32),
                pltpu.VMEM((seqs, length, qw), BF16),
                pltpu.VMEM((seqs, length, qw), BF16),
                pltpu.VMEM((width, columns), BF16),
                pltpu.VMEM((qw, width), BF16),
                pltpu.VMEM((qw, width), BF16),
                pltpu.VMEM((width, kv), BF16),
                pltpu.VMEM((1, width), F32),
                pltpu.VMEM((seqs, length, kv), BF16),
                pltpu.VMEM((8, width), F32),
                pltpu.VMEM((16, width), BF16),
                pltpu.VMEM((seqs, length, kv), BF16),
                pltpu.VMEM((16, width), BF16),
                pltpu.VMEM((n_dp, 16, part), BF16),
                pltpu.VMEM((n_dp, 8, 128), jnp.int32),
                dma((3, 2, 3)), dma((3, 2, 3)), dma((3, 3, 3)), dma((3, 3, 3)), dma((3,)),
                dma((2,)), dma((2,)),
                dma((seqs,)), dma((seqs,)), dma((seqs,)), dma((seqs,)),
                dma((seqs, 4)), dma((seqs, 4)), dma((2,)), dma((2,)),
                dma((2,)), dma((2,)), dma((seqs + 1,)), dma((seqs + 1,)),
                dma((n_dp,)), dma((n_dp,)), dma((n_dp,)), dma((n_dp,)),
            ],
            compiler_params=pltpu.CompilerParams(
                collective_id=0, has_side_effects=True, vmem_limit_bytes=60 * 1024 * 1024
            ),
        )(
            entry.reshape(block), norm_gain, w_qkv[0], w_out[0],
            final_gain.reshape(width // 128, 128), cos, sin, lengths, positive,
        )
        return result.reshape(1, rows, width)
    reach = n_dp // 4
    gathering = [
        pltpu.VMEM((width, columns), BF16),
        pltpu.VMEM((qw, width), BF16),
        pltpu.SemaphoreType.DMA((2, 2, reach)),
        pltpu.SemaphoreType.DMA((2, 2, reach)),
        pltpu.SemaphoreType.DMA((2, 2, reach + 1)),
        pltpu.SemaphoreType.DMA((2, 2, reach + 1)),
        pltpu.SemaphoreType.DMA((2,)),
    ] if ring else []
    result = pl.pallas_call(
        functools.partial(kernel, n_sec, n_dp, seqs, length, ring),
        out_shape=jax.ShapeDtypeStruct(block, BF16),
        in_specs=[vmem] * 7 + [smem] * 2,
        out_specs=vmem,
        scratch_shapes=[
            pltpu.VMEM(block, BF16),
            pltpu.VMEM(block, BF16),
            pltpu.VMEM(block, BF16),
            pltpu.VMEM((seqs, length, columns), BF16),
            pltpu.VMEM((seqs, KV_GROUPS, GROUP_HEADS * length, length), F32),
            pltpu.VMEM((seqs, 1, width), F32),
            pltpu.VMEM((n_dp, 16, part), BF16),
            pltpu.VMEM((n_dp, 8, 128), jnp.int32),
            pltpu.VMEM((seqs, length, qw), BF16),
            dma((seqs,)), dma((seqs,)), dma((seqs,)), dma((seqs,)),
            dma((n_dp,)), dma((n_dp,)), dma((n_dp,)), dma((n_dp,)),
            *gathering,
        ],
        compiler_params=pltpu.CompilerParams(
            collective_id=0, has_side_effects=True, vmem_limit_bytes=60 * 1024 * 1024
        ),
    )(
        entry.reshape(block), norm_gain, full_qkv, full_out, final_gain.reshape(1, width),
        cos, sin, lengths, positive,
    )
    return result.reshape(1, rows, width)


def solution(mesh):
    return jax.shard_map(
        per_device,
        mesh=mesh,
        in_specs=(
            P("dp", None),
            P("section", None),
            P("section", "dp", None),
            P("section", "dp", None),
            P(),
            P("dp"),
            P("dp"),
        ),
        out_specs=P("section", "dp", None),
        check_vma=False,
    )
```

```python
import functools

import jax
import jax.numpy as jnp
import numpy as np
from jax import lax
from jax.experimental import pallas as pl
from jax.experimental.pallas import tpu as pltpu
from jax.sharding import PartitionSpec as P

HEAD_DIM = 64
GROUP_HEADS = 7
KV_GROUPS = 2
HEADS = GROUP_HEADS * KV_GROUPS
ROPE_BASE = 1000000.0
EPS = 1e-06
SHARPNESS = 20.0
COEF = 256.0
MESH = pl.DeviceIdType.MESH
F32 = jnp.float32
BF16 = jnp.bfloat16
HI = lax.Precision.HIGHEST


def dot_nn(a, b):
    return lax.dot_general(a, b, (((1,), (0,)), ((), ())), preferred_element_type=F32)


def dot_nt(a, b):
    return lax.dot_general(a, b, (((1,), (1,)), ((), ())), preferred_element_type=F32)


def dot_tn(a, b):
    return lax.dot_general(a, b, (((0,), (0,)), ((), ())), preferred_element_type=F32)


def dot_hi(a, b):
    return lax.dot_general(
        a, b, (((1,), (0,)), ((), ())), preferred_element_type=F32, precision=HI
    )


def rotate(x, cos, sin_signed):
    width = x.shape[-1]
    lane = lax.broadcasted_iota(jnp.int32, x.shape, 1)
    first = lax.rem(lane, HEAD_DIM) < HEAD_DIM // 2
    ahead = pltpu.roll(x, width - HEAD_DIM // 2, 1)
    behind = pltpu.roll(x, HEAD_DIM // 2, 1)
    return x * cos + jnp.where(first, ahead, behind) * sin_signed


def low_half(shape):
    return lax.broadcasted_iota(jnp.int32, shape, 1) < HEAD_DIM


def both_halves(tile):
    wide = tile.astype(F32)
    turned = pltpu.roll(wide, HEAD_DIM, 1)
    low = low_half(wide.shape)
    return (
        jnp.where(low, wide, turned).astype(BF16),
        jnp.where(low, turned, wide).astype(BF16),
    )


def stack_heads(rows, group):
    parts = []
    for head in range(group * GROUP_HEADS, (group + 1) * GROUP_HEADS):
        tile = rows[:, head // 2 * 128 : head // 2 * 128 + 128].astype(F32)
        low = low_half(tile.shape)
        keep = low if head % 2 == 0 else jnp.logical_not(low)
        parts.append(jnp.where(keep, tile, 0.0).astype(BF16))
    return jnp.concatenate(parts, axis=0)


def merge_heads(stacks, length):
    tiles = []
    for pair in range(HEADS // 2):
        halves = []
        for head in (2 * pair, 2 * pair + 1):
            at = head % GROUP_HEADS * length
            halves.append(stacks[head // GROUP_HEADS][at : at + length])
        tiles.append(jnp.where(low_half(halves[0].shape), halves[0], halves[1]))
    return jnp.concatenate(tiles, axis=1)


def fold_groups(sums):
    full = [value + pltpu.roll(value, HEAD_DIM, 1) for value in sums]
    return jnp.where(low_half(full[0].shape), full[0], full[1])


def rms_of(wide):
    return lax.rsqrt(jnp.mean(wide * wide, axis=-1, keepdims=True) + EPS)


def kernel(
    n_sec, n_dp, seqs, length, ring,
    entry, gain, w_in, w_up, final_gain, cos_ref, sin_ref, lengths, positive,
    out,
    hin, hout, gin, xs, probs, rows_buf, emb_all, pos_all, contexts,
    f_send, f_recv, b_send, b_recv, e_send, e_recv, p_send, p_recv,
    *gathering,
):
    sec = lax.axis_index("section")
    rep = lax.axis_index("dp")
    last = n_sec - 1
    width = entry.shape[-1]
    wqkv, wout = gathering[:2] if ring else (w_in, w_up)
    qw = wout.shape[0]
    blocks = 16 // seqs
    part = width // blocks
    micro = seqs // 2

    barrier = pltpu.get_barrier_semaphore()

    def peer(step):
        return lax.rem(rep + step, n_dp)

    for near in (lax.rem(sec + 1, n_sec), lax.rem(sec + n_sec - 1, n_sec)):
        pl.semaphore_signal(barrier, inc=1, device_id={"section": near}, device_id_type=MESH)
    for step in range(1, n_dp):
        pl.semaphore_signal(barrier, inc=1, device_id={"dp": peer(step)}, device_id_type=MESH)
    pl.semaphore_wait(barrier, n_dp + 1)

    def forward_copy(m):
        return pltpu.make_async_remote_copy(
            src_ref=hout.at[m], dst_ref=hin.at[m], send_sem=f_send.at[m], recv_sem=f_recv.at[m],
            device_id={"section": sec + 1}, device_id_type=MESH,
        )

    def backward_copy(m):
        return pltpu.make_async_remote_copy(
            src_ref=out.at[m], dst_ref=gin.at[m], send_sem=b_send.at[m], recv_sem=b_recv.at[m],
            device_id={"section": sec - 1}, device_id_type=MESH,
        )

    @pl.when(sec == 0)
    def _():
        hin[...] = entry[...]

    def live_keys(m):
        keys = lax.broadcasted_iota(jnp.int32, (GROUP_HEADS * length, length), 1)
        return keys < lengths[m]

    def attend(m):
        wide = hin[m].astype(F32)
        normed = (wide * rms_of(wide) * gain[...]).astype(BF16)
        x = rotate(dot_nn(normed, wqkv[...]), cos_ref[...], sin_ref[...]).astype(BF16)
        xs[m] = x
        keys = both_halves(x[:, qw : qw + 128])
        values = both_halves(x[:, qw + 128 : qw + 256])
        live = live_keys(m)
        stacks = []
        for group in range(KV_GROUPS):
            scores = dot_nt(stack_heads(x, group), keys[group]) * HEAD_DIM ** (-0.5)
            weights = jnp.where(live, jnp.exp(scores), 0.0)
            prob = weights / jnp.sum(weights, axis=-1, keepdims=True)
            probs[m, group] = prob
            stacks.append(dot_nn(prob.astype(BF16), values[group]))
        contexts[m] = merge_heads(stacks, length).astype(BF16)

    if ring:
        hop_send, hop_recv, side_send, side_recv, keep_sem = gathering[2:]
        chips = n_dp // 2
        reach = chips // 2
        core = lax.rem(rep, 2)
        chip = rep // 2

        def place(c):
            return c + (c // 2) * (1 - 2 * lax.rem(c, 2)) if chips == 4 else c

        at = place(chip)
        pieces = ((w_in, wqkv), (w_up, wout))

        def region(piece, shard, half):
            held = pieces[piece][1]
            rows = pieces[piece][0].shape[0]
            cols = held.shape[1]
            cut = (cols // 128 + 1) // 2 * 128
            span = {None: (0, cols), 0: (0, cut), 1: (cut, cols - cut)}[half]
            start = pl.multiple_of(shard * rows, rows)
            return held.at[pl.ds(start, rows), pl.ds(*span)]

        def own(piece, half):
            mine, held = pieces[piece]
            if half is None:
                return mine
            cols = held.shape[1]
            cut = (cols // 128 + 1) // 2 * 128
            return mine.at[:, pl.ds(*((0, cut), (cut, cols - cut))[half])]

        def half_of(way, step):
            return way if step == reach else None

        def hop(piece, way, step):
            turn = 1 if way == 0 else chips - 1
            source = place(lax.rem(at + (step - 1) * (chips - turn), chips)) * 2 + core
            half = half_of(way, step)
            target = place(lax.rem(at + turn, chips)) * 2 + core
            dst = region(piece, source, half)
            return pltpu.make_async_remote_copy(
                src_ref=own(piece, half) if step == 1 else dst, dst_ref=dst,
                send_sem=hop_send.at[piece, way, step - 1],
                recv_sem=hop_recv.at[piece, way, step - 1],
                device_id={"dp": target}, device_id_type=MESH,
            )

        def side(piece, way, step):
            turn = 1 if way == 0 else chips - 1
            source = place(lax.rem(at + step * (chips - turn), chips)) * 2 + core
            half = half_of(way, step)
            dst = region(piece, source, half)
            return pltpu.make_async_remote_copy(
                src_ref=own(piece, None) if step == 0 else dst, dst_ref=dst,
                send_sem=side_send.at[piece, way, step],
                recv_sem=side_recv.at[piece, way, step],
                device_id={"dp": chip * 2 + 1 - core}, device_id_type=MESH,
            )

        def keep(piece):
            return pltpu.make_async_copy(
                own(piece, None), region(piece, rep, None), keep_sem.at[piece]
            )

        sides = [(0, 0)] + [(way, step) for step in range(1, reach + 1) for way in (0, 1)]

        def begin(piece):
            for way in (0, 1):
                hop(piece, way, 1).start()
            side(piece, 0, 0).start()
            keep(piece).start()

        def advance(piece, step):
            for way in (0, 1):
                hop(piece, way, step).wait_recv()
                if step < reach:
                    hop(piece, way, step + 1).start()
                side(piece, way, step).start()

        def finish(piece):
            advance(piece, reach)
            keep(piece).wait()
            for way, step in sides:
                side(piece, way, step).wait_recv()

        begin(0)
        for step in range(1, reach):
            advance(0, step)
        begin(1)
        finish(0)

    def early(m, carry):
        if ring:
            @pl.when(m == seqs // 2)
            def _():
                for step in range(1, reach):
                    advance(1, step)

        @pl.when(sec == 0)
        def _():
            attend(m)

        return carry

    lax.fori_loop(0, seqs, early, 0)
    if ring:
        finish(1)

    def forward(m, carry):
        @pl.when(sec > 0)
        def _():
            forward_copy(m).wait_recv()
            attend(m)

        hout[m] = (hin[m].astype(F32) + dot_nn(contexts[m], wout[...])).astype(BF16)

        @pl.when(sec < last)
        def _():
            forward_copy(m).start()

        return carry

    lax.fori_loop(0, seqs, forward, 0)

    @pl.when(sec == last)
    def _():
        fgain = final_gain[...]
        row16 = lax.broadcasted_iota(jnp.int32, (16, part), 0)
        position = lax.broadcasted_iota(jnp.int32, (length, width), 0)
        own = jnp.zeros((16, part), F32)
        for j in range(seqs):
            picked = jnp.where(position == lengths[j] - 1, hout[j].astype(F32), 0.0)
            row = jnp.sum(picked, axis=0, keepdims=True)
            rows_buf[j] = row
            pooled = row * rms_of(row) * fgain
            unit = pooled * lax.rsqrt(jnp.sum(pooled * pooled, axis=-1, keepdims=True))
            for b in range(blocks):
                own = jnp.where(row16 == b * seqs + j, unit[:, b * part : (b + 1) * part], own)
        emb_all[rep] = own.astype(BF16)
        marks = jnp.zeros((8, 128), jnp.int32)
        mark_row = lax.broadcasted_iota(jnp.int32, (8, 128), 0)
        for i in range(micro):
            marks = jnp.where(mark_row == i, positive[i], marks)
        pos_all[rep] = marks

        def exchange(step):
            to = peer(step)
            return [
                pltpu.make_async_remote_copy(
                    src_ref=buf.at[rep], dst_ref=buf.at[rep],
                    send_sem=send.at[step], recv_sem=recv.at[step],
                    device_id={"dp": to}, device_id_type=MESH,
                )
                for buf, send, recv in ((emb_all, e_send, e_recv), (pos_all, p_send, p_recv))
            ]

        copies = [exchange(step) for step in range(1, n_dp)]
        for pair in copies:
            for copy in pair:
                copy.start()
        for pair in copies:
            for copy in pair:
                copy.wait()

        total = n_dp * seqs
        tall = n_dp * 16
        everyone = emb_all[...].reshape(tall, part)
        cross = dot_nt(everyone, everyone)
        ra = lax.broadcasted_iota(jnp.int32, (tall, tall), 0)
        ca = lax.broadcasted_iota(jnp.int32, (tall, tall), 1)
        same = lax.rem(ra, 16) // seqs == lax.rem(ca, 16) // seqs
        cross = jnp.where(same, cross, 0.0)
        fr = lax.broadcasted_iota(jnp.int32, (total, tall), 0)
        fc = lax.broadcasted_iota(jnp.int32, (total, tall), 1)
        fold = (fc // 16 * seqs + lax.rem(fc, seqs) == fr).astype(F32)
        logits = SHARPNESS * lax.dot_general(
            dot_hi(fold, cross), fold, (((1,), (1,)), ((), ())),
            preferred_element_type=F32, precision=HI,
        )
        qr = lax.broadcasted_iota(jnp.int32, (total, total), 0)
        dc = lax.broadcasted_iota(jnp.int32, (total, total), 1)
        doc = lax.rem(dc, 2) == 1
        weights = jnp.where(doc, jnp.exp(logits), 0.0)
        odds = weights / jnp.sum(weights, axis=-1, keepdims=True)
        marks_all = pos_all[...].reshape(n_dp * 8, 128).astype(F32)
        pr = lax.broadcasted_iota(jnp.int32, (total, n_dp * 8), 0)
        pc = lax.broadcasted_iota(jnp.int32, (total, n_dp * 8), 1)
        pick = (pr // seqs * 8 + lax.rem(pr, seqs) // 2 == pc).astype(F32)
        target = dot_hi(pick, marks_all)[:, :1]
        hit = jnp.logical_and(doc, (dc // 2).astype(F32) == target).astype(F32)
        coef = (odds - hit) * (COEF * SHARPNESS)
        coef = jnp.where(lax.rem(qr, 2) == 0, coef, 0.0)
        both = coef + coef.T
        ar = lax.broadcasted_iota(jnp.int32, (16, total), 0)
        ac = lax.broadcasted_iota(jnp.int32, (16, total), 1)
        mine = (rep * seqs + lax.rem(ar, seqs) == ac).astype(F32)
        spread = dot_hi(dot_hi(mine, both), fold)
        br = lax.broadcasted_iota(jnp.int32, (16, tall), 0)
        bc = lax.broadcasted_iota(jnp.int32, (16, tall), 1)
        spread = jnp.where(br // seqs == lax.rem(bc, 16) // seqs, spread, 0.0)
        grad16 = dot_hi(spread, everyone.astype(F32))
        for j in range(seqs):
            grad_e = jnp.concatenate(
                [grad16[b * seqs + j : b * seqs + j + 1] for b in range(blocks)], axis=1
            )
            row = rows_buf[j]
            scale = rms_of(row)
            pooled = row * scale * fgain
            size = lax.rsqrt(jnp.sum(pooled * pooled, axis=-1, keepdims=True))
            unit = pooled * size
            grad_f = size * (grad_e - unit * jnp.sum(unit * grad_e, axis=-1, keepdims=True))
            grad_n = grad_f * fgain
            grad_r = grad_n * scale - row * (
                scale * scale * scale * jnp.mean(row * grad_n, axis=-1, keepdims=True)
            )
            gin[j] = jnp.where(position == lengths[j] - 1, grad_r, 0.0).astype(BF16)

    def backward(m, carry):
        @pl.when(sec < last)
        def _():
            backward_copy(m).wait_recv()

        grad = gin[m]
        x = xs[m]
        keys = both_halves(x[:, qw : qw + 128])
        values = both_halves(x[:, qw + 128 : qw + 256])
        grad_ctx = dot_nt(grad, wout[...]).astype(BF16)
        grad_q, grad_k, grad_v = [], [], []
        for group in range(KV_GROUPS):
            prob = probs[m, group]
            upper = stack_heads(grad_ctx, group)
            grad_p = dot_nt(upper, values[group]).astype(BF16).astype(F32)
            grad_v.append(dot_tn(prob.astype(BF16), upper))
            inner = jnp.sum(grad_p * prob, axis=-1, keepdims=True)
            grad_s = (prob * (grad_p - inner) * HEAD_DIM ** (-0.5)).astype(BF16)
            grad_q.append(dot_nn(grad_s, keys[group]))
            grad_k.append(dot_tn(grad_s, stack_heads(x, group)))
        grad_x = jnp.concatenate(
            [merge_heads(grad_q, length), fold_groups(grad_k), fold_groups(grad_v)], axis=1
        )
        grad_x = grad_x.astype(BF16).astype(F32)
        grad_x = rotate(grad_x, cos_ref[...], -sin_ref[...]).astype(BF16)
        grad_n = dot_nt(grad_x, wqkv[...]).astype(BF16).astype(F32) * gain[...]
        wide = hin[m].astype(F32)
        scale = rms_of(wide)
        slope = scale * scale * scale * jnp.mean(wide * grad_n, axis=-1, keepdims=True)
        out[m] = (grad.astype(F32) + grad_n * scale - wide * slope).astype(BF16)

        @pl.when(sec > 0)
        def _():
            backward_copy(m).start()

        return carry

    lax.fori_loop(0, seqs, backward, 0)

    @pl.when(sec < last)
    def _():
        for m in range(seqs):
            forward_copy(m).wait_send()

    @pl.when(sec > 0)
    def _():
        for m in range(seqs):
            backward_copy(m).wait_send()

    if ring:
        for piece in (0, 1):
            for way in (0, 1):
                for step in range(1, reach + 1):
                    hop(piece, way, step).wait_send()
            for way, step in sides:
                side(piece, way, step).wait_send()


def swift(
    n_sec, n_dp, seqs, length,
    entry, gain, w_in, w_up, final_gain, cos_ref, sin_ref, lengths, positive,
    out,
    hin, hbase, hnext, gin, gout, pre, xs, probs, ctx, ctxp, wqkv, wout, wprev, wkvn, gain_next,
    kvn, rowf, rown, gkv, tail, emb_all, pos_all,
    hop_send, hop_recv, side_send, side_recv, keep_sem, up_send, up_recv,
    c_send, c_recv, f_send, f_recv, b_send, b_recv, k_send, k_recv,
    v_send, v_recv, g_send, g_recv, e_send, e_recv, p_send, p_recv,
):
    sec = lax.axis_index("section")
    rep = lax.axis_index("dp")
    last = n_sec - 1
    pen = n_sec - 2
    width = entry.shape[-1]
    qw = wout.shape[0]
    blocks = 16 // seqs
    part = width // blocks
    micro = seqs // 2
    inner_plane = jnp.logical_and(sec >= 1, sec <= pen)

    barrier = pltpu.get_barrier_semaphore()

    def peer(step):
        return lax.rem(rep + step, n_dp)

    for near in (lax.rem(sec + 1, n_sec), lax.rem(sec + n_sec - 1, n_sec)):
        pl.semaphore_signal(barrier, inc=1, device_id={"section": near}, device_id_type=MESH)
    for step in range(1, n_dp):
        pl.semaphore_signal(barrier, inc=1, device_id={"dp": peer(step)}, device_id_type=MESH)
    pl.semaphore_wait(barrier, n_dp + 1)

    def to_section(src, dst, send, recv, turn):
        return pltpu.make_async_remote_copy(
            src_ref=src, dst_ref=dst, send_sem=send, recv_sem=recv,
            device_id={"section": sec + turn}, device_id_type=MESH,
        )

    core = lax.rem(rep, 2)
    chip = rep // 2
    chips = n_dp // 2

    def place(c):
        return c + (c // 2) * (1 - 2 * lax.rem(c, 2))

    at = place(chip)
    held = (wqkv, wout, wprev)
    shard_rows = (w_in.shape[0], w_up.shape[0], w_up.shape[0])

    def span(piece, half):
        cols = held[piece].shape[1]
        cut = (cols // 128 + 1) // 2 * 128
        return {None: (0, cols), 0: (0, cut), 1: (cut, cols - cut)}[half]

    def region(piece, shard, half):
        rows = shard_rows[piece]
        start = pl.multiple_of(shard * rows, rows)
        return held[piece].at[pl.ds(start, rows), pl.ds(*span(piece, half))]

    def own(piece, half):
        if piece == 2:
            return region(2, rep, half)
        return (w_in, w_up)[piece].at[:, pl.ds(*span(piece, half))]

    def source_of(way, step):
        turn = 1 if way == 0 else chips - 1
        return place(lax.rem(at + step * (chips - turn), chips)) * 2 + core

    def hop(piece, way, slot):
        turn = 1 if way == 0 else chips - 1
        target = place(lax.rem(at + turn, chips)) * 2 + core
        half = way if slot == 2 else slot
        dst = region(piece, rep if slot < 2 else source_of(way, 1), half)
        return pltpu.make_async_remote_copy(
            src_ref=own(piece, half) if slot < 2 else dst, dst_ref=dst,
            send_sem=hop_send.at[piece, way, slot], recv_sem=hop_recv.at[piece, way, slot],
            device_id={"dp": target}, device_id_type=MESH,
        )

    def hop_in(piece, way, slot):
        half = way if slot == 2 else slot
        dst = region(piece, source_of(way, 2 if slot == 2 else 1), half)
        return pltpu.make_async_remote_copy(
            src_ref=dst, dst_ref=dst,
            send_sem=hop_send.at[piece, way, slot], recv_sem=hop_recv.at[piece, way, slot],
            device_id={"dp": chip * 2 + 1 - core}, device_id_type=MESH,
        )

    def side(piece, way, slot):
        half = way if slot == 2 else slot
        shard = rep if way == 2 else source_of(way, 2 if slot == 2 else 1)
        dst = region(piece, shard, half)
        return pltpu.make_async_remote_copy(
            src_ref=own(piece, half) if way == 2 else dst, dst_ref=dst,
            send_sem=side_send.at[piece, way, slot], recv_sem=side_recv.at[piece, way, slot],
            device_id={"dp": chip * 2 + 1 - core}, device_id_type=MESH,
        )

    near = [(2, 0), (2, 1)] + [(way, slot) for slot in range(2) for way in (0, 1)]
    far = [(0, 2), (1, 2)]

    def keep(piece):
        return pltpu.make_async_copy(own(piece, None), region(piece, rep, None), keep_sem.at[piece])

    def take(piece, way, slot):
        hop_in(piece, way, slot).wait_recv()
        side(piece, way, slot).start()

    def hand_on(piece):
        take(piece, 0, 0)
        hop(piece, 0, 2).start()
        take(piece, 1, 1)
        hop(piece, 1, 2).start()

    def finish_near(piece):
        take(piece, 0, 1)
        take(piece, 1, 0)
        if piece < 2:
            keep(piece).wait()
        for way, slot in near:
            side(piece, way, slot).wait_recv()

    def finish_far(piece):
        for way, slot in far:
            take(piece, way, slot)
        for way, slot in far:
            side(piece, way, slot).wait_recv()

    def finish(piece):
        finish_near(piece)
        finish_far(piece)

    def entry_copy(dst):
        return pltpu.make_async_copy(entry, dst, keep_sem.at[2])

    def up(half):
        return to_section(own(1, half), region(2, rep, half), up_send.at[half], up_recv.at[half], 1)

    def ctx_copy(m):
        return to_section(ctx.at[m], ctxp.at[m], c_send.at[m], c_recv.at[m], 1)

    def h_copy(m):
        return to_section(hin.at[m], hbase.at[m], f_send.at[m], f_recv.at[m], 1)

    def h_last(m):
        return to_section(hnext.at[m], hbase.at[m], f_send.at[m], f_recv.at[m], 1)

    cuts = 4
    piece_width = width // cuts

    def g_copy(m, c):
        return to_section(gout.at[m, c], gin.at[m, c], b_send.at[m, c], b_recv.at[m, c], -1)

    def kv_weights():
        return (
            to_section(wqkv.at[:, pl.ds(qw, 256)], wkvn, k_send.at[0], k_recv.at[0], -1),
            to_section(gain, gain_next, k_send.at[1], k_recv.at[1], -1),
        )

    def top(buf):
        return buf.at[pl.ds(0, 8)]

    def kv_up():
        return (
            to_section(kvn, kvn, v_send.at[0], v_recv.at[0], 1),
            to_section(top(rown), top(rown), v_send.at[1], v_recv.at[1], 1),
        )

    def gkv_copy(m):
        return to_section(gkv.at[m], gkv.at[m], g_send.at[m], g_recv.at[m], -1)

    def tail_copy():
        return to_section(top(tail), top(tail), g_send.at[seqs], g_recv.at[seqs], -1)

    @pl.when(sec < pen)
    def _():
        up(0).start()
        up(1).start()

    for way in (0, 1):
        hop(0, way, way).start()
    for piece in (0, 1):
        keep(piece).start()
        side(piece, 2, 0).start()
        side(piece, 2, 1).start()

    @pl.when(jnp.logical_not(inner_plane))
    def _():
        for way in (0, 1):
            hop(0, way, 1 - way).start()

    @pl.when(sec == 0)
    def _():
        entry_copy(hin).start()

    @pl.when(sec == 1)
    def _():
        entry_copy(hbase).start()

    @pl.when(inner_plane)
    def _():
        for half in (0, 1):
            up(half).wait_recv()
            side(2, 2, half).start()
            for way in (0, 1):
                hop(2, way, half).start()
        hand_on(2)
        for way in (0, 1):
            hop(0, way, 1 - way).start()

    hand_on(0)
    for way in (0, 1):
        hop(1, way, way).start()
    for way in (0, 1):
        hop(1, way, 1 - way).start()

    def step_in(m):
        ctx_copy(m).wait_recv()

        @pl.when(sec > 1)
        def _():
            h_copy(m).wait_recv()

        hin[m] = (hbase[m].astype(F32) + dot_nn(ctxp[m], wprev[...])).astype(BF16)

    def normalise(m, carry):
        wide = hin[m].astype(F32)
        hnext[m] = (wide * rms_of(wide) * gain[...]).astype(BF16)
        return carry

    def chip_part(c):
        depth = 2 * w_in.shape[0]
        rows = pl.ds(pl.multiple_of(c * depth, depth), depth)
        left = hnext[:, :, rows].reshape(seqs * length, depth)
        return dot_nn(left, wqkv[rows, :]).reshape(seqs, length, wqkv.shape[1])

    @pl.when(sec == 0)
    def _():
        entry_copy(hin).wait()
        lax.fori_loop(0, seqs, normalise, 0)

    @pl.when(inner_plane)
    def _():
        finish(2)

    @pl.when(sec == 1)
    def _():
        entry_copy(hbase).wait()

        def ahead(m, carry):
            step_in(m)
            normalise(m, 0)

            @pl.when(jnp.logical_and(sec < pen, m < seqs - 1))
            def _():
                h_copy(m).start()

            return carry

        lax.fori_loop(0, seqs, ahead, 0)

    finish_near(0)

    @pl.when(sec <= 1)
    def _():
        pre[...] = chip_part(chip)

        def beside(step, carry):
            pre[...] += chip_part(place(lax.rem(at + 2 * step + 1, chips)))
            return carry

        lax.fori_loop(0, 2, beside, 0)

    finish_far(0)

    @pl.when(sec <= 1)
    def _():
        pre[...] += chip_part(place(lax.rem(at + 2, chips)))

    @pl.when(sec == last)
    def _():
        for copy in kv_weights():
            copy.start()

    @pl.when(sec == last)
    def _():
        hand_on(1)

    def live_keys(m, columns):
        return lax.broadcasted_iota(jnp.int32, (length, columns), 0) < lengths[m]

    def project(m):
        wide = hin[m].astype(F32)
        normed = (wide * rms_of(wide) * gain[...]).astype(BF16)
        pre[m] = dot_nn(normed, wqkv[...])

    def attend(m):
        x = rotate(pre[m], cos_ref[...], sin_ref[...]).astype(BF16)
        xs[m] = x
        keys = both_halves(x[:, qw : qw + 128])
        values = both_halves(x[:, qw + 128 : qw + 256])
        live = live_keys(m, GROUP_HEADS * length)
        stacks = []
        for group in range(KV_GROUPS):
            scores = dot_nt(keys[group], stack_heads(x, group)) * HEAD_DIM ** (-0.5)
            weights = jnp.where(live, jnp.exp(scores), 0.0)
            prob = weights / jnp.sum(weights, axis=0, keepdims=True)
            probs[m, group] = prob
            stacks.append(dot_tn(prob.astype(BF16), values[group]))
        ctx[m] = merge_heads(stacks, length).astype(BF16)

    @pl.when(sec < last)
    def _():
        def forward(m, carry):
            @pl.when(sec > 1)
            def _():
                step_in(m)

                @pl.when(sec < pen)
                def _():
                    h_copy(m).start()

                project(m)

                @pl.when(jnp.logical_and(sec == pen, m == seqs // 2))
                def _():
                    hand_on(1)

            attend(m)

            @pl.when(sec < pen)
            def _():
                ctx_copy(m).start()

                @pl.when(jnp.logical_and(sec == 1, m == seqs - 2))
                def _():
                    h_copy(seqs - 1).start()

            return carry

        lax.fori_loop(0, seqs, forward, 0)

    @pl.when(sec < pen)
    def _():
        hand_on(1)

    finish(1)

    flat = seqs * length
    row8 = lax.broadcasted_iota(jnp.int32, (8, 1), 0)
    spot = lax.broadcasted_iota(jnp.int32, (length, 1), 0)

    def pick(value, j):
        return jnp.sum(jnp.where(spot == lengths[j] - 1, value, 0.0), axis=0, keepdims=True)

    @pl.when(sec == pen)
    def _():
        for copy in kv_weights():
            copy.wait_recv()

        update = dot_nn(ctx[...].reshape(flat, qw), wout[...])
        wide_all = hin[...].reshape(flat, width).astype(F32) + update
        hnext[...] = wide_all.astype(BF16).reshape(seqs, length, width)
        rowf[...] = jnp.zeros_like(rowf)

        def next_norm(m, carry):
            wide = hnext[m].astype(F32)
            hbase[m] = (wide * rms_of(wide) * gain_next[...]).astype(BF16)
            rowf[...] = jnp.where(row8 == m, pick(wide, m), rowf[...])
            return carry

        lax.fori_loop(0, seqs, next_norm, 0)
        rown[...] = jnp.concatenate([rowf[...], rowf[...]], axis=0).astype(BF16)
        kv_all = dot_nn(hbase[...].reshape(flat, width), wkvn[...])
        for m in range(seqs):
            kvn[m] = rotate(
                kv_all[m * length : (m + 1) * length], cos_ref[:, qw:], sin_ref[:, qw:]
            ).astype(BF16)
        for copy in kv_up():
            copy.start()
        for m in range(seqs):
            h_last(m).start()

    def last_grad(m, wkv, gain_row, layer_in):
        here = spot == lengths[m] - 1
        mine = tail[0:8].astype(F32)
        query_part = jnp.sum(jnp.where(row8 == m, mine, 0.0), axis=0, keepdims=True)
        seed = jnp.sum(jnp.where(row8 == m + seqs, mine, 0.0), axis=0, keepdims=True)
        grad_n = dot_nt(gkv[m], wkv) + jnp.where(here, query_part, 0.0)
        grad_n = grad_n.astype(BF16).astype(F32) * gain_row
        wide = layer_in.astype(F32)
        scale = rms_of(wide)
        slope = scale * scale * scale * jnp.mean(wide * grad_n, axis=-1, keepdims=True)
        return (jnp.where(here, seed, 0.0) + grad_n * scale - wide * slope).astype(BF16)

    @pl.when(sec == last)
    def _():
        def gather_rows(parts):
            full = jnp.zeros((8, parts[0].shape[1]), F32)
            for j, row in enumerate(parts):
                full = jnp.where(row8 == j, row, full)
            return full

        def swap_half(head):
            return head // GROUP_HEADS != head % 2

        def half_mask(head, group_side):
            low = low_half((8, 128))
            upper_side = head // GROUP_HEADS if group_side else head % 2
            return low if upper_side == 0 else jnp.logical_not(low)

        def to_stack(rows):
            heads = []
            for head in range(HEADS):
                tile = rows[:, head // 2 * 128 : head // 2 * 128 + 128]
                if swap_half(head):
                    tile = pltpu.roll(tile, HEAD_DIM, 1)
                heads.append(jnp.where(half_mask(head, True), tile, 0.0))
            row16 = lax.broadcasted_iota(jnp.int32, (16, 128), 0)
            blocks_of = []
            for j in range(seqs):
                full = jnp.zeros((16, 128), F32)
                for head, tile in enumerate(heads):
                    full = jnp.where(row16 == head, tile[j : j + 1], full)
                blocks_of.append(full)
            return jnp.concatenate(blocks_of, axis=0).astype(BF16)

        def from_stack(stack):
            tiles = []
            for pair in range(HEADS // 2):
                halves = []
                for head in (2 * pair, 2 * pair + 1):
                    tile = gather_rows([stack[j * 16 + head : j * 16 + head + 1] for j in range(seqs)])
                    halves.append(pltpu.roll(tile, HEAD_DIM, 1) if swap_half(head) else tile)
                tiles.append(jnp.where(low_half((8, 128)), halves[0], halves[1]))
            return jnp.concatenate(tiles, axis=1)

        cos_row = gather_rows([pick(cos_ref[:, :qw], j) for j in range(seqs)])
        sin_row = gather_rows([pick(sin_ref[:, :qw], j) for j in range(seqs)])
        stacked_rows = lax.broadcasted_iota(jnp.int32, (16 * seqs, flat), 0) // 16
        key_at = lax.broadcasted_iota(jnp.int32, (16 * seqs, flat), 1)
        live = jnp.zeros((16 * seqs, flat), jnp.int32)
        for j in range(seqs):
            live = jnp.where(stacked_rows == j, j * length + lengths[j], live)
        live = jnp.logical_and(key_at >= stacked_rows * length, key_at < live)

        for copy in kv_up():
            copy.wait_recv()
        rows_in = rown[0:8].astype(F32)
        normed = (rows_in * rms_of(rows_in) * gain[...]).astype(BF16)
        query = rotate(dot_nn(normed, wqkv[:, :qw]), cos_row, sin_row).astype(BF16).astype(F32)
        keys = kvn[...].reshape(flat, 256)[:, :128]
        values = kvn[...].reshape(flat, 256)[:, 128:256]
        query_stack = to_stack(query)
        scores = dot_nt(query_stack, keys) * HEAD_DIM ** (-0.5)
        weights = jnp.where(live, jnp.exp(scores), 0.0)
        prob = weights / jnp.sum(weights, axis=-1, keepdims=True)
        prob_low = prob.astype(BF16)
        context = from_stack(dot_nn(prob_low, values)).astype(BF16)
        rows_out = (rows_in + dot_nn(context, wout[...])).astype(BF16).astype(F32)

        fgain = jnp.concatenate(
            [final_gain[i : i + 1] for i in range(final_gain.shape[0])], axis=1
        )
        row_part = lax.broadcasted_iota(jnp.int32, (16, part), 0)
        scale_out = rms_of(rows_out)
        pooled = rows_out * scale_out * fgain
        total_sq = jnp.sum(pooled * pooled, axis=-1, keepdims=True)
        size = lax.rsqrt(jnp.where(row8 < seqs, total_sq, 1.0))
        unit = pooled * size
        mine16 = jnp.zeros((16, part), F32)
        for j in range(seqs):
            for b in range(blocks):
                mine16 = jnp.where(
                    row_part == b * seqs + j, unit[j : j + 1, b * part : (b + 1) * part], mine16
                )
        emb_all[rep] = mine16.astype(BF16)
        marks = jnp.zeros((8, 128), jnp.int32)
        mark_row = lax.broadcasted_iota(jnp.int32, (8, 128), 0)
        for i in range(micro):
            marks = jnp.where(mark_row == i, positive[i], marks)
        pos_all[rep] = marks

        def exchange(step):
            to = peer(step)
            return [
                pltpu.make_async_remote_copy(
                    src_ref=buf.at[rep], dst_ref=buf.at[rep],
                    send_sem=send.at[step], recv_sem=recv.at[step],
                    device_id={"dp": to}, device_id_type=MESH,
                )
                for buf, send, recv in ((emb_all, e_send, e_recv), (pos_all, p_send, p_recv))
            ]

        copies = [exchange(step) for step in range(1, n_dp)]
        for pair in copies:
            for copy in pair:
                copy.start()
        for pair in copies:
            for copy in pair:
                copy.wait()

        total = n_dp * seqs
        tall = n_dp * 16
        everyone = emb_all[...].reshape(tall, part)
        pr = lax.broadcasted_iota(jnp.int32, (tall, tall), 0)
        pc = lax.broadcasted_iota(jnp.int32, (tall, tall), 1)
        in_block = lax.rem(pr, total)
        home = in_block // seqs * 16 + pr // total * seqs + lax.rem(in_block, seqs)
        sorted_rows = dot_nn((home == pc).astype(BF16), everyone).astype(BF16)
        every = jnp.concatenate(
            [sorted_rows[b * total : (b + 1) * total] for b in range(blocks)], axis=1
        )
        logits = SHARPNESS * dot_nt(every, every)
        qr = lax.broadcasted_iota(jnp.int32, (total, total), 0)
        dc = lax.broadcasted_iota(jnp.int32, (total, total), 1)
        doc = lax.rem(dc, 2) == 1
        weights = jnp.where(doc, jnp.exp(logits), 0.0)
        odds = weights / jnp.sum(weights, axis=-1, keepdims=True)
        marks_all = pos_all[...].reshape(n_dp * 8, 128).astype(F32)
        pr = lax.broadcasted_iota(jnp.int32, (total, n_dp * 8), 0)
        pc = lax.broadcasted_iota(jnp.int32, (total, n_dp * 8), 1)
        chosen = (pr // seqs * 8 + lax.rem(pr, seqs) // 2 == pc).astype(F32)
        target = dot_hi(chosen, marks_all)[:, :1]
        hit = jnp.logical_and(doc, (dc // 2).astype(F32) == target).astype(F32)
        coef = (odds - hit) * (COEF * SHARPNESS)
        coef = jnp.where(lax.rem(qr, 2) == 0, coef, 0.0)
        both = coef + coef.T
        own_coef = gather_rows([
            jnp.sum(jnp.where(qr == rep * seqs + j, both, 0.0), axis=0, keepdims=True)
            for j in range(seqs)
        ])
        grad_e = dot_hi(own_coef, every.astype(F32))
        grad_f = size * (grad_e - unit * jnp.sum(unit * grad_e, axis=-1, keepdims=True))
        grad_n = grad_f * fgain
        seeds = grad_n * scale_out - rows_out * (
            scale_out * scale_out * scale_out
            * jnp.mean(rows_out * grad_n, axis=-1, keepdims=True)
        )
        seed8 = jnp.where(row8 < seqs, seeds, 0.0).astype(BF16)
        grad_ctx = dot_nt(seed8, wout[...]).astype(BF16).astype(F32)
        upper = to_stack(grad_ctx)
        grad_p = dot_nt(upper, values).astype(BF16).astype(F32)
        grad_v = dot_tn(prob_low, upper)
        inner = jnp.sum(grad_p * prob, axis=-1, keepdims=True)
        grad_s = (prob * (grad_p - inner) * HEAD_DIM ** (-0.5)).astype(BF16)
        grad_k = dot_tn(grad_s, query_stack)
        grad_kv = jnp.concatenate([grad_k, grad_v], axis=1).astype(BF16).astype(F32)
        for j in range(seqs):
            gkv[j] = rotate(
                grad_kv[j * length : (j + 1) * length], cos_ref[:, qw:], -sin_ref[:, qw:]
            ).astype(BF16)
        for j in range(seqs):
            gkv_copy(j).start()
        grad_query = from_stack(dot_nn(grad_s, keys)).astype(BF16).astype(F32)
        grad_query = rotate(grad_query, cos_row, -sin_row).astype(BF16)
        query_part = dot_nt(grad_query, wqkv[:, :qw])
        seed_full = seed8.astype(F32)
        both_parts = query_part
        for j in range(seqs):
            both_parts = jnp.where(row8 == seqs + j, seed_full[j : j + 1], both_parts)
        tail[...] = jnp.concatenate([both_parts, both_parts], axis=0).astype(BF16)
        tail_copy().start()

        def own_grad(m, carry):
            h_last(m).wait_recv()
            out[m] = last_grad(m, wqkv[:, qw : qw + 256], gain[...], hbase[m])
            return carry

        lax.fori_loop(0, seqs, own_grad, 0)

    @pl.when(sec < last)
    def _():
        @pl.when(sec == pen)
        def _():
            tail_copy().wait_recv()

        def backward(m, carry):
            x = xs[m]
            keys = both_halves(x[:, qw : qw + 128])
            values = both_halves(x[:, qw + 128 : qw + 256])
            scale = rms_of(hin[m].astype(F32))
            gain_row = gain[...]

            @pl.when(sec == pen)
            def _():
                gkv_copy(m).wait_recv()
                first = last_grad(m, wkvn[...], gain_next[...], hnext[m])
                for c in range(cuts):
                    gin[m, c] = first[:, c * piece_width : (c + 1) * piece_width]

            grad_ctx = jnp.zeros((length, qw), F32)
            for c in range(cuts):
                @pl.when(sec < pen)
                def _():
                    g_copy(m, c).wait_recv()

                lanes = slice(c * piece_width, (c + 1) * piece_width)
                grad_ctx += dot_nt(gin[m, c], wout[:, lanes])
            grad_ctx = grad_ctx.astype(BF16)
            grad_q, grad_k, grad_v = [], [], []
            for group in range(KV_GROUPS):
                prob = probs[m, group]
                upper = stack_heads(grad_ctx, group)
                grad_p = dot_nt(values[group], upper).astype(BF16).astype(F32)
                grad_v.append(dot_nn(prob.astype(BF16), upper))
                inner = jnp.sum(grad_p * prob, axis=0, keepdims=True)
                grad_s = (prob * (grad_p - inner) * HEAD_DIM ** (-0.5)).astype(BF16)
                grad_q.append(dot_tn(grad_s, keys[group]))
                grad_k.append(dot_nn(grad_s, stack_heads(x, group)))
            grad_x = jnp.concatenate(
                [merge_heads(grad_q, length), fold_groups(grad_k), fold_groups(grad_v)], axis=1
            )
            grad_x = grad_x.astype(BF16).astype(F32)
            along = jnp.sum(grad_x * x.astype(F32), axis=-1, keepdims=True)
            slope = scale * scale * along * (1.0 / width)
            grad_x = rotate(grad_x, cos_ref[...], -sin_ref[...]).astype(BF16)
            for c in range(cuts):
                lanes = slice(c * piece_width, (c + 1) * piece_width)
                grad_n = dot_nt(grad_x, wqkv[lanes, :]).astype(BF16).astype(F32)
                grad_n = grad_n * gain_row[:, lanes]
                wide = hin[m, :, lanes].astype(F32)
                piece_grad = gin[m, c].astype(F32) + grad_n * scale - wide * slope
                piece_grad = piece_grad.astype(BF16)
                out[m, :, lanes] = piece_grad

                @pl.when(sec > 0)
                def _():
                    gout[m, c] = piece_grad
                    g_copy(m, c).start()

            return carry

        lax.fori_loop(0, seqs, backward, 0)

    @pl.when(sec < pen)
    def _():
        up(0).wait_send()
        up(1).wait_send()
        for m in range(seqs):
            ctx_copy(m).wait_send()

    @pl.when(jnp.logical_and(sec >= 1, sec < pen))
    def _():
        for m in range(seqs):
            h_copy(m).wait_send()

    @pl.when(inner_plane)
    def _():
        for m in range(seqs):
            for c in range(cuts):
                g_copy(m, c).wait_send()

    @pl.when(sec == pen)
    def _():
        for copy in kv_up():
            copy.wait_send()
        for m in range(seqs):
            h_last(m).wait_send()

    @pl.when(sec == last)
    def _():
        for copy in kv_weights():
            copy.wait_send()
        for m in range(seqs):
            gkv_copy(m).wait_send()
        tail_copy().wait_send()

    def settle(piece):
        for way in (0, 1):
            for slot in range(3):
                hop(piece, way, slot).wait_send()
        for way, slot in near + far:
            side(piece, way, slot).wait_send()

    settle(0)
    settle(1)

    @pl.when(inner_plane)
    def _():
        settle(2)


def tables(length, qw, columns):
    lane = np.arange(columns)
    half = HEAD_DIM // 2
    frequency = np.float32(ROPE_BASE) ** (
        -(lane % half).astype(np.float32) * np.float32(2.0 / HEAD_DIM)
    )
    angles = np.arange(length, dtype=np.float32)[:, None] * frequency[None, :]
    turned = (lane < columns - KV_GROUPS * HEAD_DIM)[None, :]
    sign = np.where(lane % HEAD_DIM < half, -1.0, 1.0)[None, :]
    cos = np.where(turned, np.cos(angles), 1.0).astype(np.float32)
    sin = np.where(turned, np.sin(angles) * sign, 0.0).astype(np.float32)
    return jnp.asarray(cos), jnp.asarray(sin)


def per_device(entry, norm_gain, w_qkv, w_out, final_gain, lengths, positive):
    n_sec = lax.axis_size("section")
    n_dp = lax.axis_size("dp")
    seqs = lengths.shape[0]
    rows, width = entry.shape
    length = rows // seqs
    qw = w_out.shape[1] * n_dp
    columns = w_qkv.shape[2]
    ring = w_qkv.shape[1] % 16 == 0 and w_out.shape[1] % 16 == 0 and n_dp % 4 == 0
    if ring:
        full_qkv, full_out = w_qkv[0], w_out[0]
    else:
        full_qkv = lax.all_gather(w_qkv, "dp", axis=1, tiled=True)[0]
        full_out = lax.all_gather(w_out, "dp", axis=1, tiled=True)[0]
    cos, sin = tables(length, qw, columns)
    vmem = pl.BlockSpec(memory_space=pltpu.VMEM)
    smem = pl.BlockSpec(memory_space=pltpu.SMEM)
    anywhere = pl.BlockSpec(memory_space=pl.ANY)
    part = width // (16 // seqs)
    dma = pltpu.SemaphoreType.DMA
    block = (seqs, length, width)
    if ring and n_dp // 2 == 4 and n_sec > 3:
        kv = columns - qw
        result = pl.pallas_call(
            functools.partial(swift, n_sec, n_dp, seqs, length),
            out_shape=jax.ShapeDtypeStruct(block, BF16),
            in_specs=[anywhere, vmem, anywhere, anywhere] + [vmem] * 3 + [smem] * 2,
            out_specs=vmem,
            scratch_shapes=[
                pltpu.VMEM(block, BF16),
                pltpu.VMEM(block, BF16),
                pltpu.VMEM(block, BF16),
                pltpu.VMEM((seqs, 4, length, width // 4), BF16),
                pltpu.VMEM((seqs, 4, length, width // 4), BF16),
                pltpu.VMEM((seqs, length, columns), F32),
                pltpu.VMEM((seqs, length, columns), BF16),
                pltpu.VMEM((seqs, KV_GROUPS, length, GROUP_HEADS * length), F32),
                pltpu.VMEM((seqs, length, qw), BF16),
                pltpu.VMEM((seqs, length, qw), BF16),
                pltpu.VMEM((width, columns), BF16),
                pltpu.VMEM((qw, width), BF16),
                pltpu.VMEM((qw, width), BF16),
                pltpu.VMEM((width, kv), BF16),
                pltpu.VMEM((1, width), F32),
                pltpu.VMEM((seqs, length, kv), BF16),
                pltpu.VMEM((8, width), F32),
                pltpu.VMEM((16, width), BF16),
                pltpu.VMEM((seqs, length, kv), BF16),
                pltpu.VMEM((16, width), BF16),
                pltpu.VMEM((n_dp, 16, part), BF16),
                pltpu.VMEM((n_dp, 8, 128), jnp.int32),
                dma((3, 2, 3)), dma((3, 2, 3)), dma((3, 3, 3)), dma((3, 3, 3)), dma((3,)),
                dma((2,)), dma((2,)),
                dma((seqs,)), dma((seqs,)), dma((seqs,)), dma((seqs,)),
                dma((seqs, 4)), dma((seqs, 4)), dma((2,)), dma((2,)),
                dma((2,)), dma((2,)), dma((seqs + 1,)), dma((seqs + 1,)),
                dma((n_dp,)), dma((n_dp,)), dma((n_dp,)), dma((n_dp,)),
            ],
            compiler_params=pltpu.CompilerParams(
                collective_id=0, has_side_effects=True, vmem_limit_bytes=60 * 1024 * 1024
            ),
        )(
            entry.reshape(block), norm_gain, w_qkv[0], w_out[0],
            final_gain.reshape(width // 128, 128), cos, sin, lengths, positive,
        )
        return result.reshape(1, rows, width)
    reach = n_dp // 4
    gathering = [
        pltpu.VMEM((width, columns), BF16),
        pltpu.VMEM((qw, width), BF16),
        pltpu.SemaphoreType.DMA((2, 2, reach)),
        pltpu.SemaphoreType.DMA((2, 2, reach)),
        pltpu.SemaphoreType.DMA((2, 2, reach + 1)),
        pltpu.SemaphoreType.DMA((2, 2, reach + 1)),
        pltpu.SemaphoreType.DMA((2,)),
    ] if ring else []
    result = pl.pallas_call(
        functools.partial(kernel, n_sec, n_dp, seqs, length, ring),
        out_shape=jax.ShapeDtypeStruct(block, BF16),
        in_specs=[vmem] * 7 + [smem] * 2,
        out_specs=vmem,
        scratch_shapes=[
            pltpu.VMEM(block, BF16),
            pltpu.VMEM(block, BF16),
            pltpu.VMEM(block, BF16),
            pltpu.VMEM((seqs, length, columns), BF16),
            pltpu.VMEM((seqs, KV_GROUPS, GROUP_HEADS * length, length), F32),
            pltpu.VMEM((seqs, 1, width), F32),
            pltpu.VMEM((n_dp, 16, part), BF16),
            pltpu.VMEM((n_dp, 8, 128), jnp.int32),
            pltpu.VMEM((seqs, length, qw), BF16),
            dma((seqs,)), dma((seqs,)), dma((seqs,)), dma((seqs,)),
            dma((n_dp,)), dma((n_dp,)), dma((n_dp,)), dma((n_dp,)),
            *gathering,
        ],
        compiler_params=pltpu.CompilerParams(
            collective_id=0, has_side_effects=True, vmem_limit_bytes=60 * 1024 * 1024
        ),
    )(
        entry.reshape(block), norm_gain, full_qkv, full_out, final_gain.reshape(1, width),
        cos, sin, lengths, positive,
    )
    return result.reshape(1, rows, width)


def solution(mesh):
    return jax.shard_map(
        per_device,
        mesh=mesh,
        in_specs=(
            P("dp", None),
            P("section", None),
            P("section", "dp", None),
            P("section", "dp", None),
            P(),
            P("dp"),
            P("dp"),
        ),
        out_specs=P("section", "dp", None),
        check_vma=False,
    )
```

```python
import functools

import jax
import jax.numpy as jnp
import numpy as np
from jax import lax
from jax.experimental import pallas as pl
from jax.experimental.pallas import tpu as pltpu
from jax.sharding import PartitionSpec as P

HEAD_DIM = 64
GROUP_HEADS = 7
KV_GROUPS = 2
HEADS = GROUP_HEADS * KV_GROUPS
ROPE_BASE = 1000000.0
EPS = 1e-06
SHARPNESS = 20.0
COEF = 256.0
MESH = pl.DeviceIdType.MESH
F32 = jnp.float32
BF16 = jnp.bfloat16
HI = lax.Precision.HIGHEST


def dot_nn(a, b):
    return lax.dot_general(a, b, (((1,), (0,)), ((), ())), preferred_element_type=F32)


def dot_nt(a, b):
    return lax.dot_general(a, b, (((1,), (1,)), ((), ())), preferred_element_type=F32)


def dot_tn(a, b):
    return lax.dot_general(a, b, (((0,), (0,)), ((), ())), preferred_element_type=F32)


def dot_hi(a, b):
    return lax.dot_general(
        a, b, (((1,), (0,)), ((), ())), preferred_element_type=F32, precision=HI
    )


def rotate(x, cos, sin_signed):
    width = x.shape[-1]
    lane = lax.broadcasted_iota(jnp.int32, x.shape, 1)
    first = lax.rem(lane, HEAD_DIM) < HEAD_DIM // 2
    ahead = pltpu.roll(x, width - HEAD_DIM // 2, 1)
    behind = pltpu.roll(x, HEAD_DIM // 2, 1)
    return x * cos + jnp.where(first, ahead, behind) * sin_signed


def low_half(shape):
    return lax.broadcasted_iota(jnp.int32, shape, 1) < HEAD_DIM


def both_halves(tile):
    wide = tile.astype(F32)
    turned = pltpu.roll(wide, HEAD_DIM, 1)
    low = low_half(wide.shape)
    return (
        jnp.where(low, wide, turned).astype(BF16),
        jnp.where(low, turned, wide).astype(BF16),
    )


def stack_heads(rows, group):
    parts = []
    for head in range(group * GROUP_HEADS, (group + 1) * GROUP_HEADS):
        tile = rows[:, head // 2 * 128 : head // 2 * 128 + 128].astype(F32)
        low = low_half(tile.shape)
        keep = low if head % 2 == 0 else jnp.logical_not(low)
        parts.append(jnp.where(keep, tile, 0.0).astype(BF16))
    return jnp.concatenate(parts, axis=0)


def merge_heads(stacks, length):
    tiles = []
    for pair in range(HEADS // 2):
        halves = []
        for head in (2 * pair, 2 * pair + 1):
            at = head % GROUP_HEADS * length
            halves.append(stacks[head // GROUP_HEADS][at : at + length])
        tiles.append(jnp.where(low_half(halves[0].shape), halves[0], halves[1]))
    return jnp.concatenate(tiles, axis=1)


def fold_groups(sums):
    full = [value + pltpu.roll(value, HEAD_DIM, 1) for value in sums]
    return jnp.where(low_half(full[0].shape), full[0], full[1])


def rms_of(wide):
    return lax.rsqrt(jnp.mean(wide * wide, axis=-1, keepdims=True) + EPS)


def kernel(
    n_sec, n_dp, seqs, length, ring,
    entry, gain, w_in, w_up, final_gain, cos_ref, sin_ref, lengths, positive,
    out,
    hin, hout, gin, xs, probs, rows_buf, emb_all, pos_all, contexts,
    f_send, f_recv, b_send, b_recv, e_send, e_recv, p_send, p_recv,
    *gathering,
):
    sec = lax.axis_index("section")
    rep = lax.axis_index("dp")
    last = n_sec - 1
    width = entry.shape[-1]
    wqkv, wout = gathering[:2] if ring else (w_in, w_up)
    qw = wout.shape[0]
    blocks = 16 // seqs
    part = width // blocks
    micro = seqs // 2

    barrier = pltpu.get_barrier_semaphore()

    def peer(step):
        return lax.rem(rep + step, n_dp)

    for near in (lax.rem(sec + 1, n_sec), lax.rem(sec + n_sec - 1, n_sec)):
        pl.semaphore_signal(barrier, inc=1, device_id={"section": near}, device_id_type=MESH)
    for step in range(1, n_dp):
        pl.semaphore_signal(barrier, inc=1, device_id={"dp": peer(step)}, device_id_type=MESH)
    pl.semaphore_wait(barrier, n_dp + 1)

    def forward_copy(m):
        return pltpu.make_async_remote_copy(
            src_ref=hout.at[m], dst_ref=hin.at[m], send_sem=f_send.at[m], recv_sem=f_recv.at[m],
            device_id={"section": sec + 1}, device_id_type=MESH,
        )

    def backward_copy(m):
        return pltpu.make_async_remote_copy(
            src_ref=out.at[m], dst_ref=gin.at[m], send_sem=b_send.at[m], recv_sem=b_recv.at[m],
            device_id={"section": sec - 1}, device_id_type=MESH,
        )

    @pl.when(sec == 0)
    def _():
        hin[...] = entry[...]

    def live_keys(m):
        keys = lax.broadcasted_iota(jnp.int32, (GROUP_HEADS * length, length), 1)
        return keys < lengths[m]

    def attend(m):
        wide = hin[m].astype(F32)
        normed = (wide * rms_of(wide) * gain[...]).astype(BF16)
        x = rotate(dot_nn(normed, wqkv[...]), cos_ref[...], sin_ref[...]).astype(BF16)
        xs[m] = x
        keys = both_halves(x[:, qw : qw + 128])
        values = both_halves(x[:, qw + 128 : qw + 256])
        live = live_keys(m)
        stacks = []
        for group in range(KV_GROUPS):
            scores = dot_nt(stack_heads(x, group), keys[group]) * HEAD_DIM ** (-0.5)
            weights = jnp.where(live, jnp.exp(scores), 0.0)
            prob = weights / jnp.sum(weights, axis=-1, keepdims=True)
            probs[m, group] = prob
            stacks.append(dot_nn(prob.astype(BF16), values[group]))
        contexts[m] = merge_heads(stacks, length).astype(BF16)

    if ring:
        hop_send, hop_recv, side_send, side_recv, keep_sem = gathering[2:]
        chips = n_dp // 2
        reach = chips // 2
        core = lax.rem(rep, 2)
        chip = rep // 2

        def place(c):
            return c + (c // 2) * (1 - 2 * lax.rem(c, 2)) if chips == 4 else c

        at = place(chip)
        pieces = ((w_in, wqkv), (w_up, wout))

        def region(piece, shard, half):
            held = pieces[piece][1]
            rows = pieces[piece][0].shape[0]
            cols = held.shape[1]
            cut = (cols // 128 + 1) // 2 * 128
            span = {None: (0, cols), 0: (0, cut), 1: (cut, cols - cut)}[half]
            start = pl.multiple_of(shard * rows, rows)
            return held.at[pl.ds(start, rows), pl.ds(*span)]

        def own(piece, half):
            mine, held = pieces[piece]
            if half is None:
                return mine
            cols = held.shape[1]
            cut = (cols // 128 + 1) // 2 * 128
            return mine.at[:, pl.ds(*((0, cut), (cut, cols - cut))[half])]

        def half_of(way, step):
            return way if step == reach else None

        def hop(piece, way, step):
            turn = 1 if way == 0 else chips - 1
            source = place(lax.rem(at + (step - 1) * (chips - turn), chips)) * 2 + core
            half = half_of(way, step)
            target = place(lax.rem(at + turn, chips)) * 2 + core
            dst = region(piece, source, half)
            return pltpu.make_async_remote_copy(
                src_ref=own(piece, half) if step == 1 else dst, dst_ref=dst,
                send_sem=hop_send.at[piece, way, step - 1],
                recv_sem=hop_recv.at[piece, way, step - 1],
                device_id={"dp": target}, device_id_type=MESH,
            )

        def side(piece, way, step):
            turn = 1 if way == 0 else chips - 1
            source = place(lax.rem(at + step * (chips - turn), chips)) * 2 + core
            half = half_of(way, step)
            dst = region(piece, source, half)
            return pltpu.make_async_remote_copy(
                src_ref=own(piece, None) if step == 0 else dst, dst_ref=dst,
                send_sem=side_send.at[piece, way, step],
                recv_sem=side_recv.at[piece, way, step],
                device_id={"dp": chip * 2 + 1 - core}, device_id_type=MESH,
            )

        def keep(piece):
            return pltpu.make_async_copy(
                own(piece, None), region(piece, rep, None), keep_sem.at[piece]
            )

        sides = [(0, 0)] + [(way, step) for step in range(1, reach + 1) for way in (0, 1)]

        def begin(piece):
            for way in (0, 1):
                hop(piece, way, 1).start()
            side(piece, 0, 0).start()
            keep(piece).start()

        def advance(piece, step):
            for way in (0, 1):
                hop(piece, way, step).wait_recv()
                if step < reach:
                    hop(piece, way, step + 1).start()
                side(piece, way, step).start()

        def finish(piece):
            advance(piece, reach)
            keep(piece).wait()
            for way, step in sides:
                side(piece, way, step).wait_recv()

        begin(0)
        for step in range(1, reach):
            advance(0, step)
        begin(1)
        finish(0)

    def early(m, carry):
        if ring:
            @pl.when(m == seqs // 2)
            def _():
                for step in range(1, reach):
                    advance(1, step)

        @pl.when(sec == 0)
        def _():
            attend(m)

        return carry

    lax.fori_loop(0, seqs, early, 0)
    if ring:
        finish(1)

    def forward(m, carry):
        @pl.when(sec > 0)
        def _():
            forward_copy(m).wait_recv()
            attend(m)

        hout[m] = (hin[m].astype(F32) + dot_nn(contexts[m], wout[...])).astype(BF16)

        @pl.when(sec < last)
        def _():
            forward_copy(m).start()

        return carry

    lax.fori_loop(0, seqs, forward, 0)

    @pl.when(sec == last)
    def _():
        fgain = final_gain[...]
        row16 = lax.broadcasted_iota(jnp.int32, (16, part), 0)
        position = lax.broadcasted_iota(jnp.int32, (length, width), 0)
        own = jnp.zeros((16, part), F32)
        for j in range(seqs):
            picked = jnp.where(position == lengths[j] - 1, hout[j].astype(F32), 0.0)
            row = jnp.sum(picked, axis=0, keepdims=True)
            rows_buf[j] = row
            pooled = row * rms_of(row) * fgain
            unit = pooled * lax.rsqrt(jnp.sum(pooled * pooled, axis=-1, keepdims=True))
            for b in range(blocks):
                own = jnp.where(row16 == b * seqs + j, unit[:, b * part : (b + 1) * part], own)
        emb_all[rep] = own.astype(BF16)
        marks = jnp.zeros((8, 128), jnp.int32)
        mark_row = lax.broadcasted_iota(jnp.int32, (8, 128), 0)
        for i in range(micro):
            marks = jnp.where(mark_row == i, positive[i], marks)
        pos_all[rep] = marks

        def exchange(step):
            to = peer(step)
            return [
                pltpu.make_async_remote_copy(
                    src_ref=buf.at[rep], dst_ref=buf.at[rep],
                    send_sem=send.at[step], recv_sem=recv.at[step],
                    device_id={"dp": to}, device_id_type=MESH,
                )
                for buf, send, recv in ((emb_all, e_send, e_recv), (pos_all, p_send, p_recv))
            ]

        copies = [exchange(step) for step in range(1, n_dp)]
        for pair in copies:
            for copy in pair:
                copy.start()
        for pair in copies:
            for copy in pair:
                copy.wait()

        total = n_dp * seqs
        tall = n_dp * 16
        everyone = emb_all[...].reshape(tall, part)
        cross = dot_nt(everyone, everyone)
        ra = lax.broadcasted_iota(jnp.int32, (tall, tall), 0)
        ca = lax.broadcasted_iota(jnp.int32, (tall, tall), 1)
        same = lax.rem(ra, 16) // seqs == lax.rem(ca, 16) // seqs
        cross = jnp.where(same, cross, 0.0)
        fr = lax.broadcasted_iota(jnp.int32, (total, tall), 0)
        fc = lax.broadcasted_iota(jnp.int32, (total, tall), 1)
        fold = (fc // 16 * seqs + lax.rem(fc, seqs) == fr).astype(F32)
        logits = SHARPNESS * lax.dot_general(
            dot_hi(fold, cross), fold, (((1,), (1,)), ((), ())),
            preferred_element_type=F32, precision=HI,
        )
        qr = lax.broadcasted_iota(jnp.int32, (total, total), 0)
        dc = lax.broadcasted_iota(jnp.int32, (total, total), 1)
        doc = lax.rem(dc, 2) == 1
        weights = jnp.where(doc, jnp.exp(logits), 0.0)
        odds = weights / jnp.sum(weights, axis=-1, keepdims=True)
        marks_all = pos_all[...].reshape(n_dp * 8, 128).astype(F32)
        pr = lax.broadcasted_iota(jnp.int32, (total, n_dp * 8), 0)
        pc = lax.broadcasted_iota(jnp.int32, (total, n_dp * 8), 1)
        pick = (pr // seqs * 8 + lax.rem(pr, seqs) // 2 == pc).astype(F32)
        target = dot_hi(pick, marks_all)[:, :1]
        hit = jnp.logical_and(doc, (dc // 2).astype(F32) == target).astype(F32)
        coef = (odds - hit) * (COEF * SHARPNESS)
        coef = jnp.where(lax.rem(qr, 2) == 0, coef, 0.0)
        both = coef + coef.T
        ar = lax.broadcasted_iota(jnp.int32, (16, total), 0)
        ac = lax.broadcasted_iota(jnp.int32, (16, total), 1)
        mine = (rep * seqs + lax.rem(ar, seqs) == ac).astype(F32)
        spread = dot_hi(dot_hi(mine, both), fold)
        br = lax.broadcasted_iota(jnp.int32, (16, tall), 0)
        bc = lax.broadcasted_iota(jnp.int32, (16, tall), 1)
        spread = jnp.where(br // seqs == lax.rem(bc, 16) // seqs, spread, 0.0)
        grad16 = dot_hi(spread, everyone.astype(F32))
        for j in range(seqs):
            grad_e = jnp.concatenate(
                [grad16[b * seqs + j : b * seqs + j + 1] for b in range(blocks)], axis=1
            )
            row = rows_buf[j]
            scale = rms_of(row)
            pooled = row * scale * fgain
            size = lax.rsqrt(jnp.sum(pooled * pooled, axis=-1, keepdims=True))
            unit = pooled * size
            grad_f = size * (grad_e - unit * jnp.sum(unit * grad_e, axis=-1, keepdims=True))
            grad_n = grad_f * fgain
            grad_r = grad_n * scale - row * (
                scale * scale * scale * jnp.mean(row * grad_n, axis=-1, keepdims=True)
            )
            gin[j] = jnp.where(position == lengths[j] - 1, grad_r, 0.0).astype(BF16)

    def backward(m, carry):
        @pl.when(sec < last)
        def _():
            backward_copy(m).wait_recv()

        grad = gin[m]
        x = xs[m]
        keys = both_halves(x[:, qw : qw + 128])
        values = both_halves(x[:, qw + 128 : qw + 256])
        grad_ctx = dot_nt(grad, wout[...]).astype(BF16)
        grad_q, grad_k, grad_v = [], [], []
        for group in range(KV_GROUPS):
            prob = probs[m, group]
            upper = stack_heads(grad_ctx, group)
            grad_p = dot_nt(upper, values[group]).astype(BF16).astype(F32)
            grad_v.append(dot_tn(prob.astype(BF16), upper))
            inner = jnp.sum(grad_p * prob, axis=-1, keepdims=True)
            grad_s = (prob * (grad_p - inner) * HEAD_DIM ** (-0.5)).astype(BF16)
            grad_q.append(dot_nn(grad_s, keys[group]))
            grad_k.append(dot_tn(grad_s, stack_heads(x, group)))
        grad_x = jnp.concatenate(
            [merge_heads(grad_q, length), fold_groups(grad_k), fold_groups(grad_v)], axis=1
        )
        grad_x = grad_x.astype(BF16).astype(F32)
        grad_x = rotate(grad_x, cos_ref[...], -sin_ref[...]).astype(BF16)
        grad_n = dot_nt(grad_x, wqkv[...]).astype(BF16).astype(F32) * gain[...]
        wide = hin[m].astype(F32)
        scale = rms_of(wide)
        slope = scale * scale * scale * jnp.mean(wide * grad_n, axis=-1, keepdims=True)
        out[m] = (grad.astype(F32) + grad_n * scale - wide * slope).astype(BF16)

        @pl.when(sec > 0)
        def _():
            backward_copy(m).start()

        return carry

    lax.fori_loop(0, seqs, backward, 0)

    @pl.when(sec < last)
    def _():
        for m in range(seqs):
            forward_copy(m).wait_send()

    @pl.when(sec > 0)
    def _():
        for m in range(seqs):
            backward_copy(m).wait_send()

    if ring:
        for piece in (0, 1):
            for way in (0, 1):
                for step in range(1, reach + 1):
                    hop(piece, way, step).wait_send()
            for way, step in sides:
                side(piece, way, step).wait_send()


def swift(
    n_sec, n_dp, seqs, length,
    entry, gain, w_in, w_up, final_gain, cos_ref, sin_ref, lengths, positive,
    out,
    hin, hbase, hnext, gin, gout, pre, xs, probs, ctx, ctxp, wqkv, wout, wprev, wkvn, wqkv_t, wout_t, wkvn_t, gain_next,
    kvn, rowf, rown, gkv, tail, emb_all, pos_all,
    hop_send, hop_recv, side_send, side_recv, keep_sem, up_send, up_recv,
    c_send, c_recv, f_send, f_recv, b_send, b_recv, k_send, k_recv,
    v_send, v_recv, g_send, g_recv, d_send, d_recv, e_send, e_recv, p_send, p_recv,
):
    sec = lax.axis_index("section")
    rep = lax.axis_index("dp")
    last = n_sec - 1
    pen = n_sec - 2
    width = entry.shape[-1]
    qw = wout.shape[0]
    blocks = 16 // seqs
    part = width // blocks
    micro = seqs // 2
    inner_plane = jnp.logical_and(sec >= 1, sec <= pen)

    barrier = pltpu.get_barrier_semaphore()

    def peer(step):
        return lax.rem(rep + step, n_dp)

    for near in (lax.rem(sec + 1, n_sec), lax.rem(sec + n_sec - 1, n_sec)):
        pl.semaphore_signal(barrier, inc=1, device_id={"section": near}, device_id_type=MESH)
    for step in range(1, n_dp):
        pl.semaphore_signal(barrier, inc=1, device_id={"dp": peer(step)}, device_id_type=MESH)
    pl.semaphore_wait(barrier, n_dp + 1)

    def to_section(src, dst, send, recv, turn):
        return pltpu.make_async_remote_copy(
            src_ref=src, dst_ref=dst, send_sem=send, recv_sem=recv,
            device_id={"section": sec + turn}, device_id_type=MESH,
        )

    core = lax.rem(rep, 2)
    chip = rep // 2
    chips = n_dp // 2

    def place(c):
        return c + (c // 2) * (1 - 2 * lax.rem(c, 2))

    at = place(chip)
    held = (wqkv, wout, wprev)
    shard_rows = (w_in.shape[0], w_up.shape[0], w_up.shape[0])

    def span(piece, half):
        cols = held[piece].shape[1]
        cut = (cols // 128 + 1) // 2 * 128
        return {None: (0, cols), 0: (0, cut), 1: (cut, cols - cut)}[half]

    def region(piece, shard, half):
        rows = shard_rows[piece]
        start = pl.multiple_of(shard * rows, rows)
        return held[piece].at[pl.ds(start, rows), pl.ds(*span(piece, half))]

    def own(piece, half):
        if piece == 2:
            return region(2, rep, half)
        return (w_in, w_up)[piece].at[:, pl.ds(*span(piece, half))]

    def source_of(way, step):
        turn = 1 if way == 0 else chips - 1
        return place(lax.rem(at + step * (chips - turn), chips)) * 2 + core

    def hop(piece, way, slot):
        turn = 1 if way == 0 else chips - 1
        target = place(lax.rem(at + turn, chips)) * 2 + core
        half = way if slot == 2 else slot
        dst = region(piece, rep if slot < 2 else source_of(way, 1), half)
        return pltpu.make_async_remote_copy(
            src_ref=own(piece, half) if slot < 2 else dst, dst_ref=dst,
            send_sem=hop_send.at[piece, way, slot], recv_sem=hop_recv.at[piece, way, slot],
            device_id={"dp": target}, device_id_type=MESH,
        )

    def hop_in(piece, way, slot):
        half = way if slot == 2 else slot
        dst = region(piece, source_of(way, 2 if slot == 2 else 1), half)
        return pltpu.make_async_remote_copy(
            src_ref=dst, dst_ref=dst,
            send_sem=hop_send.at[piece, way, slot], recv_sem=hop_recv.at[piece, way, slot],
            device_id={"dp": chip * 2 + 1 - core}, device_id_type=MESH,
        )

    def side(piece, way, slot):
        half = way if slot == 2 else slot
        shard = rep if way == 2 else source_of(way, 2 if slot == 2 else 1)
        dst = region(piece, shard, half)
        return pltpu.make_async_remote_copy(
            src_ref=own(piece, half) if way == 2 else dst, dst_ref=dst,
            send_sem=side_send.at[piece, way, slot], recv_sem=side_recv.at[piece, way, slot],
            device_id={"dp": chip * 2 + 1 - core}, device_id_type=MESH,
        )

    near = [(2, 0), (2, 1)] + [(way, slot) for slot in range(2) for way in (0, 1)]
    far = [(0, 2), (1, 2)]

    def keep(piece):
        return pltpu.make_async_copy(own(piece, None), region(piece, rep, None), keep_sem.at[piece])

    def take(piece, way, slot):
        hop_in(piece, way, slot).wait_recv()
        side(piece, way, slot).start()

    def hand_on(piece):
        take(piece, 0, 0)
        hop(piece, 0, 2).start()
        take(piece, 1, 1)
        hop(piece, 1, 2).start()

    def finish_near(piece):
        take(piece, 0, 1)
        take(piece, 1, 0)
        if piece < 2:
            keep(piece).wait()
        for way, slot in near:
            side(piece, way, slot).wait_recv()

    def finish_far(piece):
        for way, slot in far:
            take(piece, way, slot)
        for way, slot in far:
            side(piece, way, slot).wait_recv()

    def finish(piece):
        finish_near(piece)
        finish_far(piece)

    def entry_copy(dst):
        return pltpu.make_async_copy(entry, dst, keep_sem.at[2])

    def up(half):
        return to_section(own(1, half), region(2, rep, half), up_send.at[half], up_recv.at[half], 1)

    lent = span(1, 0)[1] // 2

    def lend():
        return to_section(own(1, 1), region(2, rep, 0), up_send.at[0], up_recv.at[0], 1)

    def quarter(held_ref, shard, which):
        start = pl.multiple_of(shard * w_up.shape[0], w_up.shape[0])
        return held_ref.at[pl.ds(start, w_up.shape[0]), pl.ds(which * lent, lent)]

    def narrow(held_ref, piece, way, slot):
        turn = 1 if way == 0 else chips - 1
        target = place(lax.rem(at + turn, chips)) * 2 + core
        part_of = quarter(held_ref, rep if slot < 2 else source_of(way, 1), way if slot == 2 else slot)
        return pltpu.make_async_remote_copy(
            src_ref=part_of, dst_ref=part_of,
            send_sem=hop_send.at[piece, way, slot], recv_sem=hop_recv.at[piece, way, slot],
            device_id={"dp": target}, device_id_type=MESH,
        )

    def give_back(which):
        shard = source_of(0, 2) if which == 2 else source_of(which, 1)
        return to_section(
            region(2, shard, 0), region(1, shard, 1), d_send.at[which], d_recv.at[which], -1
        )

    def ctx_copy(m):
        return to_section(ctx.at[m], ctxp.at[m], c_send.at[m], c_recv.at[m], 1)

    def h_copy(m):
        return to_section(hin.at[m], hbase.at[m], f_send.at[m], f_recv.at[m], 1)

    def h_last(m):
        return to_section(hnext.at[m], hbase.at[m], f_send.at[m], f_recv.at[m], 1)

    cuts = 4
    piece_width = width // cuts

    def g_copy(m, c):
        return to_section(gout.at[m, c], gin.at[m, c], b_send.at[m, c], b_recv.at[m, c], -1)

    kv_rows = pl.ds(pl.multiple_of(core * (width // 2), width // 2), width // 2)

    def kv_half():
        return to_section(
            wqkv.at[kv_rows, pl.ds(qw, 256)], wkvn.at[kv_rows], k_send.at[0], k_recv.at[0], -1
        )

    def kv_side():
        return pltpu.make_async_remote_copy(
            src_ref=wkvn.at[kv_rows], dst_ref=wkvn.at[kv_rows],
            send_sem=k_send.at[2], recv_sem=k_recv.at[2],
            device_id={"dp": chip * 2 + 1 - core}, device_id_type=MESH,
        )

    def gain_down():
        return to_section(gain, gain_next, k_send.at[1], k_recv.at[1], -1)

    def top(buf):
        return buf.at[pl.ds(0, 8)]

    def kv_up():
        return (
            to_section(kvn, kvn, v_send.at[0], v_recv.at[0], 1),
            to_section(top(rown), top(rown), v_send.at[1], v_recv.at[1], 1),
        )

    def gkv_copy(m):
        return to_section(gkv.at[m], gkv.at[m], g_send.at[m], g_recv.at[m], -1)

    def tail_copy():
        return to_section(top(tail), top(tail), g_send.at[seqs], g_recv.at[seqs], -1)

    @pl.when(sec < pen)
    def _():
        up(0).start()
        up(1).start()

    @pl.when(sec == pen)
    def _():
        lend().start()

    @pl.when(sec == last)
    def _():
        gain_down().start()

    for way in (0, 1):
        hop(0, way, way).start()
    for piece in (0, 1):
        keep(piece).start()
        side(piece, 2, 0).start()
        side(piece, 2, 1).start()

    @pl.when(sec == 0)
    def _():
        for way in (0, 1):
            hop(0, way, 1 - way).start()

    @pl.when(sec == last)
    def _():
        lend().wait_recv()
        for slot in (0, 1):
            for way in (0, 1):
                narrow(wprev, 2, way, slot).start()
        narrow(wprev, 2, 0, 0).wait_recv()
        narrow(wprev, 2, 0, 2).start()
        narrow(wprev, 2, 1, 1).wait_recv()
        narrow(wprev, 2, 1, 2).start()
        for way in (0, 1):
            hop(0, way, 1 - way).start()
        for way in (0, 1):
            narrow(wprev, 2, way, 1 - way).wait_recv()
            give_back(way).start()

    @pl.when(sec == 0)
    def _():
        entry_copy(hin).start()

    @pl.when(sec == 1)
    def _():
        entry_copy(hbase).start()

    @pl.when(inner_plane)
    def _():
        for half in (0, 1):
            up(half).wait_recv()
            side(2, 2, half).start()
            for way in (0, 1):
                hop(2, way, half).start()
        hand_on(2)
        for way in (0, 1):
            hop(0, way, 1 - way).start()

    hand_on(0)
    for way in (0, 1):
        @pl.when(sec != pen)
        def _():
            hop(1, way, way).start()

    for way in (0, 1):
        @pl.when(sec != pen)
        def _():
            hop(1, way, 1 - way).start()

        @pl.when(sec == pen)
        def _():
            hop(1, way, 0).start()

    @pl.when(sec == last)
    def _():
        for way in (0, 1):
            narrow(wprev, 2, way, 2).wait_recv()
        give_back(2).start()

    def step_in(m):
        ctx_copy(m).wait_recv()

        @pl.when(sec > 1)
        def _():
            h_copy(m).wait_recv()

        hin[m] = (hbase[m].astype(F32) + dot_nn(ctxp[m], wprev[...])).astype(BF16)

    def normalise(m, carry):
        wide = hin[m].astype(F32)
        hnext[m] = (wide * rms_of(wide) * gain[...]).astype(BF16)
        return carry

    def chip_part(c):
        depth = 2 * w_in.shape[0]
        rows = pl.ds(pl.multiple_of(c * depth, depth), depth)
        left = hnext[:, :, rows].reshape(seqs * length, depth)
        return dot_nn(left, wqkv[rows, :]).reshape(seqs, length, wqkv.shape[1])

    @pl.when(sec == 0)
    def _():
        entry_copy(hin).wait()
        lax.fori_loop(0, seqs, normalise, 0)

    @pl.when(inner_plane)
    def _():
        finish(2)

    @pl.when(sec == 1)
    def _():
        entry_copy(hbase).wait()

        def ahead(m, carry):
            step_in(m)
            normalise(m, 0)

            @pl.when(jnp.logical_and(sec < pen, m < seqs - 1))
            def _():
                h_copy(m).start()

            return carry

        lax.fori_loop(0, seqs, ahead, 0)

    finish_near(0)

    @pl.when(sec <= 1)
    def _():
        pre[...] = chip_part(chip)

        def beside(step, carry):
            pre[...] += chip_part(place(lax.rem(at + 2 * step + 1, chips)))
            return carry

        lax.fori_loop(0, 2, beside, 0)

    finish_far(0)

    @pl.when(sec <= 1)
    def _():
        pre[...] += chip_part(place(lax.rem(at + 2, chips)))

    @pl.when(sec == last)
    def _():
        kv_half().start()
        hand_on(1)

    def live_keys(m, columns):
        return lax.broadcasted_iota(jnp.int32, (length, columns), 0) < lengths[m]

    def project(m):
        wide = hin[m].astype(F32)
        normed = (wide * rms_of(wide) * gain[...]).astype(BF16)
        pre[m] = dot_nn(normed, wqkv[...])

    def attend(m):
        x = rotate(pre[m], cos_ref[...], sin_ref[...]).astype(BF16)
        xs[m] = x
        keys = both_halves(x[:, qw : qw + 128])
        values = both_halves(x[:, qw + 128 : qw + 256])
        live = live_keys(m, GROUP_HEADS * length)
        stacks = []
        for group in range(KV_GROUPS):
            scores = dot_nt(keys[group], stack_heads(x, group)) * HEAD_DIM ** (-0.5)
            weights = jnp.where(live, jnp.exp(scores), 0.0)
            prob = weights / jnp.sum(weights, axis=0, keepdims=True)
            probs[m, group] = prob
            stacks.append(dot_tn(prob.astype(BF16), values[group]))
        ctx[m] = merge_heads(stacks, length).astype(BF16)

    @pl.when(sec < pen)
    def _():
        def forward(m, carry):
            @pl.when(sec > 1)
            def _():
                step_in(m)
                h_copy(m).start()
                project(m)

            attend(m)
            ctx_copy(m).start()

            @pl.when(jnp.logical_and(sec == 1, m == seqs - 2))
            def _():
                h_copy(seqs - 1).start()

            return carry

        lax.fori_loop(0, seqs, forward, 0)
        hand_on(1)

    flat = seqs * length
    row8 = lax.broadcasted_iota(jnp.int32, (8, 1), 0)
    spot = lax.broadcasted_iota(jnp.int32, (length, 1), 0)

    def pick(value, j):
        return jnp.sum(jnp.where(spot == lengths[j] - 1, value, 0.0), axis=0, keepdims=True)

    @pl.when(sec == pen)
    def _():
        rowf[...] = jnp.zeros_like(rowf)

        def pair(p, carry):
            two = pl.ds(2 * p, 2)
            for i in range(2):
                ctx_copy(2 * p + i).wait_recv()
                h_copy(2 * p + i).wait_recv()
            update = dot_nn(ctxp[two].reshape(2 * length, qw), wprev[...])
            wide = (hbase[two].reshape(2 * length, width).astype(F32) + update).astype(BF16)
            hin[two] = wide.reshape(2, length, width)
            wide = wide.astype(F32)
            normed = (wide * rms_of(wide) * gain[...]).astype(BF16)
            pre[two] = dot_nn(normed, wqkv[...]).reshape(2, length, wqkv.shape[1])
            attend(2 * p)
            attend(2 * p + 1)

            @pl.when(p == 0)
            def _():
                for way in (0, 1):
                    take(1, way, 0)
                    narrow(wout, 1, way, 2).start()
                for way in (0, 1):
                    give_back(way).wait_recv()
                    side(1, way, 1).start()
                give_back(2).wait_recv()
                side(1, 1, 2).start()
                for way in (0, 1):
                    narrow(wout, 1, way, 2).wait_recv()
                side(1, 0, 2).start()
                keep(1).wait()
                for way, slot in near + far:
                    side(1, way, slot).wait_recv()
                gain_down().wait_recv()

            update = dot_nn(ctx[two].reshape(2 * length, qw), wout[...])
            wide = (hin[two].reshape(2 * length, width).astype(F32) + update).astype(BF16)
            hnext[two] = wide.reshape(2, length, width)
            for i in range(2):
                wide = hnext[2 * p + i].astype(F32)
                hbase[2 * p + i] = (wide * rms_of(wide) * gain_next[...]).astype(BF16)
                rowf[...] = jnp.where(row8 == 2 * p + i, pick(wide, 2 * p + i), rowf[...])
            return carry

        lax.fori_loop(0, seqs // 2, pair, 0)

    @pl.when(sec != pen)
    def _():
        finish(1)

    def turn_over(src, dst):
        def strip(j, carry):
            rows = pl.ds(pl.multiple_of(j * 128, 128), 128)
            dst[:, rows] = src[rows, :].T
            return carry

        lax.fori_loop(0, src.shape[0] // 128, strip, 0)

    @pl.when(sec != pen)
    def _():
        turn_over(wout, wout_t)
        turn_over(wqkv, wqkv_t)

    @pl.when(sec == pen)
    def _():
        kv_half().wait_recv()
        kv_side().start()
        kv_side().wait_recv()
        rown[...] = jnp.concatenate([rowf[...], rowf[...]], axis=0).astype(BF16)
        kv_all = dot_nn(hbase[...].reshape(flat, width), wkvn[...])
        for m in range(seqs):
            kvn[m] = rotate(
                kv_all[m * length : (m + 1) * length], cos_ref[:, qw:], sin_ref[:, qw:]
            ).astype(BF16)
        for copy in kv_up():
            copy.start()
        for m in range(seqs):
            h_last(m).start()
        turn_over(wkvn, wkvn_t)
        turn_over(wout, wout_t)
        turn_over(wqkv, wqkv_t)

    def last_grad(m, wkv_t, gain_row, layer_in):
        here = spot == lengths[m] - 1
        mine = tail[0:8].astype(F32)
        query_part = jnp.sum(jnp.where(row8 == m, mine, 0.0), axis=0, keepdims=True)
        seed = jnp.sum(jnp.where(row8 == m + seqs, mine, 0.0), axis=0, keepdims=True)
        grad_n = dot_nn(gkv[m], wkv_t) + jnp.where(here, query_part, 0.0)
        grad_n = grad_n.astype(BF16).astype(F32) * gain_row
        wide = layer_in.astype(F32)
        scale = rms_of(wide)
        slope = scale * scale * scale * jnp.mean(wide * grad_n, axis=-1, keepdims=True)
        return (jnp.where(here, seed, 0.0) + grad_n * scale - wide * slope).astype(BF16)

    @pl.when(sec == last)
    def _():
        def gather_rows(parts):
            full = jnp.zeros((8, parts[0].shape[1]), F32)
            for j, row in enumerate(parts):
                full = jnp.where(row8 == j, row, full)
            return full

        def swap_half(head):
            return head // GROUP_HEADS != head % 2

        def half_mask(head, group_side):
            low = low_half((8, 128))
            upper_side = head // GROUP_HEADS if group_side else head % 2
            return low if upper_side == 0 else jnp.logical_not(low)

        def to_stack(rows):
            heads = []
            for head in range(HEADS):
                tile = rows[:, head // 2 * 128 : head // 2 * 128 + 128]
                if swap_half(head):
                    tile = pltpu.roll(tile, HEAD_DIM, 1)
                heads.append(jnp.where(half_mask(head, True), tile, 0.0))
            row16 = lax.broadcasted_iota(jnp.int32, (16, 128), 0)
            blocks_of = []
            for j in range(seqs):
                full = jnp.zeros((16, 128), F32)
                for head, tile in enumerate(heads):
                    full = jnp.where(row16 == head, tile[j : j + 1], full)
                blocks_of.append(full)
            return jnp.concatenate(blocks_of, axis=0).astype(BF16)

        def from_stack(stack):
            tiles = []
            for pair in range(HEADS // 2):
                halves = []
                for head in (2 * pair, 2 * pair + 1):
                    tile = gather_rows([stack[j * 16 + head : j * 16 + head + 1] for j in range(seqs)])
                    halves.append(pltpu.roll(tile, HEAD_DIM, 1) if swap_half(head) else tile)
                tiles.append(jnp.where(low_half((8, 128)), halves[0], halves[1]))
            return jnp.concatenate(tiles, axis=1)

        cos_row = gather_rows([pick(cos_ref[:, :qw], j) for j in range(seqs)])
        sin_row = gather_rows([pick(sin_ref[:, :qw], j) for j in range(seqs)])
        stacked_rows = lax.broadcasted_iota(jnp.int32, (16 * seqs, flat), 0) // 16
        key_at = lax.broadcasted_iota(jnp.int32, (16 * seqs, flat), 1)
        live = jnp.zeros((16 * seqs, flat), jnp.int32)
        for j in range(seqs):
            live = jnp.where(stacked_rows == j, j * length + lengths[j], live)
        live = jnp.logical_and(key_at >= stacked_rows * length, key_at < live)

        for copy in kv_up():
            copy.wait_recv()
        rows_in = rown[0:8].astype(F32)
        normed = (rows_in * rms_of(rows_in) * gain[...]).astype(BF16)
        query = rotate(dot_nn(normed, wqkv[:, :qw]), cos_row, sin_row).astype(BF16).astype(F32)
        keys = kvn[...].reshape(flat, 256)[:, :128]
        values = kvn[...].reshape(flat, 256)[:, 128:256]
        query_stack = to_stack(query)
        scores = dot_nt(query_stack, keys) * HEAD_DIM ** (-0.5)
        weights = jnp.where(live, jnp.exp(scores), 0.0)
        prob = weights / jnp.sum(weights, axis=-1, keepdims=True)
        prob_low = prob.astype(BF16)
        context = from_stack(dot_nn(prob_low, values)).astype(BF16)
        rows_out = (rows_in + dot_nn(context, wout[...])).astype(BF16).astype(F32)

        fgain = jnp.concatenate(
            [final_gain[i : i + 1] for i in range(final_gain.shape[0])], axis=1
        )
        row_part = lax.broadcasted_iota(jnp.int32, (16, part), 0)
        scale_out = rms_of(rows_out)
        pooled = rows_out * scale_out * fgain
        total_sq = jnp.sum(pooled * pooled, axis=-1, keepdims=True)
        size = lax.rsqrt(jnp.where(row8 < seqs, total_sq, 1.0))
        unit = pooled * size
        mine16 = jnp.zeros((16, part), F32)
        for j in range(seqs):
            for b in range(blocks):
                mine16 = jnp.where(
                    row_part == b * seqs + j, unit[j : j + 1, b * part : (b + 1) * part], mine16
                )
        emb_all[rep] = mine16.astype(BF16)
        marks = jnp.zeros((8, 128), jnp.int32)
        mark_row = lax.broadcasted_iota(jnp.int32, (8, 128), 0)
        for i in range(micro):
            marks = jnp.where(mark_row == i, positive[i], marks)
        pos_all[rep] = marks

        def exchange(step):
            to = peer(step)
            return [
                pltpu.make_async_remote_copy(
                    src_ref=buf.at[rep], dst_ref=buf.at[rep],
                    send_sem=send.at[step], recv_sem=recv.at[step],
                    device_id={"dp": to}, device_id_type=MESH,
                )
                for buf, send, recv in ((emb_all, e_send, e_recv), (pos_all, p_send, p_recv))
            ]

        copies = [exchange(step) for step in range(1, n_dp)]
        for pair in copies:
            for copy in pair:
                copy.start()
        for pair in copies:
            for copy in pair:
                copy.wait()

        total = n_dp * seqs
        tall = n_dp * 16
        everyone = emb_all[...].reshape(tall, part)
        pr = lax.broadcasted_iota(jnp.int32, (tall, tall), 0)
        pc = lax.broadcasted_iota(jnp.int32, (tall, tall), 1)
        in_block = lax.rem(pr, total)
        home = in_block // seqs * 16 + pr // total * seqs + lax.rem(in_block, seqs)
        sorted_rows = dot_nn((home == pc).astype(BF16), everyone).astype(BF16)
        every = jnp.concatenate(
            [sorted_rows[b * total : (b + 1) * total] for b in range(blocks)], axis=1
        )
        logits = SHARPNESS * dot_nt(every, every)
        qr = lax.broadcasted_iota(jnp.int32, (total, total), 0)
        dc = lax.broadcasted_iota(jnp.int32, (total, total), 1)
        doc = lax.rem(dc, 2) == 1
        weights = jnp.where(doc, jnp.exp(logits), 0.0)
        odds = weights / jnp.sum(weights, axis=-1, keepdims=True)
        marks_all = pos_all[...].reshape(n_dp * 8, 128).astype(F32)
        pr = lax.broadcasted_iota(jnp.int32, (total, n_dp * 8), 0)
        pc = lax.broadcasted_iota(jnp.int32, (total, n_dp * 8), 1)
        chosen = (pr // seqs * 8 + lax.rem(pr, seqs) // 2 == pc).astype(F32)
        target = dot_hi(chosen, marks_all)[:, :1]
        hit = jnp.logical_and(doc, (dc // 2).astype(F32) == target).astype(F32)
        coef = (odds - hit) * (COEF * SHARPNESS)
        coef = jnp.where(lax.rem(qr, 2) == 0, coef, 0.0)
        both = coef + coef.T
        own_coef = gather_rows([
            jnp.sum(jnp.where(qr == rep * seqs + j, both, 0.0), axis=0, keepdims=True)
            for j in range(seqs)
        ])
        grad_e = dot_hi(own_coef, every.astype(F32))
        grad_f = size * (grad_e - unit * jnp.sum(unit * grad_e, axis=-1, keepdims=True))
        grad_n = grad_f * fgain
        seeds = grad_n * scale_out - rows_out * (
            scale_out * scale_out * scale_out
            * jnp.mean(rows_out * grad_n, axis=-1, keepdims=True)
        )
        seed8 = jnp.where(row8 < seqs, seeds, 0.0).astype(BF16)
        grad_ctx = dot_nn(seed8, wout_t[...]).astype(BF16).astype(F32)
        upper = to_stack(grad_ctx)
        grad_p = dot_nt(upper, values).astype(BF16).astype(F32)
        grad_v = dot_tn(prob_low, upper)
        inner = jnp.sum(grad_p * prob, axis=-1, keepdims=True)
        grad_s = (prob * (grad_p - inner) * HEAD_DIM ** (-0.5)).astype(BF16)
        grad_k = dot_tn(grad_s, query_stack)
        grad_kv = jnp.concatenate([grad_k, grad_v], axis=1).astype(BF16).astype(F32)
        for j in range(seqs):
            gkv[j] = rotate(
                grad_kv[j * length : (j + 1) * length], cos_ref[:, qw:], -sin_ref[:, qw:]
            ).astype(BF16)
        for j in range(seqs):
            gkv_copy(j).start()
        grad_query = from_stack(dot_nn(grad_s, keys)).astype(BF16).astype(F32)
        grad_query = rotate(grad_query, cos_row, -sin_row).astype(BF16)
        query_part = dot_nn(grad_query, wqkv_t[:qw, :])
        seed_full = seed8.astype(F32)
        both_parts = query_part
        for j in range(seqs):
            both_parts = jnp.where(row8 == seqs + j, seed_full[j : j + 1], both_parts)
        tail[...] = jnp.concatenate([both_parts, both_parts], axis=0).astype(BF16)
        tail_copy().start()

        def own_grad(m, carry):
            h_last(m).wait_recv()
            out[m] = last_grad(m, wqkv_t[qw : qw + 256, :], gain[...], hbase[m])
            return carry

        lax.fori_loop(0, seqs, own_grad, 0)

    @pl.when(sec < last)
    def _():
        @pl.when(sec == pen)
        def _():
            tail_copy().wait_recv()

        def backward(m, carry):
            x = xs[m]
            keys = both_halves(x[:, qw : qw + 128])
            values = both_halves(x[:, qw + 128 : qw + 256])
            scale = rms_of(hin[m].astype(F32))
            gain_row = gain[...]

            @pl.when(sec == pen)
            def _():
                gkv_copy(m).wait_recv()
                first = last_grad(m, wkvn_t[...], gain_next[...], hnext[m])
                for c in range(cuts):
                    gin[m, c] = first[:, c * piece_width : (c + 1) * piece_width]

            grad_ctx = jnp.zeros((length, qw), F32)
            for c in range(cuts):
                @pl.when(sec < pen)
                def _():
                    g_copy(m, c).wait_recv()

                lanes = slice(c * piece_width, (c + 1) * piece_width)
                grad_ctx += dot_nn(gin[m, c], wout_t[lanes, :])
            grad_ctx = grad_ctx.astype(BF16)
            grad_q, grad_k, grad_v = [], [], []
            for group in range(KV_GROUPS):
                prob = probs[m, group]
                upper = stack_heads(grad_ctx, group)
                grad_p = dot_nt(values[group], upper).astype(BF16).astype(F32)
                grad_v.append(dot_nn(prob.astype(BF16), upper))
                inner = jnp.sum(grad_p * prob, axis=0, keepdims=True)
                grad_s = (prob * (grad_p - inner) * HEAD_DIM ** (-0.5)).astype(BF16)
                grad_q.append(dot_tn(grad_s, keys[group]))
                grad_k.append(dot_nn(grad_s, stack_heads(x, group)))
            grad_x = jnp.concatenate(
                [merge_heads(grad_q, length), fold_groups(grad_k), fold_groups(grad_v)], axis=1
            )
            grad_x = grad_x.astype(BF16).astype(F32)
            along = jnp.sum(grad_x * x.astype(F32), axis=-1, keepdims=True)
            slope = scale * scale * along * (1.0 / width)
            grad_x = rotate(grad_x, cos_ref[...], -sin_ref[...]).astype(BF16)
            for c in range(cuts):
                lanes = slice(c * piece_width, (c + 1) * piece_width)
                grad_n = dot_nn(grad_x, wqkv_t[:, lanes]).astype(BF16).astype(F32)
                grad_n = grad_n * gain_row[:, lanes]
                wide = hin[m, :, lanes].astype(F32)
                piece_grad = gin[m, c].astype(F32) + grad_n * scale - wide * slope
                piece_grad = piece_grad.astype(BF16)
                out[m, :, lanes] = piece_grad

                @pl.when(sec > 0)
                def _():
                    gout[m, c] = piece_grad
                    g_copy(m, c).start()

            return carry

        lax.fori_loop(0, seqs, backward, 0)

    @pl.when(sec < pen)
    def _():
        up(0).wait_send()
        up(1).wait_send()
        for m in range(seqs):
            ctx_copy(m).wait_send()

    @pl.when(jnp.logical_and(sec >= 1, sec < pen))
    def _():
        for m in range(seqs):
            h_copy(m).wait_send()

    @pl.when(inner_plane)
    def _():
        for m in range(seqs):
            for c in range(cuts):
                g_copy(m, c).wait_send()

    @pl.when(sec == pen)
    def _():
        lend().wait_send()
        kv_side().wait_send()
        for copy in kv_up():
            copy.wait_send()
        for m in range(seqs):
            h_last(m).wait_send()

    @pl.when(sec == last)
    def _():
        kv_half().wait_send()
        gain_down().wait_send()
        for which in range(3):
            give_back(which).wait_send()
        for way in (0, 1):
            for slot in range(3):
                narrow(wprev, 2, way, slot).wait_send()
        for m in range(seqs):
            gkv_copy(m).wait_send()
        tail_copy().wait_send()

    def settle(piece):
        for way, slot in near + far:
            side(piece, way, slot).wait_send()
        for way in (0, 1):
            hop(piece, way, 0).wait_send()
            if piece != 1:
                hop(piece, way, 1).wait_send()
                hop(piece, way, 2).wait_send()

    settle(0)
    settle(1)

    @pl.when(sec != pen)
    def _():
        for way in (0, 1):
            hop(1, way, 1).wait_send()
            hop(1, way, 2).wait_send()

    @pl.when(sec == pen)
    def _():
        for way in (0, 1):
            narrow(wout, 1, way, 2).wait_send()

    @pl.when(inner_plane)
    def _():
        settle(2)


def tables(length, qw, columns):
    lane = np.arange(columns)
    half = HEAD_DIM // 2
    frequency = np.float32(ROPE_BASE) ** (
        -(lane % half).astype(np.float32) * np.float32(2.0 / HEAD_DIM)
    )
    angles = np.arange(length, dtype=np.float32)[:, None] * frequency[None, :]
    turned = (lane < columns - KV_GROUPS * HEAD_DIM)[None, :]
    sign = np.where(lane % HEAD_DIM < half, -1.0, 1.0)[None, :]
    cos = np.where(turned, np.cos(angles), 1.0).astype(np.float32)
    sin = np.where(turned, np.sin(angles) * sign, 0.0).astype(np.float32)
    return jnp.asarray(cos), jnp.asarray(sin)


def per_device(entry, norm_gain, w_qkv, w_out, final_gain, lengths, positive):
    n_sec = lax.axis_size("section")
    n_dp = lax.axis_size("dp")
    seqs = lengths.shape[0]
    rows, width = entry.shape
    length = rows // seqs
    qw = w_out.shape[1] * n_dp
    columns = w_qkv.shape[2]
    ring = w_qkv.shape[1] % 16 == 0 and w_out.shape[1] % 16 == 0 and n_dp % 4 == 0
    if ring:
        full_qkv, full_out = w_qkv[0], w_out[0]
    else:
        full_qkv = lax.all_gather(w_qkv, "dp", axis=1, tiled=True)[0]
        full_out = lax.all_gather(w_out, "dp", axis=1, tiled=True)[0]
    cos, sin = tables(length, qw, columns)
    vmem = pl.BlockSpec(memory_space=pltpu.VMEM)
    smem = pl.BlockSpec(memory_space=pltpu.SMEM)
    anywhere = pl.BlockSpec(memory_space=pl.ANY)
    part = width // (16 // seqs)
    dma = pltpu.SemaphoreType.DMA
    block = (seqs, length, width)
    if ring and n_dp // 2 == 4 and n_sec > 3:
        kv = columns - qw
        result = pl.pallas_call(
            functools.partial(swift, n_sec, n_dp, seqs, length),
            out_shape=jax.ShapeDtypeStruct(block, BF16),
            in_specs=[anywhere, vmem, anywhere, anywhere] + [vmem] * 3 + [smem] * 2,
            out_specs=vmem,
            scratch_shapes=[
                pltpu.VMEM(block, BF16),
                pltpu.VMEM(block, BF16),
                pltpu.VMEM(block, BF16),
                pltpu.VMEM((seqs, 4, length, width // 4), BF16),
                pltpu.VMEM((seqs, 4, length, width // 4), BF16),
                pltpu.VMEM((seqs, length, columns), F32),
                pltpu.VMEM((seqs, length, columns), BF16),
                pltpu.VMEM((seqs, KV_GROUPS, length, GROUP_HEADS * length), F32),
                pltpu.VMEM((seqs, length, qw), BF16),
                pltpu.VMEM((seqs, length, qw), BF16),
                pltpu.VMEM((width, columns), BF16),
                pltpu.VMEM((qw, width), BF16),
                pltpu.VMEM((qw, width), BF16),
                pltpu.VMEM((width, kv), BF16),
                pltpu.VMEM((columns, width), BF16),
                pltpu.VMEM((width, qw), BF16),
                pltpu.VMEM((kv, width), BF16),
                pltpu.VMEM((1, width), F32),
                pltpu.VMEM((seqs, length, kv), BF16),
                pltpu.VMEM((8, width), F32),
                pltpu.VMEM((16, width), BF16),
                pltpu.VMEM((seqs, length, kv), BF16),
                pltpu.VMEM((16, width), BF16),
                pltpu.VMEM((n_dp, 16, part), BF16),
                pltpu.VMEM((n_dp, 8, 128), jnp.int32),
                dma((3, 2, 3)), dma((3, 2, 3)), dma((3, 3, 3)), dma((3, 3, 3)), dma((3,)),
                dma((2,)), dma((2,)),
                dma((seqs,)), dma((seqs,)), dma((seqs,)), dma((seqs,)),
                dma((seqs, 4)), dma((seqs, 4)), dma((3,)), dma((3,)),
                dma((2,)), dma((2,)), dma((seqs + 1,)), dma((seqs + 1,)), dma((3,)), dma((3,)),
                dma((n_dp,)), dma((n_dp,)), dma((n_dp,)), dma((n_dp,)),
            ],
            compiler_params=pltpu.CompilerParams(
                collective_id=0, has_side_effects=True, vmem_limit_bytes=60 * 1024 * 1024
            ),
        )(
            entry.reshape(block), norm_gain, w_qkv[0], w_out[0],
            final_gain.reshape(width // 128, 128), cos, sin, lengths, positive,
        )
        return result.reshape(1, rows, width)
    reach = n_dp // 4
    gathering = [
        pltpu.VMEM((width, columns), BF16),
        pltpu.VMEM((qw, width), BF16),
        pltpu.SemaphoreType.DMA((2, 2, reach)),
        pltpu.SemaphoreType.DMA((2, 2, reach)),
        pltpu.SemaphoreType.DMA((2, 2, reach + 1)),
        pltpu.SemaphoreType.DMA((2, 2, reach + 1)),
        pltpu.SemaphoreType.DMA((2,)),
    ] if ring else []
    result = pl.pallas_call(
        functools.partial(kernel, n_sec, n_dp, seqs, length, ring),
        out_shape=jax.ShapeDtypeStruct(block, BF16),
        in_specs=[vmem] * 7 + [smem] * 2,
        out_specs=vmem,
        scratch_shapes=[
            pltpu.VMEM(block, BF16),
            pltpu.VMEM(block, BF16),
            pltpu.VMEM(block, BF16),
            pltpu.VMEM((seqs, length, columns), BF16),
            pltpu.VMEM((seqs, KV_GROUPS, GROUP_HEADS * length, length), F32),
            pltpu.VMEM((seqs, 1, width), F32),
            pltpu.VMEM((n_dp, 16, part), BF16),
            pltpu.VMEM((n_dp, 8, 128), jnp.int32),
            pltpu.VMEM((seqs, length, qw), BF16),
            dma((seqs,)), dma((seqs,)), dma((seqs,)), dma((seqs,)),
            dma((n_dp,)), dma((n_dp,)), dma((n_dp,)), dma((n_dp,)),
            *gathering,
        ],
        compiler_params=pltpu.CompilerParams(
            collective_id=0, has_side_effects=True, vmem_limit_bytes=60 * 1024 * 1024
        ),
    )(
        entry.reshape(block), norm_gain, full_qkv, full_out, final_gain.reshape(1, width),
        cos, sin, lengths, positive,
    )
    return result.reshape(1, rows, width)


def solution(mesh):
    return jax.shard_map(
        per_device,
        mesh=mesh,
        in_specs=(
            P("dp", None),
            P("section", None),
            P("section", "dp", None),
            P("section", "dp", None),
            P(),
            P("dp"),
            P("dp"),
        ),
        out_specs=P("section", "dp", None),
        check_vma=False,
    )
```

```python
import functools

import jax
import jax.numpy as jnp
import numpy as np
from jax import lax
from jax.experimental import pallas as pl
from jax.experimental.pallas import tpu as pltpu
from jax.sharding import PartitionSpec as P

HEAD_DIM = 64
GROUP_HEADS = 7
KV_GROUPS = 2
HEADS = GROUP_HEADS * KV_GROUPS
ROPE_BASE = 1000000.0
EPS = 1e-06
SHARPNESS = 20.0
COEF = 256.0
MESH = pl.DeviceIdType.MESH
F32 = jnp.float32
BF16 = jnp.bfloat16
HI = lax.Precision.HIGHEST


def dot_nn(a, b):
    return lax.dot_general(a, b, (((1,), (0,)), ((), ())), preferred_element_type=F32)


def dot_nt(a, b):
    return lax.dot_general(a, b, (((1,), (1,)), ((), ())), preferred_element_type=F32)


def dot_tn(a, b):
    return lax.dot_general(a, b, (((0,), (0,)), ((), ())), preferred_element_type=F32)


def dot_hi(a, b):
    return lax.dot_general(
        a, b, (((1,), (0,)), ((), ())), preferred_element_type=F32, precision=HI
    )


def rotate(x, cos, sin_signed):
    width = x.shape[-1]
    lane = lax.broadcasted_iota(jnp.int32, x.shape, 1)
    first = lax.rem(lane, HEAD_DIM) < HEAD_DIM // 2
    ahead = pltpu.roll(x, width - HEAD_DIM // 2, 1)
    behind = pltpu.roll(x, HEAD_DIM // 2, 1)
    return x * cos + jnp.where(first, ahead, behind) * sin_signed


def low_half(shape):
    return lax.broadcasted_iota(jnp.int32, shape, 1) < HEAD_DIM


def both_halves(tile):
    wide = tile.astype(F32)
    turned = pltpu.roll(wide, HEAD_DIM, 1)
    low = low_half(wide.shape)
    return (
        jnp.where(low, wide, turned).astype(BF16),
        jnp.where(low, turned, wide).astype(BF16),
    )


def stack_heads(rows, group):
    parts = []
    for head in range(group * GROUP_HEADS, (group + 1) * GROUP_HEADS):
        tile = rows[:, head // 2 * 128 : head // 2 * 128 + 128].astype(F32)
        low = low_half(tile.shape)
        keep = low if head % 2 == 0 else jnp.logical_not(low)
        parts.append(jnp.where(keep, tile, 0.0).astype(BF16))
    return jnp.concatenate(parts, axis=0)


def merge_heads(stacks, length):
    tiles = []
    for pair in range(HEADS // 2):
        halves = []
        for head in (2 * pair, 2 * pair + 1):
            at = head % GROUP_HEADS * length
            halves.append(stacks[head // GROUP_HEADS][at : at + length])
        tiles.append(jnp.where(low_half(halves[0].shape), halves[0], halves[1]))
    return jnp.concatenate(tiles, axis=1)


def fold_groups(sums):
    full = [value + pltpu.roll(value, HEAD_DIM, 1) for value in sums]
    return jnp.where(low_half(full[0].shape), full[0], full[1])


def rms_of(wide):
    return lax.rsqrt(jnp.mean(wide * wide, axis=-1, keepdims=True) + EPS)


def kernel(
    n_sec, n_dp, seqs, length, ring,
    entry, gain, w_in, w_up, final_gain, cos_ref, sin_ref, lengths, positive,
    out,
    hin, hout, gin, xs, probs, rows_buf, emb_all, pos_all, contexts,
    f_send, f_recv, b_send, b_recv, e_send, e_recv, p_send, p_recv,
    *gathering,
):
    sec = lax.axis_index("section")
    rep = lax.axis_index("dp")
    last = n_sec - 1
    width = entry.shape[-1]
    wqkv, wout = gathering[:2] if ring else (w_in, w_up)
    qw = wout.shape[0]
    blocks = 16 // seqs
    part = width // blocks
    micro = seqs // 2

    barrier = pltpu.get_barrier_semaphore()

    def peer(step):
        return lax.rem(rep + step, n_dp)

    for near in (lax.rem(sec + 1, n_sec), lax.rem(sec + n_sec - 1, n_sec)):
        pl.semaphore_signal(barrier, inc=1, device_id={"section": near}, device_id_type=MESH)
    for step in range(1, n_dp):
        pl.semaphore_signal(barrier, inc=1, device_id={"dp": peer(step)}, device_id_type=MESH)
    pl.semaphore_wait(barrier, n_dp + 1)

    def forward_copy(m):
        return pltpu.make_async_remote_copy(
            src_ref=hout.at[m], dst_ref=hin.at[m], send_sem=f_send.at[m], recv_sem=f_recv.at[m],
            device_id={"section": sec + 1}, device_id_type=MESH,
        )

    def backward_copy(m):
        return pltpu.make_async_remote_copy(
            src_ref=out.at[m], dst_ref=gin.at[m], send_sem=b_send.at[m], recv_sem=b_recv.at[m],
            device_id={"section": sec - 1}, device_id_type=MESH,
        )

    @pl.when(sec == 0)
    def _():
        hin[...] = entry[...]

    def live_keys(m):
        keys = lax.broadcasted_iota(jnp.int32, (GROUP_HEADS * length, length), 1)
        return keys < lengths[m]

    def attend(m):
        wide = hin[m].astype(F32)
        normed = (wide * rms_of(wide) * gain[...]).astype(BF16)
        x = rotate(dot_nn(normed, wqkv[...]), cos_ref[...], sin_ref[...]).astype(BF16)
        xs[m] = x
        keys = both_halves(x[:, qw : qw + 128])
        values = both_halves(x[:, qw + 128 : qw + 256])
        live = live_keys(m)
        stacks = []
        for group in range(KV_GROUPS):
            scores = dot_nt(stack_heads(x, group), keys[group]) * HEAD_DIM ** (-0.5)
            weights = jnp.where(live, jnp.exp(scores), 0.0)
            prob = weights / jnp.sum(weights, axis=-1, keepdims=True)
            probs[m, group] = prob
            stacks.append(dot_nn(prob.astype(BF16), values[group]))
        contexts[m] = merge_heads(stacks, length).astype(BF16)

    if ring:
        hop_send, hop_recv, side_send, side_recv, keep_sem = gathering[2:]
        chips = n_dp // 2
        reach = chips // 2
        core = lax.rem(rep, 2)
        chip = rep // 2

        def place(c):
            return c + (c // 2) * (1 - 2 * lax.rem(c, 2)) if chips == 4 else c

        at = place(chip)
        pieces = ((w_in, wqkv), (w_up, wout))

        def region(piece, shard, half):
            held = pieces[piece][1]
            rows = pieces[piece][0].shape[0]
            cols = held.shape[1]
            cut = (cols // 128 + 1) // 2 * 128
            span = {None: (0, cols), 0: (0, cut), 1: (cut, cols - cut)}[half]
            start = pl.multiple_of(shard * rows, rows)
            return held.at[pl.ds(start, rows), pl.ds(*span)]

        def own(piece, half):
            mine, held = pieces[piece]
            if half is None:
                return mine
            cols = held.shape[1]
            cut = (cols // 128 + 1) // 2 * 128
            return mine.at[:, pl.ds(*((0, cut), (cut, cols - cut))[half])]

        def half_of(way, step):
            return way if step == reach else None

        def hop(piece, way, step):
            turn = 1 if way == 0 else chips - 1
            source = place(lax.rem(at + (step - 1) * (chips - turn), chips)) * 2 + core
            half = half_of(way, step)
            target = place(lax.rem(at + turn, chips)) * 2 + core
            dst = region(piece, source, half)
            return pltpu.make_async_remote_copy(
                src_ref=own(piece, half) if step == 1 else dst, dst_ref=dst,
                send_sem=hop_send.at[piece, way, step - 1],
                recv_sem=hop_recv.at[piece, way, step - 1],
                device_id={"dp": target}, device_id_type=MESH,
            )

        def side(piece, way, step):
            turn = 1 if way == 0 else chips - 1
            source = place(lax.rem(at + step * (chips - turn), chips)) * 2 + core
            half = half_of(way, step)
            dst = region(piece, source, half)
            return pltpu.make_async_remote_copy(
                src_ref=own(piece, None) if step == 0 else dst, dst_ref=dst,
                send_sem=side_send.at[piece, way, step],
                recv_sem=side_recv.at[piece, way, step],
                device_id={"dp": chip * 2 + 1 - core}, device_id_type=MESH,
            )

        def keep(piece):
            return pltpu.make_async_copy(
                own(piece, None), region(piece, rep, None), keep_sem.at[piece]
            )

        sides = [(0, 0)] + [(way, step) for step in range(1, reach + 1) for way in (0, 1)]

        def begin(piece):
            for way in (0, 1):
                hop(piece, way, 1).start()
            side(piece, 0, 0).start()
            keep(piece).start()

        def advance(piece, step):
            for way in (0, 1):
                hop(piece, way, step).wait_recv()
                if step < reach:
                    hop(piece, way, step + 1).start()
                side(piece, way, step).start()

        def finish(piece):
            advance(piece, reach)
            keep(piece).wait()
            for way, step in sides:
                side(piece, way, step).wait_recv()

        begin(0)
        for step in range(1, reach):
            advance(0, step)
        begin(1)
        finish(0)

    def early(m, carry):
        if ring:
            @pl.when(m == seqs // 2)
            def _():
                for step in range(1, reach):
                    advance(1, step)

        @pl.when(sec == 0)
        def _():
            attend(m)

        return carry

    lax.fori_loop(0, seqs, early, 0)
    if ring:
        finish(1)

    def forward(m, carry):
        @pl.when(sec > 0)
        def _():
            forward_copy(m).wait_recv()
            attend(m)

        hout[m] = (hin[m].astype(F32) + dot_nn(contexts[m], wout[...])).astype(BF16)

        @pl.when(sec < last)
        def _():
            forward_copy(m).start()

        return carry

    lax.fori_loop(0, seqs, forward, 0)

    @pl.when(sec == last)
    def _():
        fgain = final_gain[...]
        row16 = lax.broadcasted_iota(jnp.int32, (16, part), 0)
        position = lax.broadcasted_iota(jnp.int32, (length, width), 0)
        own = jnp.zeros((16, part), F32)
        for j in range(seqs):
            picked = jnp.where(position == lengths[j] - 1, hout[j].astype(F32), 0.0)
            row = jnp.sum(picked, axis=0, keepdims=True)
            rows_buf[j] = row
            pooled = row * rms_of(row) * fgain
            unit = pooled * lax.rsqrt(jnp.sum(pooled * pooled, axis=-1, keepdims=True))
            for b in range(blocks):
                own = jnp.where(row16 == b * seqs + j, unit[:, b * part : (b + 1) * part], own)
        emb_all[rep] = own.astype(BF16)
        marks = jnp.zeros((8, 128), jnp.int32)
        mark_row = lax.broadcasted_iota(jnp.int32, (8, 128), 0)
        for i in range(micro):
            marks = jnp.where(mark_row == i, positive[i], marks)
        pos_all[rep] = marks

        def exchange(step):
            to = peer(step)
            return [
                pltpu.make_async_remote_copy(
                    src_ref=buf.at[rep], dst_ref=buf.at[rep],
                    send_sem=send.at[step], recv_sem=recv.at[step],
                    device_id={"dp": to}, device_id_type=MESH,
                )
                for buf, send, recv in ((emb_all, e_send, e_recv), (pos_all, p_send, p_recv))
            ]

        copies = [exchange(step) for step in range(1, n_dp)]
        for pair in copies:
            for copy in pair:
                copy.start()
        for pair in copies:
            for copy in pair:
                copy.wait()

        total = n_dp * seqs
        tall = n_dp * 16
        everyone = emb_all[...].reshape(tall, part)
        cross = dot_nt(everyone, everyone)
        ra = lax.broadcasted_iota(jnp.int32, (tall, tall), 0)
        ca = lax.broadcasted_iota(jnp.int32, (tall, tall), 1)
        same = lax.rem(ra, 16) // seqs == lax.rem(ca, 16) // seqs
        cross = jnp.where(same, cross, 0.0)
        fr = lax.broadcasted_iota(jnp.int32, (total, tall), 0)
        fc = lax.broadcasted_iota(jnp.int32, (total, tall), 1)
        fold = (fc // 16 * seqs + lax.rem(fc, seqs) == fr).astype(F32)
        logits = SHARPNESS * lax.dot_general(
            dot_hi(fold, cross), fold, (((1,), (1,)), ((), ())),
            preferred_element_type=F32, precision=HI,
        )
        qr = lax.broadcasted_iota(jnp.int32, (total, total), 0)
        dc = lax.broadcasted_iota(jnp.int32, (total, total), 1)
        doc = lax.rem(dc, 2) == 1
        weights = jnp.where(doc, jnp.exp(logits), 0.0)
        odds = weights / jnp.sum(weights, axis=-1, keepdims=True)
        marks_all = pos_all[...].reshape(n_dp * 8, 128).astype(F32)
        pr = lax.broadcasted_iota(jnp.int32, (total, n_dp * 8), 0)
        pc = lax.broadcasted_iota(jnp.int32, (total, n_dp * 8), 1)
        pick = (pr // seqs * 8 + lax.rem(pr, seqs) // 2 == pc).astype(F32)
        target = dot_hi(pick, marks_all)[:, :1]
        hit = jnp.logical_and(doc, (dc // 2).astype(F32) == target).astype(F32)
        coef = (odds - hit) * (COEF * SHARPNESS)
        coef = jnp.where(lax.rem(qr, 2) == 0, coef, 0.0)
        both = coef + coef.T
        ar = lax.broadcasted_iota(jnp.int32, (16, total), 0)
        ac = lax.broadcasted_iota(jnp.int32, (16, total), 1)
        mine = (rep * seqs + lax.rem(ar, seqs) == ac).astype(F32)
        spread = dot_hi(dot_hi(mine, both), fold)
        br = lax.broadcasted_iota(jnp.int32, (16, tall), 0)
        bc = lax.broadcasted_iota(jnp.int32, (16, tall), 1)
        spread = jnp.where(br // seqs == lax.rem(bc, 16) // seqs, spread, 0.0)
        grad16 = dot_hi(spread, everyone.astype(F32))
        for j in range(seqs):
            grad_e = jnp.concatenate(
                [grad16[b * seqs + j : b * seqs + j + 1] for b in range(blocks)], axis=1
            )
            row = rows_buf[j]
            scale = rms_of(row)
            pooled = row * scale * fgain
            size = lax.rsqrt(jnp.sum(pooled * pooled, axis=-1, keepdims=True))
            unit = pooled * size
            grad_f = size * (grad_e - unit * jnp.sum(unit * grad_e, axis=-1, keepdims=True))
            grad_n = grad_f * fgain
            grad_r = grad_n * scale - row * (
                scale * scale * scale * jnp.mean(row * grad_n, axis=-1, keepdims=True)
            )
            gin[j] = jnp.where(position == lengths[j] - 1, grad_r, 0.0).astype(BF16)

    def backward(m, carry):
        @pl.when(sec < last)
        def _():
            backward_copy(m).wait_recv()

        grad = gin[m]
        x = xs[m]
        keys = both_halves(x[:, qw : qw + 128])
        values = both_halves(x[:, qw + 128 : qw + 256])
        grad_ctx = dot_nt(grad, wout[...]).astype(BF16)
        grad_q, grad_k, grad_v = [], [], []
        for group in range(KV_GROUPS):
            prob = probs[m, group]
            upper = stack_heads(grad_ctx, group)
            grad_p = dot_nt(upper, values[group]).astype(BF16).astype(F32)
            grad_v.append(dot_tn(prob.astype(BF16), upper))
            inner = jnp.sum(grad_p * prob, axis=-1, keepdims=True)
            grad_s = (prob * (grad_p - inner) * HEAD_DIM ** (-0.5)).astype(BF16)
            grad_q.append(dot_nn(grad_s, keys[group]))
            grad_k.append(dot_tn(grad_s, stack_heads(x, group)))
        grad_x = jnp.concatenate(
            [merge_heads(grad_q, length), fold_groups(grad_k), fold_groups(grad_v)], axis=1
        )
        grad_x = grad_x.astype(BF16).astype(F32)
        grad_x = rotate(grad_x, cos_ref[...], -sin_ref[...]).astype(BF16)
        grad_n = dot_nt(grad_x, wqkv[...]).astype(BF16).astype(F32) * gain[...]
        wide = hin[m].astype(F32)
        scale = rms_of(wide)
        slope = scale * scale * scale * jnp.mean(wide * grad_n, axis=-1, keepdims=True)
        out[m] = (grad.astype(F32) + grad_n * scale - wide * slope).astype(BF16)

        @pl.when(sec > 0)
        def _():
            backward_copy(m).start()

        return carry

    lax.fori_loop(0, seqs, backward, 0)

    @pl.when(sec < last)
    def _():
        for m in range(seqs):
            forward_copy(m).wait_send()

    @pl.when(sec > 0)
    def _():
        for m in range(seqs):
            backward_copy(m).wait_send()

    if ring:
        for piece in (0, 1):
            for way in (0, 1):
                for step in range(1, reach + 1):
                    hop(piece, way, step).wait_send()
            for way, step in sides:
                side(piece, way, step).wait_send()


def swift(
    n_sec, n_dp, seqs, length,
    entry, gain, w_in, w_up, final_gain, cos_ref, sin_ref, lengths, positive,
    out,
    hin, hbase, hnext, gin, gout, pre, xs, probs, ctx, ctxp, wqkv, wout, wprev, wkvn, wqkv_t, wout_t, wkvn_t, gain_next,
    kvn, rowb, gkv, tail, emb_all, pos_all,
    hop_send, hop_recv, side_send, side_recv, keep_sem, up_send, up_recv,
    c_send, c_recv, f_send, f_recv, b_send, b_recv, k_send, k_recv,
    v_send, v_recv, g_send, g_recv, d_send, d_recv, e_send, e_recv, p_send, p_recv,
):
    sec = lax.axis_index("section")
    rep = lax.axis_index("dp")
    last = n_sec - 1
    pen = n_sec - 2
    width = entry.shape[-1]
    qw = wout.shape[0]
    blocks = 16 // seqs
    part = width // blocks
    micro = seqs // 2
    inner_plane = jnp.logical_and(sec >= 1, sec <= pen)

    barrier = pltpu.get_barrier_semaphore()

    def peer(step):
        return lax.rem(rep + step, n_dp)

    for near in (lax.rem(sec + 1, n_sec), lax.rem(sec + n_sec - 1, n_sec)):
        pl.semaphore_signal(barrier, inc=1, device_id={"section": near}, device_id_type=MESH)
    for step in range(1, n_dp):
        pl.semaphore_signal(barrier, inc=1, device_id={"dp": peer(step)}, device_id_type=MESH)
    pl.semaphore_wait(barrier, n_dp + 1)

    def to_section(src, dst, send, recv, turn):
        return pltpu.make_async_remote_copy(
            src_ref=src, dst_ref=dst, send_sem=send, recv_sem=recv,
            device_id={"section": sec + turn}, device_id_type=MESH,
        )

    core = lax.rem(rep, 2)
    chip = rep // 2
    chips = n_dp // 2

    def place(c):
        return c + (c // 2) * (1 - 2 * lax.rem(c, 2))

    at = place(chip)
    held = (wqkv, wout, wprev)
    shard_rows = (w_in.shape[0], w_up.shape[0], w_up.shape[0])

    def span(piece, half):
        cols = held[piece].shape[1]
        cut = (cols // 128 + 1) // 2 * 128
        return {None: (0, cols), 0: (0, cut), 1: (cut, cols - cut)}[half]

    def region(piece, shard, half):
        rows = shard_rows[piece]
        start = pl.multiple_of(shard * rows, rows)
        return held[piece].at[pl.ds(start, rows), pl.ds(*span(piece, half))]

    def own(piece, half):
        if piece == 2:
            return region(2, rep, half)
        return (w_in, w_up)[piece].at[:, pl.ds(*span(piece, half))]

    def source_of(way, step):
        turn = 1 if way == 0 else chips - 1
        return place(lax.rem(at + step * (chips - turn), chips)) * 2 + core

    def hop(piece, way, slot):
        turn = 1 if way == 0 else chips - 1
        target = place(lax.rem(at + turn, chips)) * 2 + core
        half = way if slot == 2 else slot
        dst = region(piece, rep if slot < 2 else source_of(way, 1), half)
        return pltpu.make_async_remote_copy(
            src_ref=own(piece, half) if slot < 2 else dst, dst_ref=dst,
            send_sem=hop_send.at[piece, way, slot], recv_sem=hop_recv.at[piece, way, slot],
            device_id={"dp": target}, device_id_type=MESH,
        )

    def hop_in(piece, way, slot):
        half = way if slot == 2 else slot
        dst = region(piece, source_of(way, 2 if slot == 2 else 1), half)
        return pltpu.make_async_remote_copy(
            src_ref=dst, dst_ref=dst,
            send_sem=hop_send.at[piece, way, slot], recv_sem=hop_recv.at[piece, way, slot],
            device_id={"dp": chip * 2 + 1 - core}, device_id_type=MESH,
        )

    def side(piece, way, slot):
        half = way if slot == 2 else slot
        shard = rep if way == 2 else source_of(way, 2 if slot == 2 else 1)
        dst = region(piece, shard, half)
        return pltpu.make_async_remote_copy(
            src_ref=own(piece, half) if way == 2 else dst, dst_ref=dst,
            send_sem=side_send.at[piece, way, slot], recv_sem=side_recv.at[piece, way, slot],
            device_id={"dp": chip * 2 + 1 - core}, device_id_type=MESH,
        )

    near = [(2, 0), (2, 1)] + [(way, slot) for slot in range(2) for way in (0, 1)]
    far = [(0, 2), (1, 2)]

    def keep(piece):
        return pltpu.make_async_copy(own(piece, None), region(piece, rep, None), keep_sem.at[piece])

    def take(piece, way, slot):
        hop_in(piece, way, slot).wait_recv()
        side(piece, way, slot).start()

    def hand_on(piece):
        take(piece, 0, 0)
        hop(piece, 0, 2).start()
        take(piece, 1, 1)
        hop(piece, 1, 2).start()

    def finish_near(piece):
        take(piece, 0, 1)
        take(piece, 1, 0)
        if piece < 2:
            keep(piece).wait()
        for way, slot in near:
            side(piece, way, slot).wait_recv()

    def finish_far(piece):
        for way, slot in far:
            take(piece, way, slot)
        for way, slot in far:
            side(piece, way, slot).wait_recv()

    def finish(piece):
        finish_near(piece)
        finish_far(piece)

    def entry_copy(dst):
        return pltpu.make_async_copy(entry, dst, keep_sem.at[2])

    def up(half):
        return to_section(own(1, half), region(2, rep, half), up_send.at[half], up_recv.at[half], 1)

    lent = span(1, 0)[1] // 2

    def lend():
        return to_section(own(1, 1), region(2, rep, 0), up_send.at[0], up_recv.at[0], 1)

    def quarter(held_ref, shard, which):
        start = pl.multiple_of(shard * w_up.shape[0], w_up.shape[0])
        return held_ref.at[pl.ds(start, w_up.shape[0]), pl.ds(which * lent, lent)]

    def narrow(held_ref, piece, way, slot):
        turn = 1 if way == 0 else chips - 1
        target = place(lax.rem(at + turn, chips)) * 2 + core
        part_of = quarter(held_ref, rep if slot < 2 else source_of(way, 1), way if slot == 2 else slot)
        return pltpu.make_async_remote_copy(
            src_ref=part_of, dst_ref=part_of,
            send_sem=hop_send.at[piece, way, slot], recv_sem=hop_recv.at[piece, way, slot],
            device_id={"dp": target}, device_id_type=MESH,
        )

    def give_back(which):
        shard = source_of(0, 2) if which == 2 else source_of(which, 1)
        return to_section(
            region(2, shard, 0), region(1, shard, 1), d_send.at[which], d_recv.at[which], -1
        )

    def ctx_copy(m):
        return to_section(ctx.at[m], ctxp.at[m], c_send.at[m], c_recv.at[m], 1)

    def h_copy(m):
        return to_section(hin.at[m], hbase.at[m], f_send.at[m], f_recv.at[m], 1)

    def h_last(m):
        return to_section(hnext.at[m], hbase.at[m], f_send.at[m], f_recv.at[m], 1)

    cuts = 4
    piece_width = width // cuts

    def g_copy(m, c):
        return to_section(gout.at[m, c], gin.at[m, c], b_send.at[m, c], b_recv.at[m, c], -1)

    kv_rows = pl.ds(pl.multiple_of(core * (width // 2), width // 2), width // 2)

    def kv_half():
        return to_section(
            wqkv.at[kv_rows, pl.ds(qw, 256)], wkvn.at[kv_rows], k_send.at[0], k_recv.at[0], -1
        )

    def kv_side():
        return pltpu.make_async_remote_copy(
            src_ref=wkvn.at[kv_rows], dst_ref=wkvn.at[kv_rows],
            send_sem=k_send.at[2], recv_sem=k_recv.at[2],
            device_id={"dp": chip * 2 + 1 - core}, device_id_type=MESH,
        )

    def gain_down():
        return to_section(gain, gain_next, k_send.at[1], k_recv.at[1], -1)

    def top(buf):
        return buf.at[pl.ds(0, 8)]

    def kv_up(m):
        return (
            to_section(kvn.at[m], kvn.at[m], v_send.at[m], v_recv.at[m], 1),
            to_section(rowb.at[m], rowb.at[m], v_send.at[seqs + m], v_recv.at[seqs + m], 1),
        )

    def gkv_copy(m):
        return to_section(gkv.at[m], gkv.at[m], g_send.at[m], g_recv.at[m], -1)

    def tail_copy():
        return to_section(top(tail), top(tail), g_send.at[seqs], g_recv.at[seqs], -1)

    @pl.when(sec < pen)
    def _():
        up(0).start()
        up(1).start()

    @pl.when(sec == pen)
    def _():
        lend().start()

    @pl.when(sec == last)
    def _():
        gain_down().start()

    for way in (0, 1):
        hop(0, way, way).start()
    for piece in (0, 1):
        keep(piece).start()
        side(piece, 2, 0).start()
        side(piece, 2, 1).start()

    @pl.when(sec == 0)
    def _():
        for way in (0, 1):
            hop(0, way, 1 - way).start()

    @pl.when(sec == last)
    def _():
        lend().wait_recv()
        for slot in (0, 1):
            for way in (0, 1):
                narrow(wprev, 2, way, slot).start()
        narrow(wprev, 2, 0, 0).wait_recv()
        narrow(wprev, 2, 0, 2).start()
        narrow(wprev, 2, 1, 1).wait_recv()
        narrow(wprev, 2, 1, 2).start()
        for way in (0, 1):
            hop(0, way, 1 - way).start()
        for way in (0, 1):
            narrow(wprev, 2, way, 1 - way).wait_recv()
            give_back(way).start()

    @pl.when(sec == 0)
    def _():
        entry_copy(hin).start()

    @pl.when(sec == 1)
    def _():
        entry_copy(hbase).start()

    @pl.when(inner_plane)
    def _():
        for half in (0, 1):
            up(half).wait_recv()
            side(2, 2, half).start()
            for way in (0, 1):
                hop(2, way, half).start()
        hand_on(2)
        for way in (0, 1):
            hop(0, way, 1 - way).start()

    hand_on(0)
    for way in (0, 1):
        @pl.when(sec != pen)
        def _():
            hop(1, way, way).start()

    for way in (0, 1):
        @pl.when(sec != pen)
        def _():
            hop(1, way, 1 - way).start()

        @pl.when(sec == pen)
        def _():
            hop(1, way, 0).start()

    @pl.when(sec == last)
    def _():
        for way in (0, 1):
            narrow(wprev, 2, way, 2).wait_recv()
        give_back(2).start()

    def step_in(m):
        ctx_copy(m).wait_recv()

        @pl.when(sec > 1)
        def _():
            h_copy(m).wait_recv()

        hin[m] = (hbase[m].astype(F32) + dot_nn(ctxp[m], wprev[...])).astype(BF16)

    def normalise(m, carry):
        wide = hin[m].astype(F32)
        hnext[m] = (wide * rms_of(wide) * gain[...]).astype(BF16)
        return carry

    def chip_part(c):
        depth = 2 * w_in.shape[0]
        rows = pl.ds(pl.multiple_of(c * depth, depth), depth)
        left = hnext[:, :, rows].reshape(seqs * length, depth)
        return dot_nn(left, wqkv[rows, :]).reshape(seqs, length, wqkv.shape[1])

    @pl.when(sec == 0)
    def _():
        entry_copy(hin).wait()
        lax.fori_loop(0, seqs, normalise, 0)

    @pl.when(inner_plane)
    def _():
        finish(2)

    @pl.when(sec == 1)
    def _():
        entry_copy(hbase).wait()

        def ahead(m, carry):
            step_in(m)
            normalise(m, 0)

            @pl.when(jnp.logical_and(sec < pen, m < seqs - 1))
            def _():
                h_copy(m).start()

            return carry

        lax.fori_loop(0, seqs, ahead, 0)

    finish_near(0)

    @pl.when(sec <= 1)
    def _():
        pre[...] = chip_part(chip)

        def beside(step, carry):
            pre[...] += chip_part(place(lax.rem(at + 2 * step + 1, chips)))
            return carry

        lax.fori_loop(0, 2, beside, 0)

    finish_far(0)

    @pl.when(sec <= 1)
    def _():
        pre[...] += chip_part(place(lax.rem(at + 2, chips)))

    @pl.when(sec == last)
    def _():
        kv_half().start()
        hand_on(1)

    def live_keys(m, columns):
        return lax.broadcasted_iota(jnp.int32, (length, columns), 0) < lengths[m]

    def project(m):
        wide = hin[m].astype(F32)
        normed = (wide * rms_of(wide) * gain[...]).astype(BF16)
        pre[m] = dot_nn(normed, wqkv[...])

    def attend(m):
        x = rotate(pre[m], cos_ref[...], sin_ref[...]).astype(BF16)
        xs[m] = x
        keys = both_halves(x[:, qw : qw + 128])
        values = both_halves(x[:, qw + 128 : qw + 256])
        live = live_keys(m, GROUP_HEADS * length)
        stacks = []
        for group in range(KV_GROUPS):
            scores = dot_nt(keys[group], stack_heads(x, group)) * HEAD_DIM ** (-0.5)
            weights = jnp.where(live, jnp.exp(scores), 0.0)
            prob = weights / jnp.sum(weights, axis=0, keepdims=True)
            probs[m, group] = prob
            stacks.append(dot_tn(prob.astype(BF16), values[group]))
        ctx[m] = merge_heads(stacks, length).astype(BF16)

    @pl.when(sec < pen)
    def _():
        def forward(m, carry):
            @pl.when(sec > 1)
            def _():
                step_in(m)
                h_copy(m).start()
                project(m)

            attend(m)
            ctx_copy(m).start()

            @pl.when(jnp.logical_and(sec == 1, m == seqs - 2))
            def _():
                h_copy(seqs - 1).start()

            return carry

        lax.fori_loop(0, seqs, forward, 0)
        hand_on(1)

    flat = seqs * length
    row8 = lax.broadcasted_iota(jnp.int32, (8, 1), 0)
    spot = lax.broadcasted_iota(jnp.int32, (length, 1), 0)

    def pick(value, j):
        return jnp.sum(jnp.where(spot == lengths[j] - 1, value, 0.0), axis=0, keepdims=True)

    @pl.when(sec == pen)
    def _():
        def rows_forward(m, count):
            these = pl.ds(m, count)
            for i in range(count):
                ctx_copy(m + i).wait_recv()
                h_copy(m + i).wait_recv()
            update = dot_nn(ctxp[these].reshape(count * length, qw), wprev[...])
            wide = hbase[these].reshape(count * length, width).astype(F32) + update
            wide = wide.astype(BF16)
            hin[these] = wide.reshape(count, length, width)
            wide = wide.astype(F32)
            normed = (wide * rms_of(wide) * gain[...]).astype(BF16)
            pre[these] = dot_nn(normed, wqkv[...]).reshape(count, length, wqkv.shape[1])
            for i in range(count):
                attend(m + i)

        def pair(p, carry):
            two = pl.ds(2 * p, 2)

            @pl.when(p == 0)
            def _():
                for way in (0, 1):
                    take(1, way, 0)
                    narrow(wout, 1, way, 2).start()

            rows_forward(2 * p, 2)

            @pl.when(p == 0)
            def _():
                for way in (0, 1):
                    give_back(way).wait_recv()
                    side(1, way, 1).start()
                give_back(2).wait_recv()
                side(1, 1, 2).start()
                for way in (0, 1):
                    narrow(wout, 1, way, 2).wait_recv()
                side(1, 0, 2).start()
                keep(1).wait()
                for way, slot in near + far:
                    side(1, way, slot).wait_recv()
                gain_down().wait_recv()
                kv_half().wait_recv()
                kv_side().start()
                kv_side().wait_recv()

            update = dot_nn(ctx[two].reshape(2 * length, qw), wout[...])
            wide = (hin[two].reshape(2 * length, width).astype(F32) + update).astype(BF16)
            hnext[two] = wide.reshape(2, length, width)
            wide = wide.astype(F32)
            normed = (wide * rms_of(wide) * gain_next[...]).astype(BF16)
            kv_two = dot_nn(normed, wkvn[...])
            for i in range(2):
                m = 2 * p + i
                kvn[m] = rotate(
                    kv_two[i * length : (i + 1) * length], cos_ref[:, qw:], sin_ref[:, qw:]
                ).astype(BF16)
                row = pick(wide[i * length : (i + 1) * length], m)
                tiles = [row[:, c * 128 : (c + 1) * 128] for c in range(width // 128)]
                spare = rowb.shape[1] - width // 128
                rowb[m] = jnp.concatenate(tiles + [jnp.zeros((spare, 128), F32)], axis=0).astype(BF16)
                for copy in kv_up(m):
                    copy.start()
            return carry

        lax.fori_loop(0, seqs // 2, pair, 0)

    @pl.when(sec != pen)
    def _():
        finish(1)

    def turn_over(src, dst):
        def strip(j, carry):
            rows = pl.ds(pl.multiple_of(j * 128, 128), 128)
            dst[:, rows] = src[rows, :].T
            return carry

        lax.fori_loop(0, src.shape[0] // 128, strip, 0)

    @pl.when(sec != pen)
    def _():
        turn_over(wout, wout_t)
        turn_over(wqkv, wqkv_t)

    @pl.when(sec == pen)
    def _():
        for m in range(seqs):
            h_last(m).start()
        turn_over(wkvn, wkvn_t)
        turn_over(wout, wout_t)
        turn_over(wqkv, wqkv_t)

    def last_grad(m, wkv_t, gain_row, layer_in):
        here = spot == lengths[m] - 1
        mine = tail[0:8].astype(F32)
        query_part = jnp.sum(jnp.where(row8 == m, mine, 0.0), axis=0, keepdims=True)
        seed = jnp.sum(jnp.where(row8 == m + seqs, mine, 0.0), axis=0, keepdims=True)
        grad_n = dot_nn(gkv[m], wkv_t) + jnp.where(here, query_part, 0.0)
        grad_n = grad_n.astype(BF16).astype(F32) * gain_row
        wide = layer_in.astype(F32)
        scale = rms_of(wide)
        slope = scale * scale * scale * jnp.mean(wide * grad_n, axis=-1, keepdims=True)
        return (jnp.where(here, seed, 0.0) + grad_n * scale - wide * slope).astype(BF16)

    @pl.when(sec == last)
    def _():
        def gather_rows(parts):
            full = jnp.zeros((8, parts[0].shape[1]), F32)
            for j, row in enumerate(parts):
                full = jnp.where(row8 == j, row, full)
            return full

        def swap_half(head):
            return head // GROUP_HEADS != head % 2

        def half_mask(head, group_side):
            low = low_half((8, 128))
            upper_side = head // GROUP_HEADS if group_side else head % 2
            return low if upper_side == 0 else jnp.logical_not(low)

        def to_stack(rows):
            heads = []
            for head in range(HEADS):
                tile = rows[:, head // 2 * 128 : head // 2 * 128 + 128]
                if swap_half(head):
                    tile = pltpu.roll(tile, HEAD_DIM, 1)
                heads.append(jnp.where(half_mask(head, True), tile, 0.0))
            row16 = lax.broadcasted_iota(jnp.int32, (16, 128), 0)
            blocks_of = []
            for j in range(seqs):
                full = jnp.zeros((16, 128), F32)
                for head, tile in enumerate(heads):
                    full = jnp.where(row16 == head, tile[j : j + 1], full)
                blocks_of.append(full)
            return jnp.concatenate(blocks_of, axis=0).astype(BF16)

        def from_stack(stack):
            tiles = []
            for pair in range(HEADS // 2):
                halves = []
                for head in (2 * pair, 2 * pair + 1):
                    tile = gather_rows([stack[j * 16 + head : j * 16 + head + 1] for j in range(seqs)])
                    halves.append(pltpu.roll(tile, HEAD_DIM, 1) if swap_half(head) else tile)
                tiles.append(jnp.where(low_half((8, 128)), halves[0], halves[1]))
            return jnp.concatenate(tiles, axis=1)

        cos_row = gather_rows([pick(cos_ref[:, :qw], j) for j in range(seqs)])
        sin_row = gather_rows([pick(sin_ref[:, :qw], j) for j in range(seqs)])
        stacked_rows = lax.broadcasted_iota(jnp.int32, (16 * seqs, flat), 0) // 16
        key_at = lax.broadcasted_iota(jnp.int32, (16 * seqs, flat), 1)
        live = jnp.zeros((16 * seqs, flat), jnp.int32)
        for j in range(seqs):
            live = jnp.where(stacked_rows == j, j * length + lengths[j], live)
        live = jnp.logical_and(key_at >= stacked_rows * length, key_at < live)

        for m in range(seqs):
            for copy in kv_up(m):
                copy.wait_recv()
        flat_rows = []
        for j in range(seqs):
            tiles = rowb[j].astype(F32)
            flat_rows.append(
                jnp.concatenate([tiles[c : c + 1] for c in range(width // 128)], axis=1)
            )
        rows_in = gather_rows(flat_rows)
        normed = (rows_in * rms_of(rows_in) * gain[...]).astype(BF16)
        query = rotate(dot_nn(normed, wqkv[:, :qw]), cos_row, sin_row).astype(BF16).astype(F32)
        keys = kvn[...].reshape(flat, 256)[:, :128]
        values = kvn[...].reshape(flat, 256)[:, 128:256]
        query_stack = to_stack(query)
        scores = dot_nt(query_stack, keys) * HEAD_DIM ** (-0.5)
        weights = jnp.where(live, jnp.exp(scores), 0.0)
        prob = weights / jnp.sum(weights, axis=-1, keepdims=True)
        prob_low = prob.astype(BF16)
        context = from_stack(dot_nn(prob_low, values)).astype(BF16)
        rows_out = (rows_in + dot_nn(context, wout[...])).astype(BF16).astype(F32)

        fgain = jnp.concatenate(
            [final_gain[i : i + 1] for i in range(final_gain.shape[0])], axis=1
        )
        row_part = lax.broadcasted_iota(jnp.int32, (16, part), 0)
        scale_out = rms_of(rows_out)
        pooled = rows_out * scale_out * fgain
        total_sq = jnp.sum(pooled * pooled, axis=-1, keepdims=True)
        size = lax.rsqrt(jnp.where(row8 < seqs, total_sq, 1.0))
        unit = pooled * size
        mine16 = jnp.zeros((16, part), F32)
        for j in range(seqs):
            for b in range(blocks):
                mine16 = jnp.where(
                    row_part == b * seqs + j, unit[j : j + 1, b * part : (b + 1) * part], mine16
                )
        emb_all[rep] = mine16.astype(BF16)
        marks = jnp.zeros((8, 128), jnp.int32)
        mark_row = lax.broadcasted_iota(jnp.int32, (8, 128), 0)
        for i in range(micro):
            marks = jnp.where(mark_row == i, positive[i], marks)
        pos_all[rep] = marks

        def exchange(step):
            to = peer(step)
            return [
                pltpu.make_async_remote_copy(
                    src_ref=buf.at[rep], dst_ref=buf.at[rep],
                    send_sem=send.at[step], recv_sem=recv.at[step],
                    device_id={"dp": to}, device_id_type=MESH,
                )
                for buf, send, recv in ((emb_all, e_send, e_recv), (pos_all, p_send, p_recv))
            ]

        copies = [exchange(step) for step in range(1, n_dp)]
        for pair in copies:
            for copy in pair:
                copy.start()
        for pair in copies:
            for copy in pair:
                copy.wait()

        total = n_dp * seqs
        tall = n_dp * 16
        everyone = emb_all[...].reshape(tall, part)
        pr = lax.broadcasted_iota(jnp.int32, (tall, tall), 0)
        pc = lax.broadcasted_iota(jnp.int32, (tall, tall), 1)
        in_block = lax.rem(pr, total)
        home = in_block // seqs * 16 + pr // total * seqs + lax.rem(in_block, seqs)
        sorted_rows = dot_nn((home == pc).astype(BF16), everyone).astype(BF16)
        every = jnp.concatenate(
            [sorted_rows[b * total : (b + 1) * total] for b in range(blocks)], axis=1
        )
        logits = SHARPNESS * dot_nt(every, every)
        qr = lax.broadcasted_iota(jnp.int32, (total, total), 0)
        dc = lax.broadcasted_iota(jnp.int32, (total, total), 1)
        doc = lax.rem(dc, 2) == 1
        weights = jnp.where(doc, jnp.exp(logits), 0.0)
        odds = weights / jnp.sum(weights, axis=-1, keepdims=True)
        marks_all = pos_all[...].reshape(n_dp * 8, 128).astype(F32)
        pr = lax.broadcasted_iota(jnp.int32, (total, n_dp * 8), 0)
        pc = lax.broadcasted_iota(jnp.int32, (total, n_dp * 8), 1)
        chosen = (pr // seqs * 8 + lax.rem(pr, seqs) // 2 == pc).astype(F32)
        target = dot_hi(chosen, marks_all)[:, :1]
        hit = jnp.logical_and(doc, (dc // 2).astype(F32) == target).astype(F32)
        coef = (odds - hit) * (COEF * SHARPNESS)
        coef = jnp.where(lax.rem(qr, 2) == 0, coef, 0.0)
        both = coef + coef.T
        own_coef = gather_rows([
            jnp.sum(jnp.where(qr == rep * seqs + j, both, 0.0), axis=0, keepdims=True)
            for j in range(seqs)
        ])
        high = own_coef.astype(BF16).astype(F32)
        middle = (own_coef - high).astype(BF16).astype(F32)
        parts = jnp.concatenate([high, middle, own_coef - high - middle], axis=0).astype(BF16)
        grad_parts = dot_nn(parts, every)
        grad_e = grad_parts[0:8] + grad_parts[8:16] + grad_parts[16:24]
        grad_f = size * (grad_e - unit * jnp.sum(unit * grad_e, axis=-1, keepdims=True))
        grad_n = grad_f * fgain
        seeds = grad_n * scale_out - rows_out * (
            scale_out * scale_out * scale_out
            * jnp.mean(rows_out * grad_n, axis=-1, keepdims=True)
        )
        seed8 = jnp.where(row8 < seqs, seeds, 0.0).astype(BF16)
        grad_ctx = dot_nn(seed8, wout_t[...]).astype(BF16).astype(F32)
        upper = to_stack(grad_ctx)
        grad_p = dot_nt(upper, values).astype(BF16).astype(F32)
        grad_v = dot_tn(prob_low, upper)
        inner = jnp.sum(grad_p * prob, axis=-1, keepdims=True)
        grad_s = (prob * (grad_p - inner) * HEAD_DIM ** (-0.5)).astype(BF16)
        grad_k = dot_tn(grad_s, query_stack)
        grad_kv = jnp.concatenate([grad_k, grad_v], axis=1).astype(BF16).astype(F32)
        for j in range(seqs):
            gkv[j] = rotate(
                grad_kv[j * length : (j + 1) * length], cos_ref[:, qw:], -sin_ref[:, qw:]
            ).astype(BF16)
        for j in range(seqs):
            gkv_copy(j).start()
        grad_query = from_stack(dot_nn(grad_s, keys)).astype(BF16).astype(F32)
        grad_query = rotate(grad_query, cos_row, -sin_row).astype(BF16)
        query_part = dot_nn(grad_query, wqkv_t[:qw, :])
        seed_full = seed8.astype(F32)
        both_parts = query_part
        for j in range(seqs):
            both_parts = jnp.where(row8 == seqs + j, seed_full[j : j + 1], both_parts)
        tail[...] = jnp.concatenate([both_parts, both_parts], axis=0).astype(BF16)
        tail_copy().start()

        def own_grad(m, carry):
            h_last(m).wait_recv()
            out[m] = last_grad(m, wqkv_t[qw : qw + 256, :], gain[...], hbase[m])
            return carry

        lax.fori_loop(0, seqs, own_grad, 0)

    @pl.when(sec < last)
    def _():
        @pl.when(sec == pen)
        def _():
            tail_copy().wait_recv()

        def backward(m, carry):
            x = xs[m]
            keys = both_halves(x[:, qw : qw + 128])
            values = both_halves(x[:, qw + 128 : qw + 256])
            scale = rms_of(hin[m].astype(F32))
            gain_row = gain[...]

            @pl.when(sec == pen)
            def _():
                gkv_copy(m).wait_recv()
                first = last_grad(m, wkvn_t[...], gain_next[...], hnext[m])
                for c in range(cuts):
                    gin[m, c] = first[:, c * piece_width : (c + 1) * piece_width]

            grad_ctx = jnp.zeros((length, qw), F32)
            for c in range(cuts):
                @pl.when(sec < pen)
                def _():
                    g_copy(m, c).wait_recv()

                lanes = slice(c * piece_width, (c + 1) * piece_width)
                grad_ctx += dot_nn(gin[m, c], wout_t[lanes, :])
            grad_ctx = grad_ctx.astype(BF16)
            grad_q, grad_k, grad_v = [], [], []
            for group in range(KV_GROUPS):
                prob = probs[m, group]
                upper = stack_heads(grad_ctx, group)
                grad_p = dot_nt(values[group], upper).astype(BF16).astype(F32)
                grad_v.append(dot_nn(prob.astype(BF16), upper))
                inner = jnp.sum(grad_p * prob, axis=0, keepdims=True)
                grad_s = (prob * (grad_p - inner) * HEAD_DIM ** (-0.5)).astype(BF16)
                grad_q.append(dot_tn(grad_s, keys[group]))
                grad_k.append(dot_nn(grad_s, stack_heads(x, group)))
            grad_x = jnp.concatenate(
                [merge_heads(grad_q, length), fold_groups(grad_k), fold_groups(grad_v)], axis=1
            )
            grad_x = grad_x.astype(BF16).astype(F32)
            along = jnp.sum(grad_x * x.astype(F32), axis=-1, keepdims=True)
            slope = scale * scale * along * (1.0 / width)
            grad_x = rotate(grad_x, cos_ref[...], -sin_ref[...]).astype(BF16)
            for c in range(cuts):
                lanes = slice(c * piece_width, (c + 1) * piece_width)
                grad_n = dot_nn(grad_x, wqkv_t[:, lanes]).astype(BF16).astype(F32)
                grad_n = grad_n * gain_row[:, lanes]
                wide = hin[m, :, lanes].astype(F32)
                piece_grad = gin[m, c].astype(F32) + grad_n * scale - wide * slope
                piece_grad = piece_grad.astype(BF16)
                out[m, :, lanes] = piece_grad

                @pl.when(sec > 0)
                def _():
                    gout[m, c] = piece_grad
                    g_copy(m, c).start()

            return carry

        lax.fori_loop(0, seqs, backward, 0)

    @pl.when(sec < pen)
    def _():
        up(0).wait_send()
        up(1).wait_send()
        for m in range(seqs):
            ctx_copy(m).wait_send()

    @pl.when(jnp.logical_and(sec >= 1, sec < pen))
    def _():
        for m in range(seqs):
            h_copy(m).wait_send()

    @pl.when(inner_plane)
    def _():
        for m in range(seqs):
            for c in range(cuts):
                g_copy(m, c).wait_send()

    @pl.when(sec == pen)
    def _():
        lend().wait_send()
        kv_side().wait_send()
        for m in range(seqs):
            for copy in kv_up(m):
                copy.wait_send()
        for m in range(seqs):
            h_last(m).wait_send()

    @pl.when(sec == last)
    def _():
        kv_half().wait_send()
        gain_down().wait_send()
        for which in range(3):
            give_back(which).wait_send()
        for way in (0, 1):
            for slot in range(3):
                narrow(wprev, 2, way, slot).wait_send()
        for m in range(seqs):
            gkv_copy(m).wait_send()
        tail_copy().wait_send()

    def settle(piece):
        for way, slot in near + far:
            side(piece, way, slot).wait_send()
        for way in (0, 1):
            hop(piece, way, 0).wait_send()
            if piece != 1:
                hop(piece, way, 1).wait_send()
                hop(piece, way, 2).wait_send()

    settle(0)
    settle(1)

    @pl.when(sec != pen)
    def _():
        for way in (0, 1):
            hop(1, way, 1).wait_send()
            hop(1, way, 2).wait_send()

    @pl.when(sec == pen)
    def _():
        for way in (0, 1):
            narrow(wout, 1, way, 2).wait_send()

    @pl.when(inner_plane)
    def _():
        settle(2)


def tables(length, qw, columns):
    lane = np.arange(columns)
    half = HEAD_DIM // 2
    frequency = np.float32(ROPE_BASE) ** (
        -(lane % half).astype(np.float32) * np.float32(2.0 / HEAD_DIM)
    )
    angles = np.arange(length, dtype=np.float32)[:, None] * frequency[None, :]
    turned = (lane < columns - KV_GROUPS * HEAD_DIM)[None, :]
    sign = np.where(lane % HEAD_DIM < half, -1.0, 1.0)[None, :]
    cos = np.where(turned, np.cos(angles), 1.0).astype(np.float32)
    sin = np.where(turned, np.sin(angles) * sign, 0.0).astype(np.float32)
    return jnp.asarray(cos), jnp.asarray(sin)


def per_device(entry, norm_gain, w_qkv, w_out, final_gain, lengths, positive):
    n_sec = lax.axis_size("section")
    n_dp = lax.axis_size("dp")
    seqs = lengths.shape[0]
    rows, width = entry.shape
    length = rows // seqs
    qw = w_out.shape[1] * n_dp
    columns = w_qkv.shape[2]
    ring = w_qkv.shape[1] % 16 == 0 and w_out.shape[1] % 16 == 0 and n_dp % 4 == 0
    if ring:
        full_qkv, full_out = w_qkv[0], w_out[0]
    else:
        full_qkv = lax.all_gather(w_qkv, "dp", axis=1, tiled=True)[0]
        full_out = lax.all_gather(w_out, "dp", axis=1, tiled=True)[0]
    cos, sin = tables(length, qw, columns)
    vmem = pl.BlockSpec(memory_space=pltpu.VMEM)
    smem = pl.BlockSpec(memory_space=pltpu.SMEM)
    anywhere = pl.BlockSpec(memory_space=pl.ANY)
    part = width // (16 // seqs)
    dma = pltpu.SemaphoreType.DMA
    block = (seqs, length, width)
    if ring and n_dp // 2 == 4 and n_sec > 3:
        kv = columns - qw
        result = pl.pallas_call(
            functools.partial(swift, n_sec, n_dp, seqs, length),
            out_shape=jax.ShapeDtypeStruct(block, BF16),
            in_specs=[anywhere, vmem, anywhere, anywhere] + [vmem] * 3 + [smem] * 2,
            out_specs=vmem,
            scratch_shapes=[
                pltpu.VMEM(block, BF16),
                pltpu.VMEM(block, BF16),
                pltpu.VMEM(block, BF16),
                pltpu.VMEM((seqs, 4, length, width // 4), BF16),
                pltpu.VMEM((seqs, 4, length, width // 4), BF16),
                pltpu.VMEM((seqs, length, columns), F32),
                pltpu.VMEM((seqs, length, columns), BF16),
                pltpu.VMEM((seqs, KV_GROUPS, length, GROUP_HEADS * length), F32),
                pltpu.VMEM((seqs, length, qw), BF16),
                pltpu.VMEM((seqs, length, qw), BF16),
                pltpu.VMEM((width, columns), BF16),
                pltpu.VMEM((qw, width), BF16),
                pltpu.VMEM((qw, width), BF16),
                pltpu.VMEM((width, kv), BF16),
                pltpu.VMEM((columns, width), BF16),
                pltpu.VMEM((width, qw), BF16),
                pltpu.VMEM((kv, width), BF16),
                pltpu.VMEM((1, width), F32),
                pltpu.VMEM((seqs, length, kv), BF16),
                pltpu.VMEM((seqs, (width // 128 + 15) // 16 * 16, 128), BF16),
                pltpu.VMEM((seqs, length, kv), BF16),
                pltpu.VMEM((16, width), BF16),
                pltpu.VMEM((n_dp, 16, part), BF16),
                pltpu.VMEM((n_dp, 8, 128), jnp.int32),
                dma((3, 2, 3)), dma((3, 2, 3)), dma((3, 3, 3)), dma((3, 3, 3)), dma((3,)),
                dma((2,)), dma((2,)),
                dma((seqs,)), dma((seqs,)), dma((seqs,)), dma((seqs,)),
                dma((seqs, 4)), dma((seqs, 4)), dma((3,)), dma((3,)),
                dma((2 * seqs,)), dma((2 * seqs,)), dma((seqs + 1,)), dma((seqs + 1,)),
                dma((3,)), dma((3,)),
                dma((n_dp,)), dma((n_dp,)), dma((n_dp,)), dma((n_dp,)),
            ],
            compiler_params=pltpu.CompilerParams(
                collective_id=0, has_side_effects=True, vmem_limit_bytes=60 * 1024 * 1024
            ),
        )(
            entry.reshape(block), norm_gain, w_qkv[0], w_out[0],
            final_gain.reshape(width // 128, 128), cos, sin, lengths, positive,
        )
        return result.reshape(1, rows, width)
    reach = n_dp // 4
    gathering = [
        pltpu.VMEM((width, columns), BF16),
        pltpu.VMEM((qw, width), BF16),
        pltpu.SemaphoreType.DMA((2, 2, reach)),
        pltpu.SemaphoreType.DMA((2, 2, reach)),
        pltpu.SemaphoreType.DMA((2, 2, reach + 1)),
        pltpu.SemaphoreType.DMA((2, 2, reach + 1)),
        pltpu.SemaphoreType.DMA((2,)),
    ] if ring else []
    result = pl.pallas_call(
        functools.partial(kernel, n_sec, n_dp, seqs, length, ring),
        out_shape=jax.ShapeDtypeStruct(block, BF16),
        in_specs=[vmem] * 7 + [smem] * 2,
        out_specs=vmem,
        scratch_shapes=[
            pltpu.VMEM(block, BF16),
            pltpu.VMEM(block, BF16),
            pltpu.VMEM(block, BF16),
            pltpu.VMEM((seqs, length, columns), BF16),
            pltpu.VMEM((seqs, KV_GROUPS, GROUP_HEADS * length, length), F32),
            pltpu.VMEM((seqs, 1, width), F32),
            pltpu.VMEM((n_dp, 16, part), BF16),
            pltpu.VMEM((n_dp, 8, 128), jnp.int32),
            pltpu.VMEM((seqs, length, qw), BF16),
            dma((seqs,)), dma((seqs,)), dma((seqs,)), dma((seqs,)),
            dma((n_dp,)), dma((n_dp,)), dma((n_dp,)), dma((n_dp,)),
            *gathering,
        ],
        compiler_params=pltpu.CompilerParams(
            collective_id=0, has_side_effects=True, vmem_limit_bytes=60 * 1024 * 1024
        ),
    )(
        entry.reshape(block), norm_gain, full_qkv, full_out, final_gain.reshape(1, width),
        cos, sin, lengths, positive,
    )
    return result.reshape(1, rows, width)


def solution(mesh):
    return jax.shard_map(
        per_device,
        mesh=mesh,
        in_specs=(
            P("dp", None),
            P("section", None),
            P("section", "dp", None),
            P("section", "dp", None),
            P(),
            P("dp"),
            P("dp"),
        ),
        out_specs=P("section", "dp", None),
        check_vma=False,
    )
```

```python
import functools

import jax
import jax.numpy as jnp
import numpy as np
from jax import lax
from jax.experimental import pallas as pl
from jax.experimental.pallas import tpu as pltpu
from jax.sharding import PartitionSpec as P

HEAD_DIM = 64
GROUP_HEADS = 7
KV_GROUPS = 2
HEADS = GROUP_HEADS * KV_GROUPS
ROPE_BASE = 1000000.0
EPS = 1e-06
SHARPNESS = 20.0
COEF = 256.0
MESH = pl.DeviceIdType.MESH
F32 = jnp.float32
BF16 = jnp.bfloat16
HI = lax.Precision.HIGHEST


def dot_nn(a, b):
    return lax.dot_general(a, b, (((1,), (0,)), ((), ())), preferred_element_type=F32)


def dot_nt(a, b):
    return lax.dot_general(a, b, (((1,), (1,)), ((), ())), preferred_element_type=F32)


def dot_tn(a, b):
    return lax.dot_general(a, b, (((0,), (0,)), ((), ())), preferred_element_type=F32)


def dot_hi(a, b):
    return lax.dot_general(
        a, b, (((1,), (0,)), ((), ())), preferred_element_type=F32, precision=HI
    )


def rotate(x, cos, sin_signed):
    width = x.shape[-1]
    lane = lax.broadcasted_iota(jnp.int32, x.shape, 1)
    first = lax.rem(lane, HEAD_DIM) < HEAD_DIM // 2
    ahead = pltpu.roll(x, width - HEAD_DIM // 2, 1)
    behind = pltpu.roll(x, HEAD_DIM // 2, 1)
    return x * cos + jnp.where(first, ahead, behind) * sin_signed


def low_half(shape):
    return lax.broadcasted_iota(jnp.int32, shape, 1) < HEAD_DIM


def both_halves(tile):
    wide = tile.astype(F32)
    turned = pltpu.roll(wide, HEAD_DIM, 1)
    low = low_half(wide.shape)
    return (
        jnp.where(low, wide, turned).astype(BF16),
        jnp.where(low, turned, wide).astype(BF16),
    )


def stack_heads(rows, group):
    parts = []
    for head in range(group * GROUP_HEADS, (group + 1) * GROUP_HEADS):
        tile = rows[:, head // 2 * 128 : head // 2 * 128 + 128].astype(F32)
        low = low_half(tile.shape)
        keep = low if head % 2 == 0 else jnp.logical_not(low)
        parts.append(jnp.where(keep, tile, 0.0).astype(BF16))
    return jnp.concatenate(parts, axis=0)


def merge_heads(stacks, length):
    tiles = []
    for pair in range(HEADS // 2):
        halves = []
        for head in (2 * pair, 2 * pair + 1):
            at = head % GROUP_HEADS * length
            halves.append(stacks[head // GROUP_HEADS][at : at + length])
        tiles.append(jnp.where(low_half(halves[0].shape), halves[0], halves[1]))
    return jnp.concatenate(tiles, axis=1)


def fold_groups(sums):
    full = [value + pltpu.roll(value, HEAD_DIM, 1) for value in sums]
    return jnp.where(low_half(full[0].shape), full[0], full[1])


def rms_of(wide):
    return lax.rsqrt(jnp.mean(wide * wide, axis=-1, keepdims=True) + EPS)


def kernel(
    n_sec, n_dp, seqs, length, ring,
    entry, gain, w_in, w_up, final_gain, cos_ref, sin_ref, lengths, positive,
    out,
    hin, hout, gin, xs, probs, rows_buf, emb_all, pos_all, contexts,
    f_send, f_recv, b_send, b_recv, e_send, e_recv, p_send, p_recv,
    *gathering,
):
    sec = lax.axis_index("section")
    rep = lax.axis_index("dp")
    last = n_sec - 1
    width = entry.shape[-1]
    wqkv, wout = gathering[:2] if ring else (w_in, w_up)
    qw = wout.shape[0]
    blocks = 16 // seqs
    part = width // blocks
    micro = seqs // 2

    barrier = pltpu.get_barrier_semaphore()

    def peer(step):
        return lax.rem(rep + step, n_dp)

    for near in (lax.rem(sec + 1, n_sec), lax.rem(sec + n_sec - 1, n_sec)):
        pl.semaphore_signal(barrier, inc=1, device_id={"section": near}, device_id_type=MESH)
    for step in range(1, n_dp):
        pl.semaphore_signal(barrier, inc=1, device_id={"dp": peer(step)}, device_id_type=MESH)
    pl.semaphore_wait(barrier, n_dp + 1)

    def forward_copy(m):
        return pltpu.make_async_remote_copy(
            src_ref=hout.at[m], dst_ref=hin.at[m], send_sem=f_send.at[m], recv_sem=f_recv.at[m],
            device_id={"section": sec + 1}, device_id_type=MESH,
        )

    def backward_copy(m):
        return pltpu.make_async_remote_copy(
            src_ref=out.at[m], dst_ref=gin.at[m], send_sem=b_send.at[m], recv_sem=b_recv.at[m],
            device_id={"section": sec - 1}, device_id_type=MESH,
        )

    @pl.when(sec == 0)
    def _():
        hin[...] = entry[...]

    def live_keys(m):
        keys = lax.broadcasted_iota(jnp.int32, (GROUP_HEADS * length, length), 1)
        return keys < lengths[m]

    def attend(m):
        wide = hin[m].astype(F32)
        normed = (wide * rms_of(wide) * gain[...]).astype(BF16)
        x = rotate(dot_nn(normed, wqkv[...]), cos_ref[...], sin_ref[...]).astype(BF16)
        xs[m] = x
        keys = both_halves(x[:, qw : qw + 128])
        values = both_halves(x[:, qw + 128 : qw + 256])
        live = live_keys(m)
        stacks = []
        for group in range(KV_GROUPS):
            scores = dot_nt(stack_heads(x, group), keys[group]) * HEAD_DIM ** (-0.5)
            weights = jnp.where(live, jnp.exp(scores), 0.0)
            prob = weights / jnp.sum(weights, axis=-1, keepdims=True)
            probs[m, group] = prob
            stacks.append(dot_nn(prob.astype(BF16), values[group]))
        contexts[m] = merge_heads(stacks, length).astype(BF16)

    if ring:
        hop_send, hop_recv, side_send, side_recv, keep_sem = gathering[2:]
        chips = n_dp // 2
        reach = chips // 2
        core = lax.rem(rep, 2)
        chip = rep // 2

        def place(c):
            return c + (c // 2) * (1 - 2 * lax.rem(c, 2)) if chips == 4 else c

        at = place(chip)
        pieces = ((w_in, wqkv), (w_up, wout))

        def region(piece, shard, half):
            held = pieces[piece][1]
            rows = pieces[piece][0].shape[0]
            cols = held.shape[1]
            cut = (cols // 128 + 1) // 2 * 128
            span = {None: (0, cols), 0: (0, cut), 1: (cut, cols - cut)}[half]
            start = pl.multiple_of(shard * rows, rows)
            return held.at[pl.ds(start, rows), pl.ds(*span)]

        def own(piece, half):
            mine, held = pieces[piece]
            if half is None:
                return mine
            cols = held.shape[1]
            cut = (cols // 128 + 1) // 2 * 128
            return mine.at[:, pl.ds(*((0, cut), (cut, cols - cut))[half])]

        def half_of(way, step):
            return way if step == reach else None

        def hop(piece, way, step):
            turn = 1 if way == 0 else chips - 1
            source = place(lax.rem(at + (step - 1) * (chips - turn), chips)) * 2 + core
            half = half_of(way, step)
            target = place(lax.rem(at + turn, chips)) * 2 + core
            dst = region(piece, source, half)
            return pltpu.make_async_remote_copy(
                src_ref=own(piece, half) if step == 1 else dst, dst_ref=dst,
                send_sem=hop_send.at[piece, way, step - 1],
                recv_sem=hop_recv.at[piece, way, step - 1],
                device_id={"dp": target}, device_id_type=MESH,
            )

        def side(piece, way, step):
            turn = 1 if way == 0 else chips - 1
            source = place(lax.rem(at + step * (chips - turn), chips)) * 2 + core
            half = half_of(way, step)
            dst = region(piece, source, half)
            return pltpu.make_async_remote_copy(
                src_ref=own(piece, None) if step == 0 else dst, dst_ref=dst,
                send_sem=side_send.at[piece, way, step],
                recv_sem=side_recv.at[piece, way, step],
                device_id={"dp": chip * 2 + 1 - core}, device_id_type=MESH,
            )

        def keep(piece):
            return pltpu.make_async_copy(
                own(piece, None), region(piece, rep, None), keep_sem.at[piece]
            )

        sides = [(0, 0)] + [(way, step) for step in range(1, reach + 1) for way in (0, 1)]

        def begin(piece):
            for way in (0, 1):
                hop(piece, way, 1).start()
            side(piece, 0, 0).start()
            keep(piece).start()

        def advance(piece, step):
            for way in (0, 1):
                hop(piece, way, step).wait_recv()
                if step < reach:
                    hop(piece, way, step + 1).start()
                side(piece, way, step).start()

        def finish(piece):
            advance(piece, reach)
            keep(piece).wait()
            for way, step in sides:
                side(piece, way, step).wait_recv()

        begin(0)
        for step in range(1, reach):
            advance(0, step)
        begin(1)
        finish(0)

    def early(m, carry):
        if ring:
            @pl.when(m == seqs // 2)
            def _():
                for step in range(1, reach):
                    advance(1, step)

        @pl.when(sec == 0)
        def _():
            attend(m)

        return carry

    lax.fori_loop(0, seqs, early, 0)
    if ring:
        finish(1)

    def forward(m, carry):
        @pl.when(sec > 0)
        def _():
            forward_copy(m).wait_recv()
            attend(m)

        hout[m] = (hin[m].astype(F32) + dot_nn(contexts[m], wout[...])).astype(BF16)

        @pl.when(sec < last)
        def _():
            forward_copy(m).start()

        return carry

    lax.fori_loop(0, seqs, forward, 0)

    @pl.when(sec == last)
    def _():
        fgain = final_gain[...]
        row16 = lax.broadcasted_iota(jnp.int32, (16, part), 0)
        position = lax.broadcasted_iota(jnp.int32, (length, width), 0)
        own = jnp.zeros((16, part), F32)
        for j in range(seqs):
            picked = jnp.where(position == lengths[j] - 1, hout[j].astype(F32), 0.0)
            row = jnp.sum(picked, axis=0, keepdims=True)
            rows_buf[j] = row
            pooled = row * rms_of(row) * fgain
            unit = pooled * lax.rsqrt(jnp.sum(pooled * pooled, axis=-1, keepdims=True))
            for b in range(blocks):
                own = jnp.where(row16 == b * seqs + j, unit[:, b * part : (b + 1) * part], own)
        emb_all[rep] = own.astype(BF16)
        marks = jnp.zeros((8, 128), jnp.int32)
        mark_row = lax.broadcasted_iota(jnp.int32, (8, 128), 0)
        for i in range(micro):
            marks = jnp.where(mark_row == i, positive[i], marks)
        pos_all[rep] = marks

        def exchange(step):
            to = peer(step)
            return [
                pltpu.make_async_remote_copy(
                    src_ref=buf.at[rep], dst_ref=buf.at[rep],
                    send_sem=send.at[step], recv_sem=recv.at[step],
                    device_id={"dp": to}, device_id_type=MESH,
                )
                for buf, send, recv in ((emb_all, e_send, e_recv), (pos_all, p_send, p_recv))
            ]

        copies = [exchange(step) for step in range(1, n_dp)]
        for pair in copies:
            for copy in pair:
                copy.start()
        for pair in copies:
            for copy in pair:
                copy.wait()

        total = n_dp * seqs
        tall = n_dp * 16
        everyone = emb_all[...].reshape(tall, part)
        cross = dot_nt(everyone, everyone)
        ra = lax.broadcasted_iota(jnp.int32, (tall, tall), 0)
        ca = lax.broadcasted_iota(jnp.int32, (tall, tall), 1)
        same = lax.rem(ra, 16) // seqs == lax.rem(ca, 16) // seqs
        cross = jnp.where(same, cross, 0.0)
        fr = lax.broadcasted_iota(jnp.int32, (total, tall), 0)
        fc = lax.broadcasted_iota(jnp.int32, (total, tall), 1)
        fold = (fc // 16 * seqs + lax.rem(fc, seqs) == fr).astype(F32)
        logits = SHARPNESS * lax.dot_general(
            dot_hi(fold, cross), fold, (((1,), (1,)), ((), ())),
            preferred_element_type=F32, precision=HI,
        )
        qr = lax.broadcasted_iota(jnp.int32, (total, total), 0)
        dc = lax.broadcasted_iota(jnp.int32, (total, total), 1)
        doc = lax.rem(dc, 2) == 1
        weights = jnp.where(doc, jnp.exp(logits), 0.0)
        odds = weights / jnp.sum(weights, axis=-1, keepdims=True)
        marks_all = pos_all[...].reshape(n_dp * 8, 128).astype(F32)
        pr = lax.broadcasted_iota(jnp.int32, (total, n_dp * 8), 0)
        pc = lax.broadcasted_iota(jnp.int32, (total, n_dp * 8), 1)
        pick = (pr // seqs * 8 + lax.rem(pr, seqs) // 2 == pc).astype(F32)
        target = dot_hi(pick, marks_all)[:, :1]
        hit = jnp.logical_and(doc, (dc // 2).astype(F32) == target).astype(F32)
        coef = (odds - hit) * (COEF * SHARPNESS)
        coef = jnp.where(lax.rem(qr, 2) == 0, coef, 0.0)
        both = coef + coef.T
        ar = lax.broadcasted_iota(jnp.int32, (16, total), 0)
        ac = lax.broadcasted_iota(jnp.int32, (16, total), 1)
        mine = (rep * seqs + lax.rem(ar, seqs) == ac).astype(F32)
        spread = dot_hi(dot_hi(mine, both), fold)
        br = lax.broadcasted_iota(jnp.int32, (16, tall), 0)
        bc = lax.broadcasted_iota(jnp.int32, (16, tall), 1)
        spread = jnp.where(br // seqs == lax.rem(bc, 16) // seqs, spread, 0.0)
        grad16 = dot_hi(spread, everyone.astype(F32))
        for j in range(seqs):
            grad_e = jnp.concatenate(
                [grad16[b * seqs + j : b * seqs + j + 1] for b in range(blocks)], axis=1
            )
            row = rows_buf[j]
            scale = rms_of(row)
            pooled = row * scale * fgain
            size = lax.rsqrt(jnp.sum(pooled * pooled, axis=-1, keepdims=True))
            unit = pooled * size
            grad_f = size * (grad_e - unit * jnp.sum(unit * grad_e, axis=-1, keepdims=True))
            grad_n = grad_f * fgain
            grad_r = grad_n * scale - row * (
                scale * scale * scale * jnp.mean(row * grad_n, axis=-1, keepdims=True)
            )
            gin[j] = jnp.where(position == lengths[j] - 1, grad_r, 0.0).astype(BF16)

    def backward(m, carry):
        @pl.when(sec < last)
        def _():
            backward_copy(m).wait_recv()

        grad = gin[m]
        x = xs[m]
        keys = both_halves(x[:, qw : qw + 128])
        values = both_halves(x[:, qw + 128 : qw + 256])
        grad_ctx = dot_nt(grad, wout[...]).astype(BF16)
        grad_q, grad_k, grad_v = [], [], []
        for group in range(KV_GROUPS):
            prob = probs[m, group]
            upper = stack_heads(grad_ctx, group)
            grad_p = dot_nt(upper, values[group]).astype(BF16).astype(F32)
            grad_v.append(dot_tn(prob.astype(BF16), upper))
            inner = jnp.sum(grad_p * prob, axis=-1, keepdims=True)
            grad_s = (prob * (grad_p - inner) * HEAD_DIM ** (-0.5)).astype(BF16)
            grad_q.append(dot_nn(grad_s, keys[group]))
            grad_k.append(dot_tn(grad_s, stack_heads(x, group)))
        grad_x = jnp.concatenate(
            [merge_heads(grad_q, length), fold_groups(grad_k), fold_groups(grad_v)], axis=1
        )
        grad_x = grad_x.astype(BF16).astype(F32)
        grad_x = rotate(grad_x, cos_ref[...], -sin_ref[...]).astype(BF16)
        grad_n = dot_nt(grad_x, wqkv[...]).astype(BF16).astype(F32) * gain[...]
        wide = hin[m].astype(F32)
        scale = rms_of(wide)
        slope = scale * scale * scale * jnp.mean(wide * grad_n, axis=-1, keepdims=True)
        out[m] = (grad.astype(F32) + grad_n * scale - wide * slope).astype(BF16)

        @pl.when(sec > 0)
        def _():
            backward_copy(m).start()

        return carry

    lax.fori_loop(0, seqs, backward, 0)

    @pl.when(sec < last)
    def _():
        for m in range(seqs):
            forward_copy(m).wait_send()

    @pl.when(sec > 0)
    def _():
        for m in range(seqs):
            backward_copy(m).wait_send()

    if ring:
        for piece in (0, 1):
            for way in (0, 1):
                for step in range(1, reach + 1):
                    hop(piece, way, step).wait_send()
            for way, step in sides:
                side(piece, way, step).wait_send()


def swift(
    n_sec, n_dp, seqs, length,
    entry, gain, w_in, w_up, final_gain, cos_ref, sin_ref, lengths, positive,
    out,
    hin, hbase, hnext, gin, gout, pre, xs, probs, ctx, ctxp, wqkv, wout, wprev, wkvn, wqkv_t, wout_t, wkvn_t, gain_next,
    kvn, rowb, gkv, tail, emb_all, pos_all,
    hop_send, hop_recv, side_send, side_recv, keep_sem, up_send, up_recv,
    c_send, c_recv, f_send, f_recv, b_send, b_recv, k_send, k_recv,
    v_send, v_recv, g_send, g_recv, d_send, d_recv, e_send, e_recv, p_send, p_recv,
):
    sec = lax.axis_index("section")
    rep = lax.axis_index("dp")
    last = n_sec - 1
    pen = n_sec - 2
    width = entry.shape[-1]
    qw = wout.shape[0]
    blocks = 16 // seqs
    part = width // blocks
    micro = seqs // 2
    inner_plane = jnp.logical_and(sec >= 1, sec <= pen)

    barrier = pltpu.get_barrier_semaphore()

    def peer(step):
        return lax.rem(rep + step, n_dp)

    for near in (lax.rem(sec + 1, n_sec), lax.rem(sec + n_sec - 1, n_sec)):
        pl.semaphore_signal(barrier, inc=1, device_id={"section": near}, device_id_type=MESH)
    for step in range(1, n_dp):
        pl.semaphore_signal(barrier, inc=1, device_id={"dp": peer(step)}, device_id_type=MESH)
    pl.semaphore_wait(barrier, n_dp + 1)

    def to_section(src, dst, send, recv, turn):
        return pltpu.make_async_remote_copy(
            src_ref=src, dst_ref=dst, send_sem=send, recv_sem=recv,
            device_id={"section": sec + turn}, device_id_type=MESH,
        )

    core = lax.rem(rep, 2)
    chip = rep // 2
    chips = n_dp // 2

    def place(c):
        return c + (c // 2) * (1 - 2 * lax.rem(c, 2))

    at = place(chip)
    held = (wqkv, wout, wprev)
    shard_rows = (w_in.shape[0], w_up.shape[0], w_up.shape[0])

    def span(piece, half):
        cols = held[piece].shape[1]
        cut = (cols // 128 + 1) // 2 * 128
        return {None: (0, cols), 0: (0, cut), 1: (cut, cols - cut)}[half]

    def region(piece, shard, half):
        rows = shard_rows[piece]
        start = pl.multiple_of(shard * rows, rows)
        return held[piece].at[pl.ds(start, rows), pl.ds(*span(piece, half))]

    def own(piece, half):
        if piece == 2:
            return region(2, rep, half)
        return (w_in, w_up)[piece].at[:, pl.ds(*span(piece, half))]

    def source_of(way, step):
        turn = 1 if way == 0 else chips - 1
        return place(lax.rem(at + step * (chips - turn), chips)) * 2 + core

    def hop(piece, way, slot):
        turn = 1 if way == 0 else chips - 1
        target = place(lax.rem(at + turn, chips)) * 2 + core
        half = way if slot == 2 else slot
        dst = region(piece, rep if slot < 2 else source_of(way, 1), half)
        return pltpu.make_async_remote_copy(
            src_ref=own(piece, half) if slot < 2 else dst, dst_ref=dst,
            send_sem=hop_send.at[piece, way, slot], recv_sem=hop_recv.at[piece, way, slot],
            device_id={"dp": target}, device_id_type=MESH,
        )

    def hop_in(piece, way, slot):
        half = way if slot == 2 else slot
        dst = region(piece, source_of(way, 2 if slot == 2 else 1), half)
        return pltpu.make_async_remote_copy(
            src_ref=dst, dst_ref=dst,
            send_sem=hop_send.at[piece, way, slot], recv_sem=hop_recv.at[piece, way, slot],
            device_id={"dp": chip * 2 + 1 - core}, device_id_type=MESH,
        )

    def side(piece, way, slot):
        half = way if slot == 2 else slot
        shard = rep if way == 2 else source_of(way, 2 if slot == 2 else 1)
        dst = region(piece, shard, half)
        return pltpu.make_async_remote_copy(
            src_ref=own(piece, half) if way == 2 else dst, dst_ref=dst,
            send_sem=side_send.at[piece, way, slot], recv_sem=side_recv.at[piece, way, slot],
            device_id={"dp": chip * 2 + 1 - core}, device_id_type=MESH,
        )

    near = [(2, 0), (2, 1)] + [(way, slot) for slot in range(2) for way in (0, 1)]
    far = [(0, 2), (1, 2)]

    def keep(piece):
        return pltpu.make_async_copy(own(piece, None), region(piece, rep, None), keep_sem.at[piece])

    def take(piece, way, slot):
        hop_in(piece, way, slot).wait_recv()
        side(piece, way, slot).start()

    def hand_on(piece):
        take(piece, 0, 0)
        hop(piece, 0, 2).start()
        take(piece, 1, 1)
        hop(piece, 1, 2).start()

    def finish_near(piece):
        take(piece, 0, 1)
        take(piece, 1, 0)
        if piece < 2:
            keep(piece).wait()
        for way, slot in near:
            side(piece, way, slot).wait_recv()

    def finish_far(piece):
        for way, slot in far:
            take(piece, way, slot)
        for way, slot in far:
            side(piece, way, slot).wait_recv()

    def finish(piece):
        finish_near(piece)
        finish_far(piece)

    def entry_copy(dst):
        return pltpu.make_async_copy(entry, dst, keep_sem.at[2])

    def up(half):
        return to_section(own(1, half), region(2, rep, half), up_send.at[half], up_recv.at[half], 1)

    lent = span(1, 0)[1] // 2

    def lend():
        return to_section(own(1, 1), region(2, rep, 0), up_send.at[0], up_recv.at[0], 1)

    def quarter(held_ref, shard, which):
        start = pl.multiple_of(shard * w_up.shape[0], w_up.shape[0])
        return held_ref.at[pl.ds(start, w_up.shape[0]), pl.ds(which * lent, lent)]

    def narrow(held_ref, piece, way, slot):
        turn = 1 if way == 0 else chips - 1
        target = place(lax.rem(at + turn, chips)) * 2 + core
        part_of = quarter(held_ref, rep if slot < 2 else source_of(way, 1), way if slot == 2 else slot)
        return pltpu.make_async_remote_copy(
            src_ref=part_of, dst_ref=part_of,
            send_sem=hop_send.at[piece, way, slot], recv_sem=hop_recv.at[piece, way, slot],
            device_id={"dp": target}, device_id_type=MESH,
        )

    def give_back(which):
        shard = source_of(0, 2) if which == 2 else source_of(which, 1)
        return to_section(
            region(2, shard, 0), region(1, shard, 1), d_send.at[which], d_recv.at[which], -1
        )

    def ctx_copy(m):
        return to_section(ctx.at[m], ctxp.at[m], c_send.at[m], c_recv.at[m], 1)

    def h_copy(m):
        return to_section(hin.at[m], hbase.at[m], f_send.at[m], f_recv.at[m], 1)

    def h_last(m):
        return to_section(hnext.at[m], hbase.at[m], f_send.at[m], f_recv.at[m], 1)

    cuts = 4
    piece_width = width // cuts

    def g_copy(m, c):
        return to_section(gout.at[m, c], gin.at[m, c], b_send.at[m, c], b_recv.at[m, c], -1)

    kv_rows = pl.ds(pl.multiple_of(core * (width // 2), width // 2), width // 2)

    def kv_half():
        return to_section(
            wqkv.at[kv_rows, pl.ds(qw, 256)], wkvn.at[kv_rows], k_send.at[0], k_recv.at[0], -1
        )

    def kv_side():
        return pltpu.make_async_remote_copy(
            src_ref=wkvn.at[kv_rows], dst_ref=wkvn.at[kv_rows],
            send_sem=k_send.at[2], recv_sem=k_recv.at[2],
            device_id={"dp": chip * 2 + 1 - core}, device_id_type=MESH,
        )

    def gain_down():
        return to_section(gain, gain_next, k_send.at[1], k_recv.at[1], -1)

    def top(buf):
        return buf.at[pl.ds(0, 8)]

    def kv_up(m):
        return (
            to_section(kvn.at[m], kvn.at[m], v_send.at[m], v_recv.at[m], 1),
            to_section(rowb.at[m], rowb.at[m], v_send.at[seqs + m], v_recv.at[seqs + m], 1),
        )

    def gkv_copy(m):
        return to_section(gkv.at[m], gkv.at[m], g_send.at[m], g_recv.at[m], -1)

    def tail_copy():
        return to_section(top(tail), top(tail), g_send.at[seqs], g_recv.at[seqs], -1)

    @pl.when(sec < pen)
    def _():
        up(0).start()
        up(1).start()

    @pl.when(sec == pen)
    def _():
        lend().start()

    @pl.when(sec == last)
    def _():
        gain_down().start()

    for way in (0, 1):
        hop(0, way, way).start()
    for piece in (0, 1):
        keep(piece).start()
        side(piece, 2, 0).start()
        side(piece, 2, 1).start()

    @pl.when(sec == 0)
    def _():
        for way in (0, 1):
            hop(0, way, 1 - way).start()

    @pl.when(sec == last)
    def _():
        lend().wait_recv()
        for slot in (0, 1):
            for way in (0, 1):
                narrow(wprev, 2, way, slot).start()
        narrow(wprev, 2, 0, 0).wait_recv()
        narrow(wprev, 2, 0, 2).start()
        narrow(wprev, 2, 1, 1).wait_recv()
        narrow(wprev, 2, 1, 2).start()
        for way in (0, 1):
            hop(0, way, 1 - way).start()
        for way in (0, 1):
            narrow(wprev, 2, way, 1 - way).wait_recv()
            give_back(way).start()

    @pl.when(sec == 0)
    def _():
        entry_copy(hin).start()

    @pl.when(sec == 1)
    def _():
        entry_copy(hbase).start()

    @pl.when(inner_plane)
    def _():
        for half in (0, 1):
            up(half).wait_recv()
            side(2, 2, half).start()
            for way in (0, 1):
                hop(2, way, half).start()
        hand_on(2)
        for way in (0, 1):
            hop(0, way, 1 - way).start()

    hand_on(0)
    for way in (0, 1):
        @pl.when(sec != pen)
        def _():
            hop(1, way, way).start()

    for way in (0, 1):
        @pl.when(sec != pen)
        def _():
            hop(1, way, 1 - way).start()

        @pl.when(sec == pen)
        def _():
            hop(1, way, 0).start()

    @pl.when(sec == last)
    def _():
        for way in (0, 1):
            narrow(wprev, 2, way, 2).wait_recv()
        give_back(2).start()

    def step_in(m):
        ctx_copy(m).wait_recv()

        @pl.when(sec > 1)
        def _():
            h_copy(m).wait_recv()

        hin[m] = (hbase[m].astype(F32) + dot_nn(ctxp[m], wprev[...])).astype(BF16)

    def normalise(m, carry):
        wide = hin[m].astype(F32)
        hnext[m] = (wide * rms_of(wide) * gain[...]).astype(BF16)
        return carry

    def chip_part(c):
        depth = 2 * w_in.shape[0]
        rows = pl.ds(pl.multiple_of(c * depth, depth), depth)
        left = hnext[:, :, rows].reshape(seqs * length, depth)
        return dot_nn(left, wqkv[rows, :]).reshape(seqs, length, wqkv.shape[1])

    @pl.when(sec == 0)
    def _():
        entry_copy(hin).wait()
        lax.fori_loop(0, seqs, normalise, 0)

    @pl.when(inner_plane)
    def _():
        finish(2)

    @pl.when(sec == 1)
    def _():
        entry_copy(hbase).wait()

        def ahead(m, carry):
            step_in(m)
            normalise(m, 0)

            @pl.when(jnp.logical_and(sec < pen, m < seqs - 1))
            def _():
                h_copy(m).start()

            return carry

        lax.fori_loop(0, seqs, ahead, 0)

    finish_near(0)

    @pl.when(sec <= 1)
    def _():
        pre[...] = chip_part(chip)

        def beside(step, carry):
            pre[...] += chip_part(place(lax.rem(at + 2 * step + 1, chips)))
            return carry

        lax.fori_loop(0, 2, beside, 0)

    finish_far(0)

    @pl.when(sec <= 1)
    def _():
        pre[...] += chip_part(place(lax.rem(at + 2, chips)))

    @pl.when(sec == last)
    def _():
        kv_half().start()
        hand_on(1)

    def live_keys(m, columns):
        return lax.broadcasted_iota(jnp.int32, (length, columns), 0) < lengths[m]

    def project(m):
        wide = hin[m].astype(F32)
        normed = (wide * rms_of(wide) * gain[...]).astype(BF16)
        pre[m] = dot_nn(normed, wqkv[...])

    def attend(m):
        x = rotate(pre[m], cos_ref[...], sin_ref[...]).astype(BF16)
        xs[m] = x
        keys = both_halves(x[:, qw : qw + 128])
        values = both_halves(x[:, qw + 128 : qw + 256])
        live = live_keys(m, GROUP_HEADS * length)
        stacks = []
        for group in range(KV_GROUPS):
            scores = dot_nt(keys[group], stack_heads(x, group)) * HEAD_DIM ** (-0.5)
            weights = jnp.where(live, jnp.exp(scores), 0.0)
            prob = weights / jnp.sum(weights, axis=0, keepdims=True)
            probs[m, group] = prob
            stacks.append(dot_tn(prob.astype(BF16), values[group]))
        ctx[m] = merge_heads(stacks, length).astype(BF16)

    @pl.when(sec < pen)
    def _():
        def forward(m, carry):
            @pl.when(sec > 1)
            def _():
                step_in(m)
                h_copy(m).start()
                project(m)

            attend(m)
            ctx_copy(m).start()

            @pl.when(jnp.logical_and(sec == 1, m == seqs - 2))
            def _():
                h_copy(seqs - 1).start()

            return carry

        lax.fori_loop(0, seqs, forward, 0)
        hand_on(1)

    flat = seqs * length
    row8 = lax.broadcasted_iota(jnp.int32, (8, 1), 0)
    spot = lax.broadcasted_iota(jnp.int32, (length, 1), 0)

    def pick(value, j):
        return jnp.sum(jnp.where(spot == lengths[j] - 1, value, 0.0), axis=0, keepdims=True)

    @pl.when(sec == pen)
    def _():
        def rows_forward(m, count):
            these = pl.ds(m, count)
            for i in range(count):
                ctx_copy(m + i).wait_recv()
                h_copy(m + i).wait_recv()
            update = dot_nn(ctxp[these].reshape(count * length, qw), wprev[...])
            wide = hbase[these].reshape(count * length, width).astype(F32) + update
            wide = wide.astype(BF16)
            hin[these] = wide.reshape(count, length, width)
            wide = wide.astype(F32)
            scaled = dot_nn((wide * gain[...]).astype(BF16), wqkv[...]) * rms_of(wide)
            pre[these] = scaled.reshape(count, length, wqkv.shape[1])
            for i in range(count):
                attend(m + i)

        def pair(p, carry):
            two = pl.ds(2 * p, 2)

            @pl.when(p == 0)
            def _():
                for way in (0, 1):
                    take(1, way, 0)
                    narrow(wout, 1, way, 2).start()

            rows_forward(2 * p, 2)

            @pl.when(p == 0)
            def _():
                for way in (0, 1):
                    give_back(way).wait_recv()
                    side(1, way, 1).start()
                give_back(2).wait_recv()
                side(1, 1, 2).start()
                for way in (0, 1):
                    narrow(wout, 1, way, 2).wait_recv()
                side(1, 0, 2).start()
                keep(1).wait()
                for way, slot in near + far:
                    side(1, way, slot).wait_recv()
                gain_down().wait_recv()
                kv_half().wait_recv()
                kv_side().start()
                kv_side().wait_recv()

            update = dot_nn(ctx[two].reshape(2 * length, qw), wout[...])
            wide = (hin[two].reshape(2 * length, width).astype(F32) + update).astype(BF16)
            hnext[two] = wide.reshape(2, length, width)
            wide = wide.astype(F32)
            kv_two = dot_nn((wide * gain_next[...]).astype(BF16), wkvn[...]) * rms_of(wide)
            for i in range(2):
                m = 2 * p + i
                kvn[m] = rotate(
                    kv_two[i * length : (i + 1) * length], cos_ref[:, qw:], sin_ref[:, qw:]
                ).astype(BF16)
                row = pick(wide[i * length : (i + 1) * length], m)
                tiles = [row[:, c * 128 : (c + 1) * 128] for c in range(width // 128)]
                spare = rowb.shape[1] - width // 128
                rowb[m] = jnp.concatenate(tiles + [jnp.zeros((spare, 128), F32)], axis=0).astype(BF16)
                for copy in kv_up(m):
                    copy.start()
            return carry

        lax.fori_loop(0, seqs // 2, pair, 0)

    @pl.when(sec != pen)
    def _():
        finish(1)

    def turn_over(src, dst):
        def strip(j, carry):
            rows = pl.ds(pl.multiple_of(j * 128, 128), 128)
            dst[:, rows] = src[rows, :].T
            return carry

        lax.fori_loop(0, src.shape[0] // 128, strip, 0)

    @pl.when(sec != pen)
    def _():
        turn_over(wout, wout_t)
        turn_over(wqkv, wqkv_t)

    @pl.when(sec == pen)
    def _():
        for m in range(seqs):
            h_last(m).start()
        turn_over(wkvn, wkvn_t)
        turn_over(wout, wout_t)
        turn_over(wqkv, wqkv_t)

    def last_grad(m, wkv_t, gain_row, layer_in):
        here = spot == lengths[m] - 1
        mine = tail[0:8].astype(F32)
        query_part = jnp.sum(jnp.where(row8 == m, mine, 0.0), axis=0, keepdims=True)
        seed = jnp.sum(jnp.where(row8 == m + seqs, mine, 0.0), axis=0, keepdims=True)
        grad_n = dot_nn(gkv[m], wkv_t) + jnp.where(here, query_part, 0.0)
        grad_n = grad_n.astype(BF16).astype(F32) * gain_row
        wide = layer_in.astype(F32)
        scale = rms_of(wide)
        slope = scale * scale * scale * jnp.mean(wide * grad_n, axis=-1, keepdims=True)
        return (jnp.where(here, seed, 0.0) + grad_n * scale - wide * slope).astype(BF16)

    @pl.when(sec == last)
    def _():
        def gather_rows(parts):
            full = jnp.zeros((8, parts[0].shape[1]), F32)
            for j, row in enumerate(parts):
                full = jnp.where(row8 == j, row, full)
            return full

        def swap_half(head):
            return head // GROUP_HEADS != head % 2

        def half_mask(head, group_side):
            low = low_half((8, 128))
            upper_side = head // GROUP_HEADS if group_side else head % 2
            return low if upper_side == 0 else jnp.logical_not(low)

        def to_stack(rows):
            heads = []
            for head in range(HEADS):
                tile = rows[:, head // 2 * 128 : head // 2 * 128 + 128]
                if swap_half(head):
                    tile = pltpu.roll(tile, HEAD_DIM, 1)
                heads.append(jnp.where(half_mask(head, True), tile, 0.0))
            row16 = lax.broadcasted_iota(jnp.int32, (16, 128), 0)
            blocks_of = []
            for j in range(seqs):
                full = jnp.zeros((16, 128), F32)
                for head, tile in enumerate(heads):
                    full = jnp.where(row16 == head, tile[j : j + 1], full)
                blocks_of.append(full)
            return jnp.concatenate(blocks_of, axis=0).astype(BF16)

        def from_stack(stack):
            tiles = []
            for pair in range(HEADS // 2):
                halves = []
                for head in (2 * pair, 2 * pair + 1):
                    tile = gather_rows([stack[j * 16 + head : j * 16 + head + 1] for j in range(seqs)])
                    halves.append(pltpu.roll(tile, HEAD_DIM, 1) if swap_half(head) else tile)
                tiles.append(jnp.where(low_half((8, 128)), halves[0], halves[1]))
            return jnp.concatenate(tiles, axis=1)

        cos_row = gather_rows([pick(cos_ref[:, :qw], j) for j in range(seqs)])
        sin_row = gather_rows([pick(sin_ref[:, :qw], j) for j in range(seqs)])
        stacked_rows = lax.broadcasted_iota(jnp.int32, (16 * seqs, flat), 0) // 16
        key_at = lax.broadcasted_iota(jnp.int32, (16 * seqs, flat), 1)
        live = jnp.zeros((16 * seqs, flat), jnp.int32)
        for j in range(seqs):
            live = jnp.where(stacked_rows == j, j * length + lengths[j], live)
        live = jnp.logical_and(key_at >= stacked_rows * length, key_at < live)

        for m in range(seqs):
            for copy in kv_up(m):
                copy.wait_recv()
        flat_rows = []
        for j in range(seqs):
            tiles = rowb[j].astype(F32)
            flat_rows.append(
                jnp.concatenate([tiles[c : c + 1] for c in range(width // 128)], axis=1)
            )
        rows_in = gather_rows(flat_rows)
        query = dot_nn((rows_in * gain[...]).astype(BF16), wqkv[:, :qw]) * rms_of(rows_in)
        query = rotate(query, cos_row, sin_row).astype(BF16).astype(F32)
        keys = kvn[...].reshape(flat, 256)[:, :128]
        values = kvn[...].reshape(flat, 256)[:, 128:256]
        query_stack = to_stack(query)
        scores = dot_nt(query_stack, keys) * HEAD_DIM ** (-0.5)
        weights = jnp.where(live, jnp.exp(scores), 0.0)
        prob = weights / jnp.sum(weights, axis=-1, keepdims=True)
        prob_low = prob.astype(BF16)
        context = from_stack(dot_nn(prob_low, values)).astype(BF16)
        rows_out = (rows_in + dot_nn(context, wout[...])).astype(BF16).astype(F32)

        fgain = jnp.concatenate(
            [final_gain[i : i + 1] for i in range(final_gain.shape[0])], axis=1
        )
        row_part = lax.broadcasted_iota(jnp.int32, (16, part), 0)
        scale_out = rms_of(rows_out)
        pooled = rows_out * scale_out * fgain
        total_sq = jnp.sum(pooled * pooled, axis=-1, keepdims=True)
        size = lax.rsqrt(jnp.where(row8 < seqs, total_sq, 1.0))
        unit = pooled * size
        mine16 = jnp.zeros((16, part), F32)
        for j in range(seqs):
            for b in range(blocks):
                mine16 = jnp.where(
                    row_part == b * seqs + j, unit[j : j + 1, b * part : (b + 1) * part], mine16
                )
        emb_all[rep] = mine16.astype(BF16)
        marks = jnp.zeros((8, 128), jnp.int32)
        mark_row = lax.broadcasted_iota(jnp.int32, (8, 128), 0)
        for i in range(micro):
            marks = jnp.where(mark_row == i, positive[i], marks)
        pos_all[rep] = marks

        def exchange(step):
            to = peer(step)
            return [
                pltpu.make_async_remote_copy(
                    src_ref=buf.at[rep], dst_ref=buf.at[rep],
                    send_sem=send.at[step], recv_sem=recv.at[step],
                    device_id={"dp": to}, device_id_type=MESH,
                )
                for buf, send, recv in ((emb_all, e_send, e_recv), (pos_all, p_send, p_recv))
            ]

        copies = [exchange(step) for step in range(1, n_dp)]
        for pair in copies:
            for copy in pair:
                copy.start()
        for pair in copies:
            for copy in pair:
                copy.wait()

        total = n_dp * seqs
        tall = n_dp * 16
        everyone = emb_all[...].reshape(tall, part)
        pr = lax.broadcasted_iota(jnp.int32, (tall, tall), 0)
        pc = lax.broadcasted_iota(jnp.int32, (tall, tall), 1)
        in_block = lax.rem(pr, total)
        home = in_block // seqs * 16 + pr // total * seqs + lax.rem(in_block, seqs)
        sorted_rows = dot_nn((home == pc).astype(BF16), everyone).astype(BF16)
        every = jnp.concatenate(
            [sorted_rows[b * total : (b + 1) * total] for b in range(blocks)], axis=1
        )
        logits = SHARPNESS * dot_nt(every, every)
        qr = lax.broadcasted_iota(jnp.int32, (total, total), 0)
        dc = lax.broadcasted_iota(jnp.int32, (total, total), 1)
        doc = lax.rem(dc, 2) == 1
        weights = jnp.where(doc, jnp.exp(logits), 0.0)
        odds = weights / jnp.sum(weights, axis=-1, keepdims=True)
        marks_all = pos_all[...].reshape(n_dp * 8, 128).astype(F32)
        pr = lax.broadcasted_iota(jnp.int32, (total, n_dp * 8), 0)
        pc = lax.broadcasted_iota(jnp.int32, (total, n_dp * 8), 1)
        chosen = (pr // seqs * 8 + lax.rem(pr, seqs) // 2 == pc).astype(F32)
        target = dot_hi(chosen, marks_all)[:, :1]
        hit = jnp.logical_and(doc, (dc // 2).astype(F32) == target).astype(F32)
        coef = (odds - hit) * (COEF * SHARPNESS)
        coef = jnp.where(lax.rem(qr, 2) == 0, coef, 0.0)
        both = coef + coef.T
        own_coef = gather_rows([
            jnp.sum(jnp.where(qr == rep * seqs + j, both, 0.0), axis=0, keepdims=True)
            for j in range(seqs)
        ])
        high = own_coef.astype(BF16).astype(F32)
        middle = (own_coef - high).astype(BF16).astype(F32)
        parts = jnp.concatenate([high, middle, own_coef - high - middle], axis=0).astype(BF16)
        grad_parts = dot_nn(parts, every)
        grad_e = grad_parts[0:8] + grad_parts[8:16] + grad_parts[16:24]
        grad_f = size * (grad_e - unit * jnp.sum(unit * grad_e, axis=-1, keepdims=True))
        grad_n = grad_f * fgain
        seeds = grad_n * scale_out - rows_out * (
            scale_out * scale_out * scale_out
            * jnp.mean(rows_out * grad_n, axis=-1, keepdims=True)
        )
        seed8 = jnp.where(row8 < seqs, seeds, 0.0).astype(BF16)
        grad_ctx = dot_nn(seed8, wout_t[...]).astype(BF16).astype(F32)
        upper = to_stack(grad_ctx)
        grad_p = dot_nt(upper, values).astype(BF16).astype(F32)
        grad_v = dot_tn(prob_low, upper)
        inner = jnp.sum(grad_p * prob, axis=-1, keepdims=True)
        grad_s = (prob * (grad_p - inner) * HEAD_DIM ** (-0.5)).astype(BF16)
        grad_k = dot_tn(grad_s, query_stack)
        grad_kv = jnp.concatenate([grad_k, grad_v], axis=1).astype(BF16).astype(F32)
        for j in range(seqs):
            gkv[j] = rotate(
                grad_kv[j * length : (j + 1) * length], cos_ref[:, qw:], -sin_ref[:, qw:]
            ).astype(BF16)
        for j in range(seqs):
            gkv_copy(j).start()
        grad_query = from_stack(dot_nn(grad_s, keys)).astype(BF16).astype(F32)
        grad_query = rotate(grad_query, cos_row, -sin_row).astype(BF16)
        query_part = dot_nn(grad_query, wqkv_t[:qw, :])
        seed_full = seed8.astype(F32)
        both_parts = query_part
        for j in range(seqs):
            both_parts = jnp.where(row8 == seqs + j, seed_full[j : j + 1], both_parts)
        tail[...] = jnp.concatenate([both_parts, both_parts], axis=0).astype(BF16)
        tail_copy().start()

        def own_grad(m, carry):
            h_last(m).wait_recv()
            out[m] = last_grad(m, wqkv_t[qw : qw + 256, :], gain[...], hbase[m])
            return carry

        lax.fori_loop(0, seqs, own_grad, 0)

    @pl.when(sec < last)
    def _():
        @pl.when(sec == pen)
        def _():
            tail_copy().wait_recv()

        def backward(m, carry):
            x = xs[m]
            keys = both_halves(x[:, qw : qw + 128])
            values = both_halves(x[:, qw + 128 : qw + 256])
            scale = rms_of(hin[m].astype(F32))
            gain_row = gain[...]

            @pl.when(sec == pen)
            def _():
                gkv_copy(m).wait_recv()
                first = last_grad(m, wkvn_t[...], gain_next[...], hnext[m])
                for c in range(cuts):
                    gin[m, c] = first[:, c * piece_width : (c + 1) * piece_width]

            grad_ctx = jnp.zeros((length, qw), F32)
            for c in range(cuts):
                @pl.when(sec < pen)
                def _():
                    g_copy(m, c).wait_recv()

                lanes = slice(c * piece_width, (c + 1) * piece_width)
                grad_ctx += dot_nn(gin[m, c], wout_t[lanes, :])
            grad_ctx = grad_ctx.astype(BF16)
            grad_q, grad_k, grad_v = [], [], []
            for group in range(KV_GROUPS):
                prob = probs[m, group]
                upper = stack_heads(grad_ctx, group)
                grad_p = dot_nt(values[group], upper).astype(BF16).astype(F32)
                grad_v.append(dot_nn(prob.astype(BF16), upper))
                inner = jnp.sum(grad_p * prob, axis=0, keepdims=True)
                grad_s = (prob * (grad_p - inner) * HEAD_DIM ** (-0.5)).astype(BF16)
                grad_q.append(dot_tn(grad_s, keys[group]))
                grad_k.append(dot_nn(grad_s, stack_heads(x, group)))
            grad_x = jnp.concatenate(
                [merge_heads(grad_q, length), fold_groups(grad_k), fold_groups(grad_v)], axis=1
            )
            grad_x = grad_x.astype(BF16).astype(F32)
            along = jnp.sum(grad_x * x.astype(F32), axis=-1, keepdims=True)
            slope = scale * scale * along * (1.0 / width)
            grad_x = rotate(grad_x, cos_ref[...], -sin_ref[...]).astype(BF16)
            for c in range(cuts):
                lanes = slice(c * piece_width, (c + 1) * piece_width)
                grad_n = dot_nn(grad_x, wqkv_t[:, lanes]).astype(BF16).astype(F32)
                grad_n = grad_n * gain_row[:, lanes]
                wide = hin[m, :, lanes].astype(F32)
                piece_grad = gin[m, c].astype(F32) + grad_n * scale - wide * slope
                piece_grad = piece_grad.astype(BF16)
                out[m, :, lanes] = piece_grad

                @pl.when(sec > 0)
                def _():
                    gout[m, c] = piece_grad
                    g_copy(m, c).start()

            return carry

        lax.fori_loop(0, seqs, backward, 0)

    @pl.when(sec < pen)
    def _():
        up(0).wait_send()
        up(1).wait_send()
        for m in range(seqs):
            ctx_copy(m).wait_send()

    @pl.when(jnp.logical_and(sec >= 1, sec < pen))
    def _():
        for m in range(seqs):
            h_copy(m).wait_send()

    @pl.when(inner_plane)
    def _():
        for m in range(seqs):
            for c in range(cuts):
                g_copy(m, c).wait_send()

    @pl.when(sec == pen)
    def _():
        lend().wait_send()
        kv_side().wait_send()
        for m in range(seqs):
            for copy in kv_up(m):
                copy.wait_send()
        for m in range(seqs):
            h_last(m).wait_send()

    @pl.when(sec == last)
    def _():
        kv_half().wait_send()
        gain_down().wait_send()
        for which in range(3):
            give_back(which).wait_send()
        for way in (0, 1):
            for slot in range(3):
                narrow(wprev, 2, way, slot).wait_send()
        for m in range(seqs):
            gkv_copy(m).wait_send()
        tail_copy().wait_send()

    def settle(piece):
        for way, slot in near + far:
            side(piece, way, slot).wait_send()
        for way in (0, 1):
            hop(piece, way, 0).wait_send()
            if piece != 1:
                hop(piece, way, 1).wait_send()
                hop(piece, way, 2).wait_send()

    settle(0)
    settle(1)

    @pl.when(sec != pen)
    def _():
        for way in (0, 1):
            hop(1, way, 1).wait_send()
            hop(1, way, 2).wait_send()

    @pl.when(sec == pen)
    def _():
        for way in (0, 1):
            narrow(wout, 1, way, 2).wait_send()

    @pl.when(inner_plane)
    def _():
        settle(2)


def tables(length, qw, columns):
    lane = np.arange(columns)
    half = HEAD_DIM // 2
    frequency = np.float32(ROPE_BASE) ** (
        -(lane % half).astype(np.float32) * np.float32(2.0 / HEAD_DIM)
    )
    angles = np.arange(length, dtype=np.float32)[:, None] * frequency[None, :]
    turned = (lane < columns - KV_GROUPS * HEAD_DIM)[None, :]
    sign = np.where(lane % HEAD_DIM < half, -1.0, 1.0)[None, :]
    cos = np.where(turned, np.cos(angles), 1.0).astype(np.float32)
    sin = np.where(turned, np.sin(angles) * sign, 0.0).astype(np.float32)
    return jnp.asarray(cos), jnp.asarray(sin)


def per_device(entry, norm_gain, w_qkv, w_out, final_gain, lengths, positive):
    n_sec = lax.axis_size("section")
    n_dp = lax.axis_size("dp")
    seqs = lengths.shape[0]
    rows, width = entry.shape
    length = rows // seqs
    qw = w_out.shape[1] * n_dp
    columns = w_qkv.shape[2]
    ring = w_qkv.shape[1] % 16 == 0 and w_out.shape[1] % 16 == 0 and n_dp % 4 == 0
    if ring:
        full_qkv, full_out = w_qkv[0], w_out[0]
    else:
        full_qkv = lax.all_gather(w_qkv, "dp", axis=1, tiled=True)[0]
        full_out = lax.all_gather(w_out, "dp", axis=1, tiled=True)[0]
    cos, sin = tables(length, qw, columns)
    vmem = pl.BlockSpec(memory_space=pltpu.VMEM)
    smem = pl.BlockSpec(memory_space=pltpu.SMEM)
    anywhere = pl.BlockSpec(memory_space=pl.ANY)
    part = width // (16 // seqs)
    dma = pltpu.SemaphoreType.DMA
    block = (seqs, length, width)
    if ring and n_dp // 2 == 4 and n_sec > 3:
        kv = columns - qw
        result = pl.pallas_call(
            functools.partial(swift, n_sec, n_dp, seqs, length),
            out_shape=jax.ShapeDtypeStruct(block, BF16),
            in_specs=[anywhere, vmem, anywhere, anywhere] + [vmem] * 3 + [smem] * 2,
            out_specs=vmem,
            scratch_shapes=[
                pltpu.VMEM(block, BF16),
                pltpu.VMEM(block, BF16),
                pltpu.VMEM(block, BF16),
                pltpu.VMEM((seqs, 4, length, width // 4), BF16),
                pltpu.VMEM((seqs, 4, length, width // 4), BF16),
                pltpu.VMEM((seqs, length, columns), F32),
                pltpu.VMEM((seqs, length, columns), BF16),
                pltpu.VMEM((seqs, KV_GROUPS, length, GROUP_HEADS * length), F32),
                pltpu.VMEM((seqs, length, qw), BF16),
                pltpu.VMEM((seqs, length, qw), BF16),
                pltpu.VMEM((width, columns), BF16),
                pltpu.VMEM((qw, width), BF16),
                pltpu.VMEM((qw, width), BF16),
                pltpu.VMEM((width, kv), BF16),
                pltpu.VMEM((columns, width), BF16),
                pltpu.VMEM((width, qw), BF16),
                pltpu.VMEM((kv, width), BF16),
                pltpu.VMEM((1, width), F32),
                pltpu.VMEM((seqs, length, kv), BF16),
                pltpu.VMEM((seqs, (width // 128 + 15) // 16 * 16, 128), BF16),
                pltpu.VMEM((seqs, length, kv), BF16),
                pltpu.VMEM((16, width), BF16),
                pltpu.VMEM((n_dp, 16, part), BF16),
                pltpu.VMEM((n_dp, 8, 128), jnp.int32),
                dma((3, 2, 3)), dma((3, 2, 3)), dma((3, 3, 3)), dma((3, 3, 3)), dma((3,)),
                dma((2,)), dma((2,)),
                dma((seqs,)), dma((seqs,)), dma((seqs,)), dma((seqs,)),
                dma((seqs, 4)), dma((seqs, 4)), dma((3,)), dma((3,)),
                dma((2 * seqs,)), dma((2 * seqs,)), dma((seqs + 1,)), dma((seqs + 1,)),
                dma((3,)), dma((3,)),
                dma((n_dp,)), dma((n_dp,)), dma((n_dp,)), dma((n_dp,)),
            ],
            compiler_params=pltpu.CompilerParams(
                collective_id=0, has_side_effects=True, vmem_limit_bytes=60 * 1024 * 1024
            ),
        )(
            entry.reshape(block), norm_gain, w_qkv[0], w_out[0],
            final_gain.reshape(width // 128, 128), cos, sin, lengths, positive,
        )
        return result.reshape(1, rows, width)
    reach = n_dp // 4
    gathering = [
        pltpu.VMEM((width, columns), BF16),
        pltpu.VMEM((qw, width), BF16),
        pltpu.SemaphoreType.DMA((2, 2, reach)),
        pltpu.SemaphoreType.DMA((2, 2, reach)),
        pltpu.SemaphoreType.DMA((2, 2, reach + 1)),
        pltpu.SemaphoreType.DMA((2, 2, reach + 1)),
        pltpu.SemaphoreType.DMA((2,)),
    ] if ring else []
    result = pl.pallas_call(
        functools.partial(kernel, n_sec, n_dp, seqs, length, ring),
        out_shape=jax.ShapeDtypeStruct(block, BF16),
        in_specs=[vmem] * 7 + [smem] * 2,
        out_specs=vmem,
        scratch_shapes=[
            pltpu.VMEM(block, BF16),
            pltpu.VMEM(block, BF16),
            pltpu.VMEM(block, BF16),
            pltpu.VMEM((seqs, length, columns), BF16),
            pltpu.VMEM((seqs, KV_GROUPS, GROUP_HEADS * length, length), F32),
            pltpu.VMEM((seqs, 1, width), F32),
            pltpu.VMEM((n_dp, 16, part), BF16),
            pltpu.VMEM((n_dp, 8, 128), jnp.int32),
            pltpu.VMEM((seqs, length, qw), BF16),
            dma((seqs,)), dma((seqs,)), dma((seqs,)), dma((seqs,)),
            dma((n_dp,)), dma((n_dp,)), dma((n_dp,)), dma((n_dp,)),
            *gathering,
        ],
        compiler_params=pltpu.CompilerParams(
            collective_id=0, has_side_effects=True, vmem_limit_bytes=60 * 1024 * 1024
        ),
    )(
        entry.reshape(block), norm_gain, full_qkv, full_out, final_gain.reshape(1, width),
        cos, sin, lengths, positive,
    )
    return result.reshape(1, rows, width)


def solution(mesh):
    return jax.shard_map(
        per_device,
        mesh=mesh,
        in_specs=(
            P("dp", None),
            P("section", None),
            P("section", "dp", None),
            P("section", "dp", None),
            P(),
            P("dp"),
            P("dp"),
        ),
        out_specs=P("section", "dp", None),
        check_vma=False,
    )
```
